32 devices in a mesh: dp: 2 (over x), tp: 4 (over z), cp: 4 (over y, core).
Axes of the slice: x: 2, y: 2, z: 4, core: 2. Of those that a mesh axis runs over, the one named last changes fastest.
Arguments:
- hidden: bfloat16 [16, 64, 4096], P('dp'), parts along dimension 0
- prefix_len: int32 [16], P('dp'), parts along dimension 0
- k_cache: bfloat16 [16, 16384, 8, 128], P('dp', 'cp', 'tp'), parts along dimension 0
- v_cache: bfloat16 [16, 16384, 8, 128], P('dp', 'cp', 'tp'), parts along dimension 0
- attn_norm: bfloat16 [4096], replicated
- w_q: bfloat16 [4096, 4096], P(None, 'tp')
- w_k: bfloat16 [4096, 1024], P(None, 'tp')
- w_v: bfloat16 [4096, 1024], P(None, 'tp')
- w_o: bfloat16 [4096, 4096], P('tp')
- q_norm: bfloat16 [128], replicated
- k_norm: bfloat16 [128], replicated
Outputs:
- output 1: bfloat16 [16, 64, 4096], P('dp'), parts along dimension 0
- output 2: bfloat16 [16, 64, 8, 128], P('dp', None, 'tp'), parts along dimension 0
- output 3: bfloat16 [16, 64, 8, 128], P('dp', None, 'tp'), parts along dimension 0
There are 2 independent parts. The reference program is written for one: setup_inputs(seed, part) draws one part's arguments, and reference() takes and returns one part's arrays. A program takes and returns all parts, laid end to end along the dimension named above; an argument that names none is the same for every part.
All inputs are finite; a program needn't handle non-finite values.
Results may differ from the reference program's by a relative error of at most 0.00828708.
Values sent between devices are 32-bit elements.
A program may use at most 1 GiB of HBM per device.

```python
import jax
import jax.numpy as jnp
from jax import lax

NUM_SEQ = 8
NEW_TOKENS = 64
CACHE_LEN = 16384
D_MODEL = 4096
N_HEADS = 32
KV_HEADS = 8
HEAD_DIM = 128


def rms_scale(tensor, norm_gain):
    mean_sq = jnp.mean(jnp.square(tensor), axis=-1, keepdims=True)
    return tensor * lax.rsqrt(mean_sq + 1e-6) * norm_gain


def rope_apply(tensor, positions):
    half_dim = HEAD_DIM // 2
    inv_freq = 1.0 / (1000000.0 ** (jnp.arange(half_dim, dtype=jnp.float32) * 2.0 / HEAD_DIM))
    angles = positions.astype(jnp.float32)[..., None] * inv_freq
    cos_t = jnp.cos(angles)[..., None, :]
    sin_t = jnp.sin(angles)[..., None, :]
    lead_half = tensor[..., :half_dim]
    tail_half = tensor[..., half_dim:]
    return jnp.concatenate([lead_half * cos_t - tail_half * sin_t, tail_half * cos_t + lead_half * sin_t], axis=-1)


def smooth_field(key, amplitude):
    n_freq = 4
    coords = (jnp.arange(CACHE_LEN, dtype=jnp.float32) + 0.5) / CACHE_LEN
    angles = jnp.pi * coords[:, None] * jnp.arange(1, n_freq + 1, dtype=jnp.float32)[None, :]
    cos_basis = jnp.concatenate([jnp.cos(angles), jnp.sin(angles)], axis=1)
    coeffs = jax.random.normal(key, (NUM_SEQ, 2 * n_freq, KV_HEADS, HEAD_DIM), jnp.float32) * (amplitude / n_freq ** 0.5)
    return jnp.einsum('pf,bfke->bpke', cos_basis, coeffs)


def setup_inputs(seed: int = 0, part: int = 0) -> dict:
    shared = jax.random.split(jax.random.key(seed), 8)
    part_keys = jax.random.split(jax.random.fold_in(jax.random.key(seed + 1), part), 8)
    cache_shape = (NUM_SEQ, CACHE_LEN, KV_HEADS, HEAD_DIM)
    len_draw = jax.random.randint(part_keys[1], (NUM_SEQ,), 0, CACHE_LEN + 1)
    full_at = jax.random.randint(part_keys[2], (), 0, NUM_SEQ)
    prefix_len = jnp.where(jnp.arange(NUM_SEQ) == full_at, CACHE_LEN, len_draw).astype(jnp.int32)
    k_cache = smooth_field(part_keys[3], 2.0) + 0.5 * jax.random.normal(part_keys[4], cache_shape, jnp.float32)
    v_cache = smooth_field(part_keys[5], 1.0) + 0.5 * jax.random.normal(part_keys[6], cache_shape, jnp.float32)
    q_width = N_HEADS * HEAD_DIM
    kv_width = KV_HEADS * HEAD_DIM
    return {
        'hidden': jax.random.normal(part_keys[0], (NUM_SEQ, NEW_TOKENS, D_MODEL), jnp.float32).astype(jnp.bfloat16),
        'prefix_len': prefix_len,
        'k_cache': k_cache.astype(jnp.bfloat16),
        'v_cache': v_cache.astype(jnp.bfloat16),
        'attn_norm': (1.0 + 0.4 * jax.random.normal(shared[0], (D_MODEL,), jnp.float32)).astype(jnp.bfloat16),
        'w_q': (jax.random.normal(shared[1], (D_MODEL, q_width), jnp.float32) * D_MODEL ** -0.5).astype(jnp.bfloat16),
        'w_k': (jax.random.normal(shared[2], (D_MODEL, kv_width), jnp.float32) * D_MODEL ** -0.5).astype(jnp.bfloat16),
        'w_v': (jax.random.normal(shared[3], (D_MODEL, kv_width), jnp.float32) * D_MODEL ** -0.5).astype(jnp.bfloat16),
        'w_o': (jax.random.normal(shared[4], (q_width, D_MODEL), jnp.float32) * q_width ** -0.5).astype(jnp.bfloat16),
        'q_norm': (1.0 + 0.4 * jax.random.normal(shared[5], (HEAD_DIM,), jnp.float32)).astype(jnp.bfloat16),
        'k_norm': (1.0 + 0.4 * jax.random.normal(shared[6], (HEAD_DIM,), jnp.float32)).astype(jnp.bfloat16),
    }


def reference(hidden, prefix_len, k_cache, v_cache, attn_norm, w_q, w_k, w_v, w_o, q_norm, k_norm):
    group_size = N_HEADS // KV_HEADS
    flat_rows = hidden.reshape(NUM_SEQ * NEW_TOKENS, D_MODEL)
    normed = rms_scale(flat_rows.astype(jnp.float32), attn_norm.astype(jnp.float32)).astype(jnp.bfloat16)
    q_lin = jnp.dot(normed, w_q, preferred_element_type=jnp.float32).astype(jnp.bfloat16)
    k_lin = jnp.dot(normed, w_k, preferred_element_type=jnp.float32).astype(jnp.bfloat16)
    v_lin = jnp.dot(normed, w_v, preferred_element_type=jnp.float32).astype(jnp.bfloat16)
    positions = prefix_len[:, None] + jnp.arange(NEW_TOKENS, dtype=jnp.int32)[None, :]
    q_heads = q_lin.reshape(NUM_SEQ, NEW_TOKENS, N_HEADS, HEAD_DIM).astype(jnp.float32)
    k_heads = k_lin.reshape(NUM_SEQ, NEW_TOKENS, KV_HEADS, HEAD_DIM).astype(jnp.float32)
    q_rot = rope_apply(rms_scale(q_heads, q_norm.astype(jnp.float32)), positions).astype(jnp.bfloat16)
    k_new = rope_apply(rms_scale(k_heads, k_norm.astype(jnp.float32)), positions).astype(jnp.bfloat16)
    v_new = v_lin.reshape(NUM_SEQ, NEW_TOKENS, KV_HEADS, HEAD_DIM)
    causal = jnp.arange(NEW_TOKENS)[:, None] >= jnp.arange(NEW_TOKENS)[None, :]
    score_scale = HEAD_DIM ** -0.5

    def one_sequence(operands):
        q_seq, k_seq, v_seq, kc_seq, vc_seq, seq_len = operands
        cache_ok = jnp.arange(CACHE_LEN) < seq_len
        key_mask = jnp.concatenate([jnp.broadcast_to(cache_ok[None, :], (NEW_TOKENS, CACHE_LEN)), causal], axis=1)

        def one_head_group(group_ops):
            q_grp, key_all, val_all = group_ops
            scores = jnp.einsum('cgd,kd->gck', q_grp.astype(jnp.float32), key_all.astype(jnp.float32)) * score_scale
            scores = jnp.where(key_mask[None], scores, -jnp.inf)
            prob_mat = jax.nn.softmax(scores, axis=-1)
            return jnp.einsum('gck,kd->cgd', prob_mat, val_all.astype(jnp.float32))

        key_all = jnp.concatenate([kc_seq, k_seq], axis=0).transpose(1, 0, 2)
        val_all = jnp.concatenate([vc_seq, v_seq], axis=0).transpose(1, 0, 2)
        q_grp = q_seq.reshape(NEW_TOKENS, KV_HEADS, group_size, HEAD_DIM).transpose(1, 0, 2, 3)
        out_grp = lax.map(one_head_group, (q_grp, key_all, val_all))
        return out_grp.transpose(1, 0, 2, 3).reshape(NEW_TOKENS, N_HEADS * HEAD_DIM)

    attn_seq = lax.map(one_sequence, (q_rot, k_new, v_new, k_cache, v_cache, prefix_len))
    attn_rows = attn_seq.reshape(NUM_SEQ * NEW_TOKENS, N_HEADS * HEAD_DIM).astype(jnp.bfloat16)
    block_out = flat_rows.astype(jnp.float32) + jnp.dot(attn_rows, w_o, preferred_element_type=jnp.float32)
    return block_out.astype(jnp.bfloat16).reshape(NUM_SEQ, NEW_TOKENS, D_MODEL), k_new, v_new
```

```python
import functools

import jax
import jax.numpy as jnp
from jax import lax
from jax.experimental import pallas as pl
from jax.experimental.pallas import tpu as pltpu
from jax.sharding import PartitionSpec as P

HEAD_DIM = 128
MASKED = -1e30
EXP2_SCALE = HEAD_DIM**-0.5 * 1.4426950408889634
STAT_ROWS = 264
MESH = pl.DeviceIdType.MESH


def project_kernel(
    x_hbm, gain, wq_hbm, wk_hbm, wv_hbm, q_gain, k_gain, cos_t, sin_t,
    q_out, k_out, v_out, x_buf, h_buf, w_buf, x_sem, w_sem,
):
    rows, d_model = x_buf.shape
    n_q = wq_hbm.shape[1] // 256
    x_copy = pltpu.make_async_copy(x_hbm, x_buf, x_sem)
    x_copy.start()
    w_copies = [
        pltpu.make_async_copy(wq_hbm.at[:, pl.ds(256 * i, 256)], w_buf.at[i], w_sem.at[i]) for i in range(n_q)
    ]
    w_copies.append(pltpu.make_async_copy(wk_hbm, w_buf.at[n_q], w_sem.at[n_q]))
    w_copies.append(pltpu.make_async_copy(wv_hbm, w_buf.at[n_q + 1], w_sem.at[n_q + 1]))
    for copy in w_copies:
        copy.start()
    x_copy.wait()

    def norm_rows(i, carry):
        sel = pl.ds(pl.multiple_of(i * 32, 32), 32)
        x = x_buf[sel, :].astype(jnp.float32)
        mean_sq = jnp.mean(x * x, axis=-1, keepdims=True)
        h_buf[sel, :] = (x * lax.rsqrt(mean_sq + 1e-6) * gain[...]).astype(jnp.bfloat16)
        return carry

    lax.fori_loop(0, rows // 32, norm_rows, 0)

    def head_rope(lin, head_gain):
        mean_sq = jnp.mean(lin * lin, axis=-1, keepdims=True)
        t = lin * lax.rsqrt(mean_sq + 1e-6) * head_gain
        return (t * cos_t[...] + pltpu.roll(t, 64, 1) * sin_t[...]).astype(jnp.bfloat16)

    for i in range(n_q + 2):
        w_copies[i].wait()
        lin = jnp.dot(h_buf[...], w_buf[i], preferred_element_type=jnp.float32).astype(jnp.bfloat16)
        if i == n_q + 1:
            v_out[...] = lin
            continue
        head_gain = q_gain[...] if i < n_q else k_gain[...]
        lin = lin.astype(jnp.float32)
        for u in range(2):
            res = head_rope(lin[:, 128 * u : 128 * u + 128], head_gain)
            if i < n_q:
                q_out[:, 256 * i + 128 * u : 256 * i + 128 * u + 128] = res
            else:
                k_out[:, 128 * u : 128 * u + 128] = res


def project(x2, gain, w_q, w_k, w_v, q_gain, k_gain, cos_t, sin_t):
    rows, d_model = x2.shape
    n_tiles = w_q.shape[1] // 256 + 2
    any_spec = pl.BlockSpec(memory_space=pl.ANY)
    vmem = pl.BlockSpec(memory_space=pltpu.VMEM)
    return pl.pallas_call(
        project_kernel,
        out_shape=(
            jax.ShapeDtypeStruct((rows, w_q.shape[1]), jnp.bfloat16),
            jax.ShapeDtypeStruct((rows, 256), jnp.bfloat16),
            jax.ShapeDtypeStruct((rows, 256), jnp.bfloat16),
        ),
        in_specs=[any_spec, vmem, any_spec, any_spec, any_spec, vmem, vmem, vmem, vmem],
        out_specs=(vmem, vmem, vmem),
        scratch_shapes=[
            pltpu.VMEM((rows, d_model), jnp.bfloat16),
            pltpu.VMEM((rows, d_model), jnp.bfloat16),
            pltpu.VMEM((n_tiles, d_model, 256), jnp.bfloat16),
            pltpu.SemaphoreType.DMA,
            pltpu.SemaphoreType.DMA((n_tiles,)),
        ],
        compiler_params=pltpu.CompilerParams(vmem_limit_bytes=56 * 1024 * 1024),
        cost_estimate=pl.CostEstimate(flops=2 * rows * d_model * 256 * n_tiles, bytes_accessed=20 << 20, transcendentals=0),
        name="project",
    )(x2, gain, w_q, w_k, w_v, q_gain, k_gain, cos_t, sin_t)


def attend_kernel(
    nv_ref, q_ref, k_ref, v_ref, kn_ref, vn_ref, o_ref, qt_ref, s_ref, sn_ref, acc_ref, *, tile,
):
    b = pl.program_id(0)
    n_rows = 2 * nv_ref[b]
    has_new = nv_ref[pl.num_programs(0)]
    n_new = kn_ref.shape[1]
    n_tiles = (n_rows + tile - 1) // tile
    q = q_ref[...]
    for h in range(2):
        blocks = [
            q[th * 32 : th * 32 + 32, (h * 4 + g) * 128 : (h * 4 + g) * 128 + 128]
            for th in range(2)
            for g in range(4)
        ]
        qt_ref[h * 128 : h * 128 + 128, :] = jnp.concatenate(blocks, axis=0).T
    sub16 = lax.broadcasted_iota(jnp.int32, (16, 128), 0) & 1
    even_rows = jnp.where(sub16 == 0, 1.0, 0.0).astype(jnp.bfloat16)
    odd_rows = jnp.where(sub16 == 0, 0.0, 1.0).astype(jnp.bfloat16)
    sub8 = lax.broadcasted_iota(jnp.int32, (8, 256), 0) & 1

    def split_rows(k):
        n = k.shape[0]
        k3 = k.reshape(n // 16, 16, 128)
        return jnp.concatenate(
            [(k3 * even_rows[None]).reshape(n, 128), (k3 * odd_rows[None]).reshape(n, 128)], axis=1
        )

    def split_lanes(v):
        n = v.shape[0]
        lane = lax.broadcasted_iota(jnp.int32, (16, n), 1) & 1
        even = jnp.where(lane == 0, 1.0, 0.0).astype(jnp.bfloat16)
        odd = jnp.where(lane == 0, 0.0, 1.0).astype(jnp.bfloat16)
        vt = v.T.reshape(8, 16, n)
        return jnp.concatenate([(vt * even[None]).reshape(128, n), (vt * odd[None]).reshape(128, n)], axis=0)

    def scores(k):
        return jnp.dot(split_rows(k), qt_ref[...], preferred_element_type=jnp.float32)

    def score_tile(t, top):
        sel = pl.ds(pl.multiple_of(t * tile, tile), tile)
        s = scores(k_ref[0, sel, :])
        row = t * tile + lax.broadcasted_iota(jnp.int32, (tile, 256), 0)
        s = jnp.where(row < n_rows, s, MASKED)
        s_ref[sel, :] = s
        return jnp.maximum(top, jnp.max(s.reshape(tile // 8, 8, 256), axis=0))

    top = lax.fori_loop(0, n_tiles, score_tile, jnp.full((8, 256), MASKED, jnp.float32))

    key = lax.broadcasted_iota(jnp.int32, (n_new, 256), 0) // 2
    col = lax.broadcasted_iota(jnp.int32, (n_new, 256), 1)
    token = (col // 128) * 32 + (col % 32)
    s_new = jnp.where((key <= token) & (has_new > 0), scores(kn_ref[0]), MASKED)
    sn_ref[...] = s_new
    top = jnp.maximum(top, jnp.max(s_new.reshape(n_new // 8, 8, 256), axis=0))
    top0 = jnp.max(jnp.where(sub8 == 0, top, MASKED), axis=0, keepdims=True)
    top1 = jnp.max(jnp.where(sub8 == 0, MASKED, top), axis=0, keepdims=True)
    top = jnp.where(sub8 == 0, top0, top1)

    def weigh(s, v, keep):
        n = s.shape[0]
        p = jnp.exp2((s.reshape(n // 8, 8, 256) - top[None]) * EXP2_SCALE)
        if keep is not None:
            p = jnp.where(keep, p, 0.0)
        total = jnp.sum(p, axis=0)
        out = jnp.dot(split_lanes(v), p.reshape(n, 256).astype(jnp.bfloat16), preferred_element_type=jnp.float32)
        return total, out

    total, out = weigh(sn_ref[...], vn_ref[0], has_new > 0)
    acc_ref[...] = out

    def weigh_tile(t, total):
        sel = pl.ds(pl.multiple_of(t * tile, tile), tile)
        more, out = weigh(s_ref[sel, :], v_ref[0, sel, :], None)
        acc_ref[...] += out
        return total + more

    total = lax.fori_loop(0, n_tiles, weigh_tile, total)
    sum0 = jnp.sum(jnp.where(sub8 == 0, total, 0.0), axis=0, keepdims=True)
    sum1 = jnp.sum(jnp.where(sub8 == 0, 0.0, total), axis=0, keepdims=True)
    stats = jnp.concatenate([top0, top1, sum0, sum1, jnp.zeros((4, 256), jnp.float32)], axis=0)
    for th in range(2):
        o_ref[0, th, 0:256, :] = acc_ref[:, th * 128 : th * 128 + 128]
        o_ref[0, th, 256:264, :] = stats[:, th * 128 : th * 128 + 128]


def attend(n_valid, q2, kc, vc, kn, vn):
    n_seq, cache_rows, _ = kc.shape
    new_rows = kn.shape[1]
    tile = min(2048, cache_rows)
    return pl.pallas_call(
        functools.partial(attend_kernel, tile=tile),
        out_shape=jax.ShapeDtypeStruct((n_seq, 2, STAT_ROWS, 128), jnp.float32),
        grid_spec=pltpu.PrefetchScalarGridSpec(
            num_scalar_prefetch=1,
            grid=(n_seq,),
            in_specs=[
                pl.BlockSpec((q2.shape[0] // n_seq, q2.shape[1]), lambda b, nv: (b, 0)),
                pl.BlockSpec((1, cache_rows, 128), lambda b, nv: (b, 0, 0)),
                pl.BlockSpec((1, cache_rows, 128), lambda b, nv: (b, 0, 0)),
                pl.BlockSpec((1, new_rows, 128), lambda b, nv: (b, 0, 0)),
                pl.BlockSpec((1, new_rows, 128), lambda b, nv: (b, 0, 0)),
            ],
            out_specs=pl.BlockSpec((1, 2, STAT_ROWS, 128), lambda b, nv: (b, 0, 0, 0)),
            scratch_shapes=[
                pltpu.VMEM((256, 256), jnp.bfloat16),
                pltpu.VMEM((cache_rows, 256), jnp.float32),
                pltpu.VMEM((new_rows, 256), jnp.float32),
                pltpu.VMEM((256, 256), jnp.float32),
            ],
        ),
        compiler_params=pltpu.CompilerParams(
            vmem_limit_bytes=56 * 1024 * 1024, dimension_semantics=("arbitrary",)
        ),
        cost_estimate=pl.CostEstimate(
            flops=4 * n_seq * cache_rows * 256 * 256, bytes_accessed=40 << 20, transcendentals=n_seq * cache_rows * 256
        ),
        name="attend",
    )(n_valid, q2, kc, vc, kn, vn)


def finish_kernel(
    part, x_hbm, wo_hbm, out_hbm,
    wo, xs, got1, chip, got2, prod, from_l, from_r, full, stage,
    wo_sem, xs_sem, out_sem, a1s, a1r, a2s, a2r, brs, brr, bls, blr, crs, crr, cls, clr, cys, cyr, cps, cpr,
):
    dp, z, c = lax.axis_index("dp"), lax.axis_index("tp"), lax.axis_index("cp")
    y, core = c // 2, c % 2
    mate = 2 * y + (1 - core)
    over = 2 * (1 - y) + core
    over_mate = 2 * (1 - y) + (1 - core)
    n_chunks, n_part = full.shape[0], full.shape[2]
    width = full.shape[4]
    last = n_part - 1

    def send(src, dst, send_sem, recv_sem, tp, cp):
        copy = pltpu.make_async_remote_copy(
            src_ref=src, dst_ref=dst, send_sem=send_sem, recv_sem=recv_sem, device_id=(dp, tp, cp), device_id_type=MESH
        )
        return copy

    wo_copy = pltpu.make_async_copy(wo_hbm, wo, wo_sem)
    wo_copy.start()
    x_copies = [
        pltpu.make_async_copy(
            x_hbm.at[pl.ds(pl.multiple_of(128 * j + 32 * c, 32), 32), pl.ds(pl.multiple_of(width * z, width), width)],
            xs.at[j],
            xs_sem.at[j],
        )
        for j in range(n_chunks)
    ]
    for copy in x_copies:
        copy.start()

    barrier = pltpu.get_barrier_semaphore()
    for peer in (mate, over):
        pl.semaphore_signal(barrier, inc=1, device_id=(dp, z, peer), device_id_type=MESH)

    @pl.when(z > 0)
    def _():
        pl.semaphore_signal(barrier, inc=1, device_id=(dp, z - 1, c), device_id_type=MESH)

    @pl.when(z < last)
    def _():
        pl.semaphore_signal(barrier, inc=1, device_id=(dp, z + 1, c), device_id_type=MESH)

    @pl.when((z == 0) | (z == last))
    def _():
        pl.semaphore_wait(barrier, 3)

    @pl.when((z > 0) & (z < last))
    def _():
        pl.semaphore_wait(barrier, 4)

    def a1(j):
        return send(part.at[pl.ds(2 * j, 2), 1 - core], got1.at[j], a1s.at[j], a1r.at[j], z, mate)

    def a2(j):
        return send(chip.at[j, 1 - y], got2.at[j], a2s.at[j], a2r.at[j], z, over)

    def b_right(j, p):
        return send(prod.at[j, p], from_l.at[j, p], brs.at[j, p], brr.at[j, p], z + 1, c)

    def b_left(j, p):
        return send(prod.at[j, p], from_r.at[j, p], bls.at[j, p], blr.at[j, p], z - 1, c)

    def c_right(j, p):
        return send(full.at[j, c, p], full.at[j, c, p], crs.at[j, p], crr.at[j, p], z + 1, c)

    def c_left(j, p):
        return send(full.at[j, c, p], full.at[j, c, p], cls.at[j, p], clr.at[j, p], z - 1, c)

    def c_over(j, p):
        return send(full.at[j, c, p], full.at[j, c, p], cys.at[j, p], cyr.at[j, p], z, over)

    def c_over_in(j, p):
        return send(full.at[j, over, p], full.at[j, over, p], cys.at[j, p], cyr.at[j, p], z, over)

    def c_mate(j, q, u, p):
        return send(full.at[j, q, p], full.at[j, q, p], cps.at[j, u, p], cpr.at[j, u, p], z, mate)

    def merge(a, b):
        top_a, top_b = a[256:258], b[256:258]
        top = jnp.maximum(top_a, top_b)
        fa = jnp.exp2((top_a - top) * EXP2_SCALE)
        fb = jnp.exp2((top_b - top) * EXP2_SCALE)
        vals = [
            a[128 * h : 128 * h + 128] * fa[h : h + 1] + b[128 * h : 128 * h + 128] * fb[h : h + 1] for h in range(2)
        ]
        return vals, top, a[258:260] * fa + b[258:260] * fb

    for j in range(n_chunks):
        a1(j).start()

    def stage_a1(j):
        a1(j).wait_recv()
        for s in range(2):
            vals, top, total = merge(part[2 * j + s, core], got1[j, s])
            chip[j, s, 0:128] = vals[0]
            chip[j, s, 128:256] = vals[1]
            chip[j, s, 256:264] = jnp.concatenate([top, total, jnp.zeros((4, 128), jnp.float32)], axis=0)
        a2(j).start()

    def stage_a2(j):
        a2(j).wait_recv()
        vals, _, total = merge(chip[j, y], got2[j])
        turned = [(vals[h] / total[h : h + 1]).T for h in range(2)]
        o = jnp.concatenate([turned[h][32 * g : 32 * g + 32] for h in range(2) for g in range(4)], axis=1)
        o = o.astype(jnp.bfloat16)
        if j == 0:
            wo_copy.wait()

        def one_part(p, carry):
            prod[j, p] = jnp.dot(
                o, wo[:, pl.ds(pl.multiple_of(p * width, width), width)], preferred_element_type=jnp.float32
            )
            return carry

        lax.fori_loop(0, n_part, one_part, 0)

        @pl.when(z == 0)
        def _():
            for p in range(last, 0, -1):
                b_right(j, p).start()

        @pl.when(z == last)
        def _():
            for p in range(last):
                b_left(j, p).start()

    def pass_right(j, p):
        b_right(j, p).wait_recv()
        prod[j, p] = prod[j, p] + from_l[j, p]
        b_right(j, p).start()

    def pass_left(j, p):
        b_left(j, p).wait_recv()
        prod[j, p] = prod[j, p] + from_r[j, p]
        b_left(j, p).start()

    def stage_b1(j):
        @pl.when(z == 1)
        def _():
            pass_right(j, 3)
            pass_right(j, 2)

        @pl.when(z == 2)
        def _():
            pass_left(j, 0)
            pass_left(j, 1)

    def stage_b2(j):
        @pl.when(z == 2)
        def _():
            pass_right(j, 3)

        @pl.when(z == 1)
        def _():
            pass_left(j, 0)

    def stage_c0(j):
        x_copies[j].wait()

        @pl.when(z > 0)
        def _():
            b_right(j, z).wait_recv()
            prod[j, z] = prod[j, z] + from_l[j, z]

        @pl.when(z < last)
        def _():
            b_left(j, z).wait_recv()
            prod[j, z] = prod[j, z] + from_r[j, z]

        full[j, c, z] = prod[j, z] + xs[j].astype(jnp.float32)

        @pl.when(z < last)
        def _():
            c_right(j, z).start()

        @pl.when(z > 0)
        def _():
            c_left(j, z).start()

        c_over(j, z).start()
        c_mate(j, c, 0, z).start()

    def stage_c(j, d):
        @pl.when(z - d >= 0)
        def _():
            p = z - d
            c_right(j, p).wait_recv()

            @pl.when(z < last)
            def _():
                c_right(j, p).start()

            c_over(j, p).start()
            c_mate(j, c, 0, p).start()

        @pl.when(z + d <= last)
        def _():
            p = z + d
            c_left(j, p).wait_recv()

            @pl.when(z > 0)
            def _():
                c_left(j, p).start()

            c_over(j, p).start()
            c_mate(j, c, 0, p).start()

    def stage_over(j):
        for p in range(n_part):
            c_over_in(j, p).wait_recv()
            c_mate(j, over, 1, p).start()

    def out_copy(j):
        return pltpu.make_async_copy(stage.at[j], out_hbm.at[pl.ds(128 * j, 128)], out_sem.at[j])

    def stage_out(j):
        for p in range(n_part):
            c_mate(j, mate, 0, p).wait_recv()
            c_mate(j, over_mate, 1, p).wait_recv()
        for q in range(4):
            for p in range(n_part):
                stage[j, 32 * q : 32 * q + 32, width * p : width * p + width] = full[j, q, p].astype(jnp.bfloat16)
        out_copy(j).start()

    stages = [
        stage_a1, stage_a2, stage_b1, stage_b2, stage_c0,
        functools.partial(stage_c, d=1), functools.partial(stage_c, d=2), functools.partial(stage_c, d=3),
        stage_over, stage_out,
    ]
    for r in range(n_chunks + len(stages) - 1):
        for i, stage_fn in enumerate(stages):
            if 0 <= r - i < n_chunks:
                stage_fn(r - i)

    for j in range(n_chunks):
        a1(j).wait_send()
        a2(j).wait_send()
        for p in range(n_part):
            @pl.when(z < p)
            def _():
                b_right(j, p).wait_send()

            @pl.when(z > p)
            def _():
                b_left(j, p).wait_send()

            @pl.when((z >= p) & (z < last))
            def _():
                c_right(j, p).wait_send()

            @pl.when((z <= p) & (z > 0))
            def _():
                c_left(j, p).wait_send()

            c_over(j, p).wait_send()
            c_mate(j, c, 0, p).wait_send()
            c_mate(j, over, 1, p).wait_send()
        out_copy(j).wait()


def finish(part, x2, w_o):
    rows, d_model = x2.shape
    n_chunks, n_part = rows // 128, 4
    width = d_model // n_part
    any_spec = pl.BlockSpec(memory_space=pl.ANY)
    piece = (32, width)
    f32 = jnp.float32
    sems = pltpu.SemaphoreType.DMA
    per_part = [sems((n_chunks, n_part))] * 10
    return pl.pallas_call(
        finish_kernel,
        out_shape=jax.ShapeDtypeStruct((rows, d_model), jnp.bfloat16),
        in_specs=[pl.BlockSpec(memory_space=pltpu.VMEM), any_spec, any_spec],
        out_specs=any_spec,
        scratch_shapes=[
            pltpu.VMEM(w_o.shape, jnp.bfloat16),
            pltpu.VMEM((n_chunks, *piece), jnp.bfloat16),
            pltpu.VMEM((n_chunks, 2, STAT_ROWS, 128), f32),
            pltpu.VMEM((n_chunks, 2, STAT_ROWS, 128), f32),
            pltpu.VMEM((n_chunks, STAT_ROWS, 128), f32),
            pltpu.VMEM((n_chunks, n_part, *piece), f32),
            pltpu.VMEM((n_chunks, n_part, *piece), f32),
            pltpu.VMEM((n_chunks, n_part, *piece), f32),
            pltpu.VMEM((n_chunks, 4, n_part, *piece), f32),
            pltpu.VMEM((n_chunks, 128, d_model), jnp.bfloat16),
            sems,
            sems((n_chunks,)),
            sems((n_chunks,)),
            *[sems((n_chunks,))] * 4,
            *per_part,
            sems((n_chunks, 2, n_part)),
            sems((n_chunks, 2, n_part)),
        ],
        compiler_params=pltpu.CompilerParams(
            collective_id=0, has_side_effects=True, vmem_limit_bytes=56 * 1024 * 1024
        ),
        cost_estimate=pl.CostEstimate(flops=2 * 128 * 1024 * 4096, bytes_accessed=16 << 20, transcendentals=0),
        name="finish",
    )(part, x2, w_o)


def rope_tables(positions):
    half_dim = HEAD_DIM // 2
    inv_freq = 1.0 / (1000000.0 ** (jnp.arange(half_dim, dtype=jnp.float32) * 2.0 / HEAD_DIM))
    angles = positions.astype(jnp.float32)[..., None] * inv_freq
    cos_t, sin_t = jnp.cos(angles), jnp.sin(angles)
    return jnp.concatenate([cos_t, cos_t], axis=-1), jnp.concatenate([-sin_t, sin_t], axis=-1)


def solution(mesh):
    n_cp = mesh.shape["cp"]

    def per_device(hidden, prefix_len, k_cache, v_cache, attn_norm, w_q, w_k, w_v, w_o, q_norm, k_norm):
        n_seq, n_new, d_model = hidden.shape
        slots = k_cache.shape[1]
        cp_index = lax.axis_index("cp")
        x2 = hidden.reshape(n_seq * n_new, d_model)
        positions = prefix_len[:, None] + jnp.arange(n_new, dtype=jnp.int32)[None, :]
        cos_t, sin_t = rope_tables(positions.reshape(-1))
        q2, k2, v2 = project(
            x2, attn_norm.astype(jnp.float32)[None], w_q, w_k, w_v,
            q_norm.astype(jnp.float32)[None], k_norm.astype(jnp.float32)[None], cos_t, sin_t,
        )
        k_new = k2.reshape(n_seq, n_new, 2, HEAD_DIM)
        v_new = v2.reshape(n_seq, n_new, 2, HEAD_DIM)
        n_valid = jnp.clip(prefix_len - cp_index * slots, 0, slots)
        n_valid = jnp.concatenate([n_valid, (cp_index == n_cp - 1).astype(jnp.int32)[None]])
        part = attend(
            n_valid, q2,
            k_cache.reshape(n_seq, slots * 2, HEAD_DIM), v_cache.reshape(n_seq, slots * 2, HEAD_DIM),
            k_new.reshape(n_seq, n_new * 2, HEAD_DIM), v_new.reshape(n_seq, n_new * 2, HEAD_DIM),
        )
        out = finish(part, x2, w_o)
        return out.reshape(hidden.shape), k_new, v_new

    cache_spec = P("dp", "cp", "tp", None)
    arg_specs = (P("dp", None, None), P("dp"), cache_spec, cache_spec, P(None), P(None, "tp"), P(None, "tp"), P(None, "tp"), P("tp", None), P(None), P(None))
    out_specs = (P("dp", None, None), P("dp", None, "tp", None), P("dp", None, "tp", None))
    return jax.shard_map(per_device, mesh=mesh, in_specs=arg_specs, out_specs=out_specs, check_vma=False)
```

```python
import functools

import jax
import jax.numpy as jnp
import numpy as np
from jax import lax
from jax.experimental import pallas as pl
from jax.experimental.pallas import tpu as pltpu
from jax.sharding import PartitionSpec as P

HEAD_DIM = 128
MASKED = -1e30
EXP2_SCALE = HEAD_DIM**-0.5 * 1.4426950408889634
STAT_ROWS = 264
MESH = pl.DeviceIdType.MESH


def project_kernel(
    len_ref, x_hbm, gain, wq_hbm, wk_hbm, wv_hbm, q_gain, k_gain, freq,
    q_out, k_out, v_out, x_buf, h_buf, w_buf, cos_t, sin_t, turn, x_sem, w_sem,
):
    rows, d_model = x_buf.shape
    n_q = wq_hbm.shape[1] // 256
    n_seq = len_ref.shape[0]
    n_new = rows // n_seq
    piece = rows // 4
    x_copies = [
        pltpu.make_async_copy(x_hbm.at[pl.ds(piece * i, piece)], x_buf.at[pl.ds(piece * i, piece)], x_sem.at[i])
        for i in range(4)
    ]
    for copy in x_copies:
        copy.start()
    w_copies = [
        pltpu.make_async_copy(wq_hbm.at[:, pl.ds(256 * i, 256)], w_buf.at[i], w_sem.at[i]) for i in range(n_q)
    ]
    w_copies.append(pltpu.make_async_copy(wk_hbm, w_buf.at[n_q], w_sem.at[n_q]))
    w_copies.append(pltpu.make_async_copy(wv_hbm, w_buf.at[n_q + 1], w_sem.at[n_q + 1]))

    lane = lax.broadcasted_iota(jnp.int32, (n_new, 128), 1)
    token = lax.broadcasted_iota(jnp.int32, (n_new, 128), 0)

    def rope_rows(b, carry):
        angle = (token + len_ref[b]).astype(jnp.float32) * freq[...]
        sel = pl.ds(pl.multiple_of(b * n_new, n_new), n_new)
        cos_t[sel, :] = jnp.cos(angle)
        sin = jnp.sin(angle)
        sin_t[sel, :] = jnp.where(lane < 64, -sin, sin)
        return carry

    lax.fori_loop(0, n_seq, rope_rows, 0)
    x_gain = gain[...].astype(jnp.float32).reshape(1, d_model)

    def norm_rows(i, carry):
        sel = pl.ds(pl.multiple_of(i * 32, 32), 32)
        x = x_buf[sel, :].astype(jnp.float32)
        mean_sq = jnp.mean(x * x, axis=-1, keepdims=True)
        h_buf[sel, :] = (x * lax.rsqrt(mean_sq + 1e-6) * x_gain).astype(jnp.bfloat16)
        return carry

    for i in range(4):
        x_copies[i].wait()
        if i == 0:
            for copy in w_copies:
                copy.start()
    lax.fori_loop(0, rows // 32, norm_rows, 0)
    q_gain_row = q_gain[...].astype(jnp.float32).reshape(1, 128)
    k_gain_row = k_gain[...].astype(jnp.float32).reshape(1, 128)

    def one_tile(i, carry):
        pltpu.make_async_copy(w_buf.at[i], w_buf.at[i], w_sem.at[i]).wait()
        lin = jnp.dot(h_buf[...], w_buf[i], preferred_element_type=jnp.float32).astype(jnp.bfloat16)
        lin = lin.astype(jnp.float32)
        head_gain = jnp.where(i < n_q, q_gain_row, k_gain_row)
        for u in range(2):
            raw = lin[:, 128 * u : 128 * u + 128]
            mean_sq = jnp.mean(raw * raw, axis=-1, keepdims=True)
            t = raw * lax.rsqrt(mean_sq + 1e-6) * head_gain
            t = t * cos_t[...] + pltpu.roll(t, 64, 1) * sin_t[...]

            @pl.when(i < n_q)
            def _():
                q_out[i, :, 128 * u : 128 * u + 128] = t.astype(jnp.bfloat16)

            @pl.when(i >= n_q)
            def _():
                turn[pl.ds(u, rows, stride=2), :] = jnp.where(i == n_q, t, raw)

        @pl.when(i == n_q)
        def _():
            k_out[...] = turn[...].astype(jnp.bfloat16)

        @pl.when(i == n_q + 1)
        def _():
            v_out[...] = turn[...].astype(jnp.bfloat16)

        return carry

    lax.fori_loop(0, n_q + 2, one_tile, 0)


def project(prefix_len, x2, gain, w_q, w_k, w_v, q_gain, k_gain):
    rows, d_model = x2.shape
    n_q = w_q.shape[1] // 256
    half_dim = HEAD_DIM // 2
    freq = 1.0 / (1000000.0 ** (np.arange(half_dim, dtype=np.float64) * 2.0 / HEAD_DIM))
    freq = jnp.asarray(np.concatenate([freq, freq])[None], jnp.float32)
    any_spec = pl.BlockSpec(memory_space=pl.ANY)
    vmem = pl.BlockSpec(memory_space=pltpu.VMEM)
    return pl.pallas_call(
        project_kernel,
        out_shape=(
            jax.ShapeDtypeStruct((n_q, rows, 256), jnp.bfloat16),
            jax.ShapeDtypeStruct((2 * rows, 128), jnp.bfloat16),
            jax.ShapeDtypeStruct((2 * rows, 128), jnp.bfloat16),
        ),
        in_specs=[pl.BlockSpec(memory_space=pltpu.SMEM), any_spec, vmem, any_spec, any_spec, any_spec, vmem, vmem, vmem],
        out_specs=(vmem, vmem, vmem),
        scratch_shapes=[
            pltpu.VMEM((rows, d_model), jnp.bfloat16),
            pltpu.VMEM((rows, d_model), jnp.bfloat16),
            pltpu.VMEM((n_q + 2, d_model, 256), jnp.bfloat16),
            pltpu.VMEM((rows, 128), jnp.float32),
            pltpu.VMEM((rows, 128), jnp.float32),
            pltpu.VMEM((2 * rows, 128), jnp.float32),
            pltpu.SemaphoreType.DMA((4,)),
            pltpu.SemaphoreType.DMA((n_q + 2,)),
        ],
        compiler_params=pltpu.CompilerParams(vmem_limit_bytes=56 * 1024 * 1024),
        cost_estimate=pl.CostEstimate(
            flops=2 * rows * d_model * 256 * (n_q + 2), bytes_accessed=20 << 20, transcendentals=0
        ),
        name="project",
    )(prefix_len, x2, gain, w_q, w_k, w_v, q_gain, k_gain, freq)


def attend_kernel(
    len_ref, q_ref, k_ref, v_ref, kn_ref, vn_ref, o_ref, qt_ref, s_ref, sn_ref, acc_ref, *, tile, n_cp,
):
    b = pl.program_id(0)
    cp = lax.axis_index("cp")
    slots = k_ref.shape[1] // 2
    n_rows = 2 * jnp.clip(len_ref[b] - cp * slots, 0, slots)
    has_new = cp == n_cp - 1
    n_new = kn_ref.shape[0]
    n_tiles = (n_rows + tile - 1) // tile
    for h in range(2):
        blocks = [
            q_ref[h * 2 + g // 2, th * 32 : th * 32 + 32, (g % 2) * 128 : (g % 2) * 128 + 128]
            for th in range(2)
            for g in range(4)
        ]
        qt_ref[h * 128 : h * 128 + 128, :] = jnp.concatenate(blocks, axis=0).T
    sub16 = lax.broadcasted_iota(jnp.int32, (16, 128), 0) & 1
    even_rows = jnp.where(sub16 == 0, 1.0, 0.0).astype(jnp.bfloat16)
    odd_rows = jnp.where(sub16 == 0, 0.0, 1.0).astype(jnp.bfloat16)
    sub8 = lax.broadcasted_iota(jnp.int32, (8, 256), 0) & 1

    def split_rows(k):
        n = k.shape[0]
        k3 = k.reshape(n // 16, 16, 128)
        return jnp.concatenate(
            [(k3 * even_rows[None]).reshape(n, 128), (k3 * odd_rows[None]).reshape(n, 128)], axis=1
        )

    def split_lanes(v):
        n = v.shape[0]
        lane = lax.broadcasted_iota(jnp.int32, (16, n), 1) & 1
        even = jnp.where(lane == 0, 1.0, 0.0).astype(jnp.bfloat16)
        odd = jnp.where(lane == 0, 0.0, 1.0).astype(jnp.bfloat16)
        vt = v.T.reshape(8, 16, n)
        return jnp.concatenate([(vt * even[None]).reshape(128, n), (vt * odd[None]).reshape(128, n)], axis=0)

    def scores(k):
        return jnp.dot(split_rows(k), qt_ref[...], preferred_element_type=jnp.float32)

    def score_tile(t, top):
        sel = pl.ds(pl.multiple_of(t * tile, tile), tile)
        s = scores(k_ref[0, sel, :])
        row = t * tile + lax.broadcasted_iota(jnp.int32, (tile, 256), 0)
        s = jnp.where(row < n_rows, s, MASKED)
        s_ref[sel, :] = s
        return jnp.maximum(top, jnp.max(s.reshape(tile // 8, 8, 256), axis=0))

    top = lax.fori_loop(0, n_tiles, score_tile, jnp.full((8, 256), MASKED, jnp.float32))

    key = lax.broadcasted_iota(jnp.int32, (n_new, 256), 0) // 2
    col = lax.broadcasted_iota(jnp.int32, (n_new, 256), 1)
    token = (col // 128) * 32 + (col % 32)
    s_new = jnp.where((key <= token) & has_new, scores(kn_ref[...]), MASKED)
    sn_ref[...] = s_new
    top = jnp.maximum(top, jnp.max(s_new.reshape(n_new // 8, 8, 256), axis=0))
    top0 = jnp.max(jnp.where(sub8 == 0, top, MASKED), axis=0, keepdims=True)
    top1 = jnp.max(jnp.where(sub8 == 0, MASKED, top), axis=0, keepdims=True)
    top = jnp.where(sub8 == 0, top0, top1)

    def weigh(s, v, keep):
        n = s.shape[0]
        p = jnp.exp2((s.reshape(n // 8, 8, 256) - top[None]) * EXP2_SCALE)
        if keep is not None:
            p = jnp.where(keep, p, 0.0)
        total = jnp.sum(p, axis=0)
        out = jnp.dot(split_lanes(v), p.reshape(n, 256).astype(jnp.bfloat16), preferred_element_type=jnp.float32)
        return total, out

    total, out = weigh(sn_ref[...], vn_ref[...], has_new)
    acc_ref[...] = out

    def weigh_tile(t, total):
        sel = pl.ds(pl.multiple_of(t * tile, tile), tile)
        more, out = weigh(s_ref[sel, :], v_ref[0, sel, :], None)
        acc_ref[...] += out
        return total + more

    total = lax.fori_loop(0, n_tiles, weigh_tile, total)
    sum0 = jnp.sum(jnp.where(sub8 == 0, total, 0.0), axis=0, keepdims=True)
    sum1 = jnp.sum(jnp.where(sub8 == 0, 0.0, total), axis=0, keepdims=True)
    stats = jnp.concatenate([top0, top1, sum0, sum1, jnp.zeros((4, 256), jnp.float32)], axis=0)
    for th in range(2):
        o_ref[0, th, 0:256, :] = acc_ref[:, th * 128 : th * 128 + 128]
        o_ref[0, th, 256:264, :] = stats[:, th * 128 : th * 128 + 128]


def attend(prefix_len, q3, kc, vc, kn, vn, n_cp):
    n_seq, cache_rows, _ = kc.shape
    new_rows = kn.shape[0] // n_seq
    tile = min(2048, cache_rows)
    return pl.pallas_call(
        functools.partial(attend_kernel, tile=tile, n_cp=n_cp),
        out_shape=jax.ShapeDtypeStruct((n_seq, 2, STAT_ROWS, 128), jnp.float32),
        grid_spec=pltpu.PrefetchScalarGridSpec(
            num_scalar_prefetch=1,
            grid=(n_seq,),
            in_specs=[
                pl.BlockSpec((q3.shape[0], q3.shape[1] // n_seq, 256), lambda b, nv: (0, b, 0)),
                pl.BlockSpec((1, cache_rows, 128), lambda b, nv: (b, 0, 0)),
                pl.BlockSpec((1, cache_rows, 128), lambda b, nv: (b, 0, 0)),
                pl.BlockSpec((new_rows, 128), lambda b, nv: (b, 0)),
                pl.BlockSpec((new_rows, 128), lambda b, nv: (b, 0)),
            ],
            out_specs=pl.BlockSpec((1, 2, STAT_ROWS, 128), lambda b, nv: (b, 0, 0, 0)),
            scratch_shapes=[
                pltpu.VMEM((256, 256), jnp.bfloat16),
                pltpu.VMEM((cache_rows, 256), jnp.float32),
                pltpu.VMEM((new_rows, 256), jnp.float32),
                pltpu.VMEM((256, 256), jnp.float32),
            ],
        ),
        compiler_params=pltpu.CompilerParams(
            vmem_limit_bytes=56 * 1024 * 1024, dimension_semantics=("arbitrary",)
        ),
        cost_estimate=pl.CostEstimate(
            flops=4 * n_seq * cache_rows * 256 * 256, bytes_accessed=40 << 20, transcendentals=n_seq * cache_rows * 256
        ),
        name="attend",
    )(prefix_len, q3, kc, vc, kn, vn)


def finish_kernel(
    part, x_hbm, wo_hbm, out_hbm,
    wo, xs, got1, chip, got2, prod, from_l, from_r, full, stage,
    wo_sem, xs_sem, out_sem, a1s, a1r, a2s, a2r, brs, brr, bls, blr, crs, crr, cls, clr, cys, cyr, cps, cpr,
):
    dp, z, c = lax.axis_index("dp"), lax.axis_index("tp"), lax.axis_index("cp")
    y, core = c // 2, c % 2
    mate = 2 * y + (1 - core)
    over = 2 * (1 - y) + core
    over_mate = 2 * (1 - y) + (1 - core)
    n_chunks, n_part = full.shape[0], full.shape[2]
    width = full.shape[4]
    last = n_part - 1

    def send(src, dst, send_sem, recv_sem, tp, cp):
        copy = pltpu.make_async_remote_copy(
            src_ref=src, dst_ref=dst, send_sem=send_sem, recv_sem=recv_sem, device_id=(dp, tp, cp), device_id_type=MESH
        )
        return copy

    wo_copy = pltpu.make_async_copy(wo_hbm, wo, wo_sem)
    wo_copy.start()
    x_copies = [
        pltpu.make_async_copy(
            x_hbm.at[pl.ds(pl.multiple_of(128 * j + 32 * c, 32), 32), pl.ds(pl.multiple_of(width * z, width), width)],
            xs.at[j],
            xs_sem.at[j],
        )
        for j in range(n_chunks)
    ]
    for copy in x_copies:
        copy.start()

    barrier = pltpu.get_barrier_semaphore()
    for peer in (mate, over):
        pl.semaphore_signal(barrier, inc=1, device_id=(dp, z, peer), device_id_type=MESH)

    @pl.when(z > 0)
    def _():
        pl.semaphore_signal(barrier, inc=1, device_id=(dp, z - 1, c), device_id_type=MESH)

    @pl.when(z < last)
    def _():
        pl.semaphore_signal(barrier, inc=1, device_id=(dp, z + 1, c), device_id_type=MESH)

    @pl.when((z == 0) | (z == last))
    def _():
        pl.semaphore_wait(barrier, 3)

    @pl.when((z > 0) & (z < last))
    def _():
        pl.semaphore_wait(barrier, 4)

    def a1(j):
        return send(part.at[pl.ds(2 * j, 2), 1 - core], got1.at[j], a1s.at[j], a1r.at[j], z, mate)

    def a2(j):
        return send(chip.at[j, 1 - y], got2.at[j], a2s.at[j], a2r.at[j], z, over)

    def b_right(j, p):
        return send(prod.at[j, p], from_l.at[j, p], brs.at[j, p], brr.at[j, p], z + 1, c)

    def b_left(j, p):
        return send(prod.at[j, p], from_r.at[j, p], bls.at[j, p], blr.at[j, p], z - 1, c)

    def c_right(j, p):
        return send(full.at[j, c, p], full.at[j, c, p], crs.at[j, p], crr.at[j, p], z + 1, c)

    def c_left(j, p):
        return send(full.at[j, c, p], full.at[j, c, p], cls.at[j, p], clr.at[j, p], z - 1, c)

    def c_over(j, p):
        return send(full.at[j, c, p], full.at[j, c, p], cys.at[j, p], cyr.at[j, p], z, over)

    def c_over_in(j, p):
        return send(full.at[j, over, p], full.at[j, over, p], cys.at[j, p], cyr.at[j, p], z, over)

    def c_mate(j, q, u, p):
        return send(full.at[j, q, p], full.at[j, q, p], cps.at[j, u, p], cpr.at[j, u, p], z, mate)

    def merge(a, b):
        top_a, top_b = a[256:258], b[256:258]
        top = jnp.maximum(top_a, top_b)
        fa = jnp.exp2((top_a - top) * EXP2_SCALE)
        fb = jnp.exp2((top_b - top) * EXP2_SCALE)
        vals = [
            a[128 * h : 128 * h + 128] * fa[h : h + 1] + b[128 * h : 128 * h + 128] * fb[h : h + 1] for h in range(2)
        ]
        return vals, top, a[258:260] * fa + b[258:260] * fb

    for j in range(n_chunks):
        a1(j).start()

    def stage_a1(j):
        a1(j).wait_recv()
        for s in range(2):
            vals, top, total = merge(part[2 * j + s, core], got1[j, s])
            chip[j, s, 0:128] = vals[0]
            chip[j, s, 128:256] = vals[1]
            chip[j, s, 256:264] = jnp.concatenate([top, total, jnp.zeros((4, 128), jnp.float32)], axis=0)
        a2(j).start()

    def stage_a2(j):
        a2(j).wait_recv()
        vals, _, total = merge(chip[j, y], got2[j])
        turned = [(vals[h] / total[h : h + 1]).T for h in range(2)]
        o = jnp.concatenate([turned[h][32 * g : 32 * g + 32] for h in range(2) for g in range(4)], axis=1)
        o = o.astype(jnp.bfloat16)
        if j == 0:
            wo_copy.wait()

        def one_part(p, carry):
            prod[j, p] = jnp.dot(
                o, wo[:, pl.ds(pl.multiple_of(p * width, width), width)], preferred_element_type=jnp.float32
            )
            return carry

        lax.fori_loop(0, n_part, one_part, 0)

        @pl.when(z == 0)
        def _():
            for p in range(last, 0, -1):
                b_right(j, p).start()

        @pl.when(z == last)
        def _():
            for p in range(last):
                b_left(j, p).start()

    def pass_right(j, p):
        b_right(j, p).wait_recv()
        prod[j, p] = prod[j, p] + from_l[j, p]
        b_right(j, p).start()

    def pass_left(j, p):
        b_left(j, p).wait_recv()
        prod[j, p] = prod[j, p] + from_r[j, p]
        b_left(j, p).start()

    def stage_b1(j):
        @pl.when(z == 1)
        def _():
            pass_right(j, 3)
            pass_right(j, 2)

        @pl.when(z == 2)
        def _():
            pass_left(j, 0)
            pass_left(j, 1)

    def stage_b2(j):
        @pl.when(z == 2)
        def _():
            pass_right(j, 3)

        @pl.when(z == 1)
        def _():
            pass_left(j, 0)

    def stage_c0(j):
        x_copies[j].wait()

        @pl.when(z > 0)
        def _():
            b_right(j, z).wait_recv()
            prod[j, z] = prod[j, z] + from_l[j, z]

        @pl.when(z < last)
        def _():
            b_left(j, z).wait_recv()
            prod[j, z] = prod[j, z] + from_r[j, z]

        full[j, c, z] = prod[j, z] + xs[j].astype(jnp.float32)

        @pl.when(z < last)
        def _():
            c_right(j, z).start()

        @pl.when(z > 0)
        def _():
            c_left(j, z).start()

        c_over(j, z).start()
        c_mate(j, c, 0, z).start()

    def stage_c(j, d):
        @pl.when(z - d >= 0)
        def _():
            p = z - d
            c_right(j, p).wait_recv()

            @pl.when(z < last)
            def _():
                c_right(j, p).start()

            c_over(j, p).start()
            c_mate(j, c, 0, p).start()

        @pl.when(z + d <= last)
        def _():
            p = z + d
            c_left(j, p).wait_recv()

            @pl.when(z > 0)
            def _():
                c_left(j, p).start()

            c_over(j, p).start()
            c_mate(j, c, 0, p).start()

    def stage_over(j):
        for p in range(n_part):
            c_over_in(j, p).wait_recv()
            c_mate(j, over, 1, p).start()

    def out_copy(j):
        return pltpu.make_async_copy(stage.at[j], out_hbm.at[pl.ds(128 * j, 128)], out_sem.at[j])

    def stage_out(j):
        for p in range(n_part):
            c_mate(j, mate, 0, p).wait_recv()
            c_mate(j, over_mate, 1, p).wait_recv()
        for q in range(4):
            for p in range(n_part):
                stage[j, 32 * q : 32 * q + 32, width * p : width * p + width] = full[j, q, p].astype(jnp.bfloat16)
        out_copy(j).start()

    stages = [
        stage_a1, stage_a2, stage_b1, stage_b2, stage_c0,
        functools.partial(stage_c, d=1), functools.partial(stage_c, d=2), functools.partial(stage_c, d=3),
        stage_over, stage_out,
    ]
    for r in range(n_chunks + len(stages) - 1):
        for i, stage_fn in enumerate(stages):
            if 0 <= r - i < n_chunks:
                stage_fn(r - i)

    for j in range(n_chunks):
        a1(j).wait_send()
        a2(j).wait_send()
        for p in range(n_part):
            @pl.when(z < p)
            def _():
                b_right(j, p).wait_send()

            @pl.when(z > p)
            def _():
                b_left(j, p).wait_send()

            @pl.when((z >= p) & (z < last))
            def _():
                c_right(j, p).wait_send()

            @pl.when((z <= p) & (z > 0))
            def _():
                c_left(j, p).wait_send()

            c_over(j, p).wait_send()
            c_mate(j, c, 0, p).wait_send()
            c_mate(j, over, 1, p).wait_send()
        out_copy(j).wait()


def finish(part, x2, w_o):
    rows, d_model = x2.shape
    n_chunks, n_part = rows // 128, 4
    width = d_model // n_part
    any_spec = pl.BlockSpec(memory_space=pl.ANY)
    piece = (32, width)
    f32 = jnp.float32
    sems = pltpu.SemaphoreType.DMA
    per_part = [sems((n_chunks, n_part))] * 10
    return pl.pallas_call(
        finish_kernel,
        out_shape=jax.ShapeDtypeStruct((rows, d_model), jnp.bfloat16),
        in_specs=[pl.BlockSpec(memory_space=pltpu.VMEM), any_spec, any_spec],
        out_specs=any_spec,
        scratch_shapes=[
            pltpu.VMEM(w_o.shape, jnp.bfloat16),
            pltpu.VMEM((n_chunks, *piece), jnp.bfloat16),
            pltpu.VMEM((n_chunks, 2, STAT_ROWS, 128), f32),
            pltpu.VMEM((n_chunks, 2, STAT_ROWS, 128), f32),
            pltpu.VMEM((n_chunks, STAT_ROWS, 128), f32),
            pltpu.VMEM((n_chunks, n_part, *piece), f32),
            pltpu.VMEM((n_chunks, n_part, *piece), f32),
            pltpu.VMEM((n_chunks, n_part, *piece), f32),
            pltpu.VMEM((n_chunks, 4, n_part, *piece), f32),
            pltpu.VMEM((n_chunks, 128, d_model), jnp.bfloat16),
            sems,
            sems((n_chunks,)),
            sems((n_chunks,)),
            *[sems((n_chunks,))] * 4,
            *per_part,
            sems((n_chunks, 2, n_part)),
            sems((n_chunks, 2, n_part)),
        ],
        compiler_params=pltpu.CompilerParams(
            collective_id=0, has_side_effects=True, vmem_limit_bytes=56 * 1024 * 1024
        ),
        cost_estimate=pl.CostEstimate(flops=2 * 128 * 1024 * 4096, bytes_accessed=16 << 20, transcendentals=0),
        name="finish",
    )(part, x2, w_o)


def solution(mesh):
    n_cp = mesh.shape["cp"]

    def per_device(hidden, prefix_len, k_cache, v_cache, attn_norm, w_q, w_k, w_v, w_o, q_norm, k_norm):
        n_seq, n_new, d_model = hidden.shape
        x2 = hidden.reshape(n_seq * n_new, d_model)
        q3, k_rows, v_rows = project(prefix_len, x2, attn_norm, w_q, w_k, w_v, q_norm, k_norm)
        part = attend(
            prefix_len, q3, k_cache.reshape(n_seq, -1, HEAD_DIM), v_cache.reshape(n_seq, -1, HEAD_DIM), k_rows, v_rows, n_cp
        )
        out = finish(part, x2, w_o)
        new_shape = (n_seq, n_new, 2, HEAD_DIM)
        return out.reshape(hidden.shape), k_rows.reshape(new_shape), v_rows.reshape(new_shape)

    cache_spec = P("dp", "cp", "tp", None)
    arg_specs = (P("dp", None, None), P("dp"), cache_spec, cache_spec, P(None), P(None, "tp"), P(None, "tp"), P(None, "tp"), P("tp", None), P(None), P(None))
    out_specs = (P("dp", None, None), P("dp", None, "tp", None), P("dp", None, "tp", None))
    return jax.shard_map(per_device, mesh=mesh, in_specs=arg_specs, out_specs=out_specs, check_vma=False)
```

```python
import functools

import jax
import jax.numpy as jnp
import numpy as np
from jax import lax
from jax.experimental import pallas as pl
from jax.experimental.pallas import tpu as pltpu
from jax.sharding import PartitionSpec as P

HEAD_DIM = 128
MASKED = -1e30
EXP2_SCALE = HEAD_DIM**-0.5 * 1.4426950408889634
MESH = pl.DeviceIdType.MESH


def project_kernel(
    len_ref, x_hbm, gain, wq_hbm, wk_hbm, wv_hbm, q_gain, k_gain, freq,
    q_out, k_out, v_out, x_buf, h_buf, w_buf, cos_t, sin_t, turn, x_sem, w_sem,
):
    rows, d_model = x_buf.shape
    n_q = wq_hbm.shape[1] // 256
    n_seq = len_ref.shape[0]
    n_new = rows // n_seq
    piece = rows // 4
    x_copies = [
        pltpu.make_async_copy(x_hbm.at[pl.ds(piece * i, piece)], x_buf.at[pl.ds(piece * i, piece)], x_sem.at[i])
        for i in range(4)
    ]
    for copy in x_copies:
        copy.start()
    w_copies = [
        pltpu.make_async_copy(wq_hbm.at[:, pl.ds(256 * i, 256)], w_buf.at[i], w_sem.at[i]) for i in range(n_q)
    ]
    w_copies.append(pltpu.make_async_copy(wk_hbm, w_buf.at[n_q], w_sem.at[n_q]))
    w_copies.append(pltpu.make_async_copy(wv_hbm, w_buf.at[n_q + 1], w_sem.at[n_q + 1]))

    lane = lax.broadcasted_iota(jnp.int32, (n_new, 128), 1)
    token = lax.broadcasted_iota(jnp.int32, (n_new, 128), 0)

    def rope_rows(b, carry):
        angle = (token + len_ref[b]).astype(jnp.float32) * freq[...]
        sel = pl.ds(pl.multiple_of(b * n_new, n_new), n_new)
        cos_t[sel, :] = jnp.cos(angle)
        sin = jnp.sin(angle)
        sin_t[sel, :] = jnp.where(lane < 64, -sin, sin)
        return carry

    lax.fori_loop(0, n_seq, rope_rows, 0)
    x_gain = gain[...].astype(jnp.float32).reshape(1, d_model)

    def norm_rows(i, carry):
        sel = pl.ds(pl.multiple_of(i * 32, 32), 32)
        x = x_buf[sel, :].astype(jnp.float32)
        mean_sq = jnp.mean(x * x, axis=-1, keepdims=True)
        h_buf[sel, :] = (x * lax.rsqrt(mean_sq + 1e-6) * x_gain).astype(jnp.bfloat16)
        return carry

    for i in range(4):
        x_copies[i].wait()
        if i == 0:
            for copy in w_copies:
                copy.start()
    lax.fori_loop(0, rows // 32, norm_rows, 0)
    q_gain_row = q_gain[...].astype(jnp.float32).reshape(1, 128)
    k_gain_row = k_gain[...].astype(jnp.float32).reshape(1, 128)

    def one_tile(i, carry):
        pltpu.make_async_copy(w_buf.at[i], w_buf.at[i], w_sem.at[i]).wait()
        lin = jnp.dot(h_buf[...], w_buf[i], preferred_element_type=jnp.float32).astype(jnp.bfloat16)
        lin = lin.astype(jnp.float32)
        head_gain = jnp.where(i < n_q, q_gain_row, k_gain_row)
        for u in range(2):
            raw = lin[:, 128 * u : 128 * u + 128]
            mean_sq = jnp.mean(raw * raw, axis=-1, keepdims=True)
            t = raw * lax.rsqrt(mean_sq + 1e-6) * head_gain
            t = t * cos_t[...] + pltpu.roll(t, 64, 1) * sin_t[...]

            @pl.when(i < n_q)
            def _():
                q_out[i, :, 128 * u : 128 * u + 128] = t.astype(jnp.bfloat16)

            @pl.when(i >= n_q)
            def _():
                turn[pl.ds(u, rows, stride=2), :] = jnp.where(i == n_q, t, raw)

        @pl.when(i == n_q)
        def _():
            k_out[...] = turn[...].astype(jnp.bfloat16)

        @pl.when(i == n_q + 1)
        def _():
            v_out[...] = turn[...].astype(jnp.bfloat16)

        return carry

    lax.fori_loop(0, n_q + 2, one_tile, 0)


def project(prefix_len, x2, gain, w_q, w_k, w_v, q_gain, k_gain):
    rows, d_model = x2.shape
    n_q = w_q.shape[1] // 256
    half_dim = HEAD_DIM // 2
    freq = 1.0 / (1000000.0 ** (np.arange(half_dim, dtype=np.float64) * 2.0 / HEAD_DIM))
    freq = jnp.asarray(np.concatenate([freq, freq])[None], jnp.float32)
    any_spec = pl.BlockSpec(memory_space=pl.ANY)
    vmem = pl.BlockSpec(memory_space=pltpu.VMEM)
    return pl.pallas_call(
        project_kernel,
        out_shape=(
            jax.ShapeDtypeStruct((n_q, rows, 256), jnp.bfloat16),
            jax.ShapeDtypeStruct((2 * rows, 128), jnp.bfloat16),
            jax.ShapeDtypeStruct((2 * rows, 128), jnp.bfloat16),
        ),
        in_specs=[pl.BlockSpec(memory_space=pltpu.SMEM), any_spec, vmem, any_spec, any_spec, any_spec, vmem, vmem, vmem],
        out_specs=(vmem, vmem, vmem),
        scratch_shapes=[
            pltpu.VMEM((rows, d_model), jnp.bfloat16),
            pltpu.VMEM((rows, d_model), jnp.bfloat16),
            pltpu.VMEM((n_q + 2, d_model, 256), jnp.bfloat16),
            pltpu.VMEM((rows, 128), jnp.float32),
            pltpu.VMEM((rows, 128), jnp.float32),
            pltpu.VMEM((2 * rows, 128), jnp.float32),
            pltpu.SemaphoreType.DMA((4,)),
            pltpu.SemaphoreType.DMA((n_q + 2,)),
        ],
        compiler_params=pltpu.CompilerParams(vmem_limit_bytes=56 * 1024 * 1024),
        cost_estimate=pl.CostEstimate(
            flops=2 * rows * d_model * 256 * (n_q + 2), bytes_accessed=20 << 20, transcendentals=0
        ),
        name="project",
    )(prefix_len, x2, gain, w_q, w_k, w_v, q_gain, k_gain, freq)


def block_kernel(
    len_ref, q_ref, kn_ref, vn_ref, kc_hbm, vc_hbm, x_hbm, wo_hbm, out_hbm,
    kbuf, vbuf, qt, s_buf, sn_buf, acc, top_buf,
    wo, xs, part, got1, chip, got2, ob, prod, from_l, from_r, full, stage,
    k_sem, v_sem, wo_sem, xs_sem, out_sem, a1s, a1r, a2s, a2r, a3s, a3r,
    brs, brr, bls, blr, crs, crr, cls, clr, cys, cyr, cps, cpr, *, tile,
):
    dp, z, c = lax.axis_index("dp"), lax.axis_index("tp"), lax.axis_index("cp")
    y, core = c // 2, c % 2
    mate = 2 * y + (1 - core)
    over = 2 * (1 - y) + core
    over_mate = 2 * (1 - y) + (1 - core)
    n_seq, n_part, width = full.shape[0], full.shape[2], full.shape[4]
    last = n_part - 1
    cache_rows = kbuf.shape[1]
    n_new = kn_ref.shape[0] // n_seq
    n_tiles = cache_rows // tile

    def send(src, dst, send_sem, recv_sem, tp, cp):
        return pltpu.make_async_remote_copy(
            src_ref=src, dst_ref=dst, send_sem=send_sem, recv_sem=recv_sem, device_id=(dp, tp, cp), device_id_type=MESH
        )

    def k_copy(b):
        return pltpu.make_async_copy(kc_hbm.at[b], kbuf.at[b % 2], k_sem.at[b % 2])

    def v_copy(b):
        return pltpu.make_async_copy(vc_hbm.at[b], vbuf.at[b % 2], v_sem.at[b % 2])

    def wo_copy(p):
        cols = pl.ds(pl.multiple_of(n_part * width * core + width * p, width), width)
        return pltpu.make_async_copy(wo_hbm.at[:, cols], wo.at[p], wo_sem.at[p])

    def x_copy(j):
        rows = pl.ds(pl.multiple_of(64 * j + 32 * y, 32), 32)
        cols = pl.ds(pl.multiple_of(n_part * width * core + width * z, width), width)
        return pltpu.make_async_copy(x_hbm.at[rows, cols], xs.at[j], xs_sem.at[j])

    k_copy(0).start()
    v_copy(0).start()
    for p in range(n_part):
        wo_copy(p).start()
    for j in range(n_seq):
        x_copy(j).start()

    barrier = pltpu.get_barrier_semaphore()
    for peer in (mate, over):
        pl.semaphore_signal(barrier, inc=1, device_id=(dp, z, peer), device_id_type=MESH)

    @pl.when(z > 0)
    def _():
        pl.semaphore_signal(barrier, inc=1, device_id=(dp, z - 1, c), device_id_type=MESH)

    @pl.when(z < last)
    def _():
        pl.semaphore_signal(barrier, inc=1, device_id=(dp, z + 1, c), device_id_type=MESH)

    @pl.when((z == 0) | (z == last))
    def _():
        pl.semaphore_wait(barrier, 3)

    @pl.when((z > 0) & (z < last))
    def _():
        pl.semaphore_wait(barrier, 4)

    sub16 = lax.broadcasted_iota(jnp.int32, (16, 128), 0) & 1
    even_rows = jnp.where(sub16 == 0, 1.0, 0.0).astype(jnp.bfloat16)
    odd_rows = jnp.where(sub16 == 0, 0.0, 1.0).astype(jnp.bfloat16)
    sub8 = lax.broadcasted_iota(jnp.int32, (8, 256), 0) & 1

    def split_rows(k):
        n = k.shape[0]
        k3 = k.reshape(n // 16, 16, 128)
        return jnp.concatenate(
            [(k3 * even_rows[None]).reshape(n, 128), (k3 * odd_rows[None]).reshape(n, 128)], axis=1
        )

    def split_lanes(v):
        n = v.shape[0]
        lane = lax.broadcasted_iota(jnp.int32, (16, n), 1) & 1
        even = jnp.where(lane == 0, 1.0, 0.0).astype(jnp.bfloat16)
        odd = jnp.where(lane == 0, 0.0, 1.0).astype(jnp.bfloat16)
        vt = v.T.reshape(8, 16, n)
        return jnp.concatenate([(vt * even[None]).reshape(128, n), (vt * odd[None]).reshape(128, n)], axis=0)

    def scores(k):
        return jnp.dot(split_rows(k), qt[...], preferred_element_type=jnp.float32)

    def score_pass(b):
        @pl.when(b + 1 < n_seq)
        def _():
            k_copy(b + 1).start()
            v_copy(b + 1).start()

        q_rows = pl.multiple_of(64 * b, 64)
        for h in range(2):
            blocks = [
                q_ref[h * 2 + g // 2, pl.ds(q_rows + th * 32, 32), (g % 2) * 128 : (g % 2) * 128 + 128]
                for th in range(2)
                for g in range(4)
            ]
            qt[h * 128 : h * 128 + 128, :] = jnp.concatenate(blocks, axis=0).T
        n_rows = 2 * (len_ref[b] - c * (cache_rows // 2))
        k_copy(b).wait()

        def score_tile(t, top):
            sel = pl.ds(pl.multiple_of(t * tile, tile), tile)
            s = scores(kbuf[b % 2, sel, :])
            row = t * tile + lax.broadcasted_iota(jnp.int32, (tile, 256), 0)
            s = jnp.where(row < n_rows, s, MASKED)
            s_buf[sel, :] = s
            return jnp.maximum(top, jnp.max(s.reshape(tile // 8, 8, 256), axis=0))

        top = lax.fori_loop(0, n_tiles, score_tile, jnp.full((8, 256), MASKED, jnp.float32))

        key = lax.broadcasted_iota(jnp.int32, (n_new, 256), 0) // 2
        col = lax.broadcasted_iota(jnp.int32, (n_new, 256), 1)
        token = (col // 128) * 32 + (col % 32)
        token = jnp.where(c == 3, token, -1)
        s_new = jnp.where(key <= token, scores(kn_ref[pl.ds(pl.multiple_of(n_new * b, n_new), n_new), :]), MASKED)
        sn_buf[...] = s_new
        top = jnp.maximum(top, jnp.max(s_new.reshape(n_new // 8, 8, 256), axis=0))
        top0 = jnp.max(jnp.where(sub8 == 0, top, MASKED), axis=0, keepdims=True)
        top1 = jnp.max(jnp.where(sub8 == 0, MASKED, top), axis=0, keepdims=True)
        top_buf[...] = jnp.where(sub8 == 0, top0, top1)

    def weigh_pass(b):
        top = top_buf[...]
        base = jnp.where(top > 0.5 * MASKED, top, 0.0)

        def weigh(s, v):
            n = s.shape[0]
            p = jnp.exp2((s.reshape(n // 8, 8, 256) - base[None]) * EXP2_SCALE)
            total = jnp.sum(p, axis=0)
            out = jnp.dot(split_lanes(v), p.reshape(n, 256).astype(jnp.bfloat16), preferred_element_type=jnp.float32)
            return total, out

        total, out = weigh(sn_buf[...], vn_ref[pl.ds(pl.multiple_of(n_new * b, n_new), n_new), :])
        acc[...] = out
        v_copy(b).wait()

        def weigh_tile(t, total):
            sel = pl.ds(pl.multiple_of(t * tile, tile), tile)
            more, out = weigh(s_buf[sel, :], vbuf[b % 2, sel, :])
            acc[...] += out
            return total + more

        total = lax.fori_loop(0, n_tiles, weigh_tile, total)
        pad = jnp.zeros((6, 256), jnp.float32)
        for h in range(2):
            part[b, h, 0:128, :] = acc[h * 128 : h * 128 + 128, :]
            total_h = jnp.sum(jnp.where(sub8 == h, total, 0.0), axis=0, keepdims=True)
            part[b, h, 128:136, :] = jnp.concatenate([top[h : h + 1], total_h, pad], axis=0)
        a1(b).start()

    def a1(j):
        return send(part.at[j, 1 - core], got1.at[j], a1s.at[j], a1r.at[j], z, mate)

    def a2(j):
        return send(chip.at[j, 1 - y], got2.at[j], a2s.at[j], a2r.at[j], z, over)

    def a3(j, h):
        return send(ob.at[j, h], ob.at[j, h], a3s.at[j], a3r.at[j], z, mate)

    def b_right(j, p):
        return send(prod.at[j, p], from_l.at[j, p], brs.at[j, p], brr.at[j, p], z + 1, c)

    def b_left(j, p):
        return send(prod.at[j, p], from_r.at[j, p], bls.at[j, p], blr.at[j, p], z - 1, c)

    def c_right(j, p):
        return send(full.at[j, c, p], full.at[j, c, p], crs.at[j, p], crr.at[j, p], z + 1, c)

    def c_left(j, p):
        return send(full.at[j, c, p], full.at[j, c, p], cls.at[j, p], clr.at[j, p], z - 1, c)

    def c_over(j, q, p):
        return send(full.at[j, q, p], full.at[j, q, p], cys.at[j, p], cyr.at[j, p], z, over)

    def c_mate(j, q, u, p):
        return send(full.at[j, q, p], full.at[j, q, p], cps.at[j, u, p], cpr.at[j, u, p], z, mate)

    def merge(a, b):
        top = jnp.maximum(a[128:129], b[128:129])
        fa = jnp.exp2((a[128:129] - top) * EXP2_SCALE)
        fb = jnp.exp2((b[128:129] - top) * EXP2_SCALE)
        return a[0:128] * fa + b[0:128] * fb, top, a[129:130] * fa + b[129:130] * fb

    def stage_a1(j):
        a1(j).wait_recv()
        vals, top, total = merge(part[j, core], got1[j])
        for th in range(2):
            sel = slice(128 * th, 128 * th + 128)
            chip[j, th, 0:128] = vals[:, sel]
            chip[j, th, 128:136] = jnp.concatenate([top[:, sel], total[:, sel], jnp.zeros((6, 128), jnp.float32)], axis=0)
        a2(j).start()

    def stage_a2(j):
        a2(j).wait_recv()
        vals, _, total = merge(chip[j, y], got2[j])
        ob[j, core] = (vals / total).T
        a3(j, core).start()

    def stage_a3(j):
        a3(j, 1 - core).wait_recv()

        @pl.when(j == 0)
        def _():
            for p in range(n_part):
                wo_copy(p).wait()

        o = jnp.concatenate([ob[j, h, 32 * g : 32 * g + 32, :] for h in range(2) for g in range(4)], axis=1)
        o = o.astype(jnp.bfloat16)
        for p in range(n_part):
            prod[j, p] = jnp.dot(o, wo[p], preferred_element_type=jnp.float32)

        @pl.when(z == 0)
        def _():
            for p in range(last, 0, -1):
                b_right(j, p).start()

        @pl.when(z == last)
        def _():
            for p in range(last):
                b_left(j, p).start()

    def pass_right(j, p):
        b_right(j, p).wait_recv()
        prod[j, p] = prod[j, p] + from_l[j, p]
        b_right(j, p).start()

    def pass_left(j, p):
        b_left(j, p).wait_recv()
        prod[j, p] = prod[j, p] + from_r[j, p]
        b_left(j, p).start()

    def stage_b1(j):
        @pl.when(z == 1)
        def _():
            pass_right(j, 3)
            pass_right(j, 2)

        @pl.when(z == 2)
        def _():
            pass_left(j, 0)
            pass_left(j, 1)

    def stage_b2(j):
        @pl.when(z == 2)
        def _():
            pass_right(j, 3)

        @pl.when(z == 1)
        def _():
            pass_left(j, 0)

    def stage_c0(j):
        x_copy(j).wait()

        @pl.when(z > 0)
        def _():
            b_right(j, z).wait_recv()
            prod[j, z] = prod[j, z] + from_l[j, z]

        @pl.when(z < last)
        def _():
            b_left(j, z).wait_recv()
            prod[j, z] = prod[j, z] + from_r[j, z]

        full[j, c, z] = prod[j, z] + xs[j].astype(jnp.float32)

        @pl.when(z < last)
        def _():
            c_right(j, z).start()

        @pl.when(z > 0)
        def _():
            c_left(j, z).start()

        c_over(j, c, z).start()
        c_mate(j, c, 0, z).start()

    def stage_c(j, d):
        @pl.when(z - d >= 0)
        def _():
            p = z - d
            c_right(j, p).wait_recv()

            @pl.when(z < last)
            def _():
                c_right(j, p).start()

            c_over(j, c, p).start()
            c_mate(j, c, 0, p).start()

        @pl.when(z + d <= last)
        def _():
            p = z + d
            c_left(j, p).wait_recv()

            @pl.when(z > 0)
            def _():
                c_left(j, p).start()

            c_over(j, c, p).start()
            c_mate(j, c, 0, p).start()

    def stage_over(j):
        for p in range(n_part):
            c_over(j, over, p).wait_recv()
            c_mate(j, over, 1, p).start()

    def out_copy(j):
        return pltpu.make_async_copy(
            stage.at[j], out_hbm.at[pl.ds(pl.multiple_of(64 * j, 64), 64)], out_sem.at[j]
        )

    def stage_out(j):
        for p in range(n_part):
            c_mate(j, mate, 0, p).wait_recv()
            c_mate(j, over_mate, 1, p).wait_recv()
        for q in range(4):
            for p in range(n_part):
                col = width * (n_part * (q % 2) + p)
                stage[j, 32 * (q // 2) : 32 * (q // 2) + 32, col : col + width] = full[j, q, p].astype(jnp.bfloat16)
        out_copy(j).start()

    stages = [
        stage_a1, stage_a2, stage_a3, stage_b1, stage_b2, stage_c0,
        functools.partial(stage_c, d=1), functools.partial(stage_c, d=2), functools.partial(stage_c, d=3),
        stage_over, stage_out,
    ]

    def slot(s, carry):
        b = s // 2

        @pl.when((s % 2 == 0) & (b < n_seq))
        def _():
            score_pass(b)

        @pl.when((s % 2 == 1) & (b < n_seq))
        def _():
            weigh_pass(b)

        for i, stage_fn in enumerate(stages):
            t = s - 2 - i

            @pl.when((t >= 0) & (t % 2 == 0) & (t < 2 * n_seq))
            def _():
                stage_fn(t // 2)

        return carry

    lax.fori_loop(0, 2 * n_seq + len(stages), slot, 0)

    def drain(j, carry):
        a1(j).wait_send()
        a2(j).wait_send()
        a3(j, core).wait_send()
        for p in range(n_part):
            @pl.when(z < p)
            def _():
                b_right(j, p).wait_send()

            @pl.when(z > p)
            def _():
                b_left(j, p).wait_send()

            @pl.when((z >= p) & (z < last))
            def _():
                c_right(j, p).wait_send()

            @pl.when((z <= p) & (z > 0))
            def _():
                c_left(j, p).wait_send()

            c_over(j, c, p).wait_send()
            c_mate(j, c, 0, p).wait_send()
            c_mate(j, over, 1, p).wait_send()
        out_copy(j).wait()
        return carry

    lax.fori_loop(0, n_seq, drain, 0)


def attend_and_project(prefix_len, q3, kn, vn, kc, vc, x2, w_o):
    rows, d_model = x2.shape
    n_seq, cache_rows, _ = kc.shape
    n_part = 4
    width = d_model // (2 * n_part)
    new_rows = kn.shape[0] // n_seq
    tile = min(2048, cache_rows)
    any_spec = pl.BlockSpec(memory_space=pl.ANY)
    vmem = pl.BlockSpec(memory_space=pltpu.VMEM)
    f32, bf16 = jnp.float32, jnp.bfloat16
    sems = pltpu.SemaphoreType.DMA
    piece = (32, width)
    return pl.pallas_call(
        functools.partial(block_kernel, tile=tile),
        out_shape=jax.ShapeDtypeStruct((rows, d_model), bf16),
        in_specs=[pl.BlockSpec(memory_space=pltpu.SMEM), vmem, vmem, vmem, any_spec, any_spec, any_spec, any_spec],
        out_specs=any_spec,
        scratch_shapes=[
            pltpu.VMEM((2, cache_rows, 128), bf16),
            pltpu.VMEM((2, cache_rows, 128), bf16),
            pltpu.VMEM((256, 256), bf16),
            pltpu.VMEM((cache_rows, 256), f32),
            pltpu.VMEM((new_rows, 256), f32),
            pltpu.VMEM((256, 256), f32),
            pltpu.VMEM((8, 256), f32),
            pltpu.VMEM((n_part, w_o.shape[0], width), bf16),
            pltpu.VMEM((n_seq, *piece), bf16),
            pltpu.VMEM((n_seq, 2, 136, 256), f32),
            pltpu.VMEM((n_seq, 136, 256), f32),
            pltpu.VMEM((n_seq, 2, 136, 128), f32),
            pltpu.VMEM((n_seq, 136, 128), f32),
            pltpu.VMEM((n_seq, 2, 128, 128), f32),
            pltpu.VMEM((n_seq, n_part, *piece), f32),
            pltpu.VMEM((n_seq, n_part, *piece), f32),
            pltpu.VMEM((n_seq, n_part, *piece), f32),
            pltpu.VMEM((n_seq, 4, n_part, *piece), f32),
            pltpu.VMEM((n_seq, 64, d_model), bf16),
            sems((2,)),
            sems((2,)),
            sems((n_part,)),
            sems((n_seq,)),
            sems((n_seq,)),
            *[sems((n_seq,))] * 6,
            *[sems((n_seq, n_part))] * 10,
            sems((n_seq, 2, n_part)),
            sems((n_seq, 2, n_part)),
        ],
        compiler_params=pltpu.CompilerParams(
            collective_id=0, has_side_effects=True, vmem_limit_bytes=63 * 1024 * 1024
        ),
        cost_estimate=pl.CostEstimate(
            flops=4 * n_seq * cache_rows * 256 * 256, bytes_accessed=60 << 20, transcendentals=n_seq * cache_rows * 256
        ),
        name="attend_and_project",
    )(prefix_len, q3, kn, vn, kc, vc, x2, w_o)


def solution(mesh):
    def per_device(hidden, prefix_len, k_cache, v_cache, attn_norm, w_q, w_k, w_v, w_o, q_norm, k_norm):
        n_seq, n_new, d_model = hidden.shape
        x2 = hidden.reshape(n_seq * n_new, d_model)
        q3, k_rows, v_rows = project(prefix_len, x2, attn_norm, w_q, w_k, w_v, q_norm, k_norm)
        out = attend_and_project(
            prefix_len, q3, k_rows, v_rows,
            k_cache.reshape(n_seq, -1, HEAD_DIM), v_cache.reshape(n_seq, -1, HEAD_DIM), x2, w_o,
        )
        new_shape = (n_seq, n_new, 2, HEAD_DIM)
        return out.reshape(hidden.shape), k_rows.reshape(new_shape), v_rows.reshape(new_shape)

    cache_spec = P("dp", "cp", "tp", None)
    arg_specs = (P("dp", None, None), P("dp"), cache_spec, cache_spec, P(None), P(None, "tp"), P(None, "tp"), P(None, "tp"), P("tp", None), P(None), P(None))
    out_specs = (P("dp", None, None), P("dp", None, "tp", None), P("dp", None, "tp", None))
    return jax.shard_map(per_device, mesh=mesh, in_specs=arg_specs, out_specs=out_specs, check_vma=False)
```

```python
import functools

import jax
import jax.numpy as jnp
import numpy as np
from jax import lax
from jax.experimental import pallas as pl
from jax.experimental.pallas import tpu as pltpu
from jax.sharding import PartitionSpec as P

HEAD_DIM = 128
MASKED = -1e30
EXP2_SCALE = HEAD_DIM**-0.5 * 1.4426950408889634
MESH = pl.DeviceIdType.MESH


def project_kernel(
    len_ref, x_hbm, gain, wq_hbm, wk_hbm, wv_hbm, q_gain, k_gain, freq,
    q_out, k_out, v_out, x_buf, h_buf, w_buf, cos_t, sin_t, turn, x_sem, w_sem,
):
    rows, d_model = x_buf.shape
    n_q = wq_hbm.shape[1] // 256
    n_seq = len_ref.shape[0]
    n_new = rows // n_seq
    piece = rows // 4
    x_copies = [
        pltpu.make_async_copy(x_hbm.at[pl.ds(piece * i, piece)], x_buf.at[pl.ds(piece * i, piece)], x_sem.at[i])
        for i in range(4)
    ]
    for copy in x_copies:
        copy.start()
    w_copies = [
        pltpu.make_async_copy(wq_hbm.at[:, pl.ds(256 * i, 256)], w_buf.at[i], w_sem.at[i]) for i in range(n_q)
    ]
    w_copies.append(pltpu.make_async_copy(wk_hbm, w_buf.at[n_q], w_sem.at[n_q]))
    w_copies.append(pltpu.make_async_copy(wv_hbm, w_buf.at[n_q + 1], w_sem.at[n_q + 1]))

    lane = lax.broadcasted_iota(jnp.int32, (n_new, 128), 1)
    token = lax.broadcasted_iota(jnp.int32, (n_new, 128), 0)

    def rope_rows(b, carry):
        angle = (token + len_ref[b]).astype(jnp.float32) * freq[...]
        sel = pl.ds(pl.multiple_of(b * n_new, n_new), n_new)
        cos_t[sel, :] = jnp.cos(angle)
        sin = jnp.sin(angle)
        sin_t[sel, :] = jnp.where(lane < 64, -sin, sin)
        return carry

    lax.fori_loop(0, n_seq, rope_rows, 0)
    x_gain = gain[...].astype(jnp.float32).reshape(1, d_model)

    def norm_rows(i, carry):
        sel = pl.ds(pl.multiple_of(i * 32, 32), 32)
        x = x_buf[sel, :].astype(jnp.float32)
        mean_sq = jnp.mean(x * x, axis=-1, keepdims=True)
        h_buf[sel, :] = (x * lax.rsqrt(mean_sq + 1e-6) * x_gain).astype(jnp.bfloat16)
        return carry

    for i in range(4):
        x_copies[i].wait()
        if i == 0:
            for copy in w_copies:
                copy.start()
    lax.fori_loop(0, rows // 32, norm_rows, 0)
    q_gain_row = q_gain[...].astype(jnp.float32).reshape(1, 128)
    k_gain_row = k_gain[...].astype(jnp.float32).reshape(1, 128)

    def one_tile(i, carry):
        pltpu.make_async_copy(w_buf.at[i], w_buf.at[i], w_sem.at[i]).wait()
        lin = jnp.dot(h_buf[...], w_buf[i], preferred_element_type=jnp.float32).astype(jnp.bfloat16)
        lin = lin.astype(jnp.float32)
        head_gain = jnp.where(i < n_q, q_gain_row, k_gain_row)
        for u in range(2):
            raw = lin[:, 128 * u : 128 * u + 128]
            mean_sq = jnp.mean(raw * raw, axis=-1, keepdims=True)
            t = raw * lax.rsqrt(mean_sq + 1e-6) * head_gain
            t = t * cos_t[...] + pltpu.roll(t, 64, 1) * sin_t[...]

            @pl.when(i < n_q)
            def _():
                q_out[i, :, 128 * u : 128 * u + 128] = t.astype(jnp.bfloat16)

            @pl.when(i >= n_q)
            def _():
                turn[pl.ds(u, rows, stride=2), :] = jnp.where(i == n_q, t, raw)

        @pl.when(i == n_q)
        def _():
            k_out[...] = turn[...].astype(jnp.bfloat16)

        @pl.when(i == n_q + 1)
        def _():
            v_out[...] = turn[...].astype(jnp.bfloat16)

        return carry

    lax.fori_loop(0, n_q + 2, one_tile, 0)


def project(prefix_len, x2, gain, w_q, w_k, w_v, q_gain, k_gain):
    rows, d_model = x2.shape
    n_q = w_q.shape[1] // 256
    half_dim = HEAD_DIM // 2
    freq = 1.0 / (1000000.0 ** (np.arange(half_dim, dtype=np.float64) * 2.0 / HEAD_DIM))
    freq = jnp.asarray(np.concatenate([freq, freq])[None], jnp.float32)
    any_spec = pl.BlockSpec(memory_space=pl.ANY)
    vmem = pl.BlockSpec(memory_space=pltpu.VMEM)
    return pl.pallas_call(
        project_kernel,
        out_shape=(
            jax.ShapeDtypeStruct((n_q, rows, 256), jnp.bfloat16),
            jax.ShapeDtypeStruct((2 * rows, 128), jnp.bfloat16),
            jax.ShapeDtypeStruct((2 * rows, 128), jnp.bfloat16),
        ),
        in_specs=[pl.BlockSpec(memory_space=pltpu.SMEM), any_spec, vmem, any_spec, any_spec, any_spec, vmem, vmem, vmem],
        out_specs=(vmem, vmem, vmem),
        scratch_shapes=[
            pltpu.VMEM((rows, d_model), jnp.bfloat16),
            pltpu.VMEM((rows, d_model), jnp.bfloat16),
            pltpu.VMEM((n_q + 2, d_model, 256), jnp.bfloat16),
            pltpu.VMEM((rows, 128), jnp.float32),
            pltpu.VMEM((rows, 128), jnp.float32),
            pltpu.VMEM((2 * rows, 128), jnp.float32),
            pltpu.SemaphoreType.DMA((4,)),
            pltpu.SemaphoreType.DMA((n_q + 2,)),
        ],
        compiler_params=pltpu.CompilerParams(vmem_limit_bytes=56 * 1024 * 1024),
        cost_estimate=pl.CostEstimate(
            flops=2 * rows * d_model * 256 * (n_q + 2), bytes_accessed=20 << 20, transcendentals=0
        ),
        name="project",
    )(prefix_len, x2, gain, w_q, w_k, w_v, q_gain, k_gain, freq)


def block_kernel(
    len_ref, q_ref, kn_ref, vn_ref, kc_hbm, vc_hbm, x_hbm, wo_hbm, out_ref,
    kbuf, vbuf, qt, s_buf, sn_buf, acc, top_buf, run_top, run_sum,
    wo, xs, part, got1, chip, got2, ob, prod, from_l, from_r, full,
    k_sem, v_sem, wo_sem, xs_sem, a1s, a1r, a2s, a2r, a3s, a3r,
    brs, brr, bls, blr, crs, crr, cls, clr, cys, cyr, cps, cpr, *, tile,
):
    dp, z, c = lax.axis_index("dp"), lax.axis_index("tp"), lax.axis_index("cp")
    y, core = c // 2, c % 2
    mate = 2 * y + (1 - core)
    over = 2 * (1 - y) + core
    over_mate = 2 * (1 - y) + (1 - core)
    n_seq, n_part, width = full.shape[0], full.shape[2], full.shape[4]
    last = n_part - 1
    cache_rows = kbuf.shape[1]
    n_new = kn_ref.shape[0] // n_seq
    n_tiles = cache_rows // tile

    def send(src, dst, send_sem, recv_sem, tp, cp):
        return pltpu.make_async_remote_copy(
            src_ref=src, dst_ref=dst, send_sem=send_sem, recv_sem=recv_sem, device_id=(dp, tp, cp), device_id_type=MESH
        )

    def k_copy(b):
        return pltpu.make_async_copy(kc_hbm.at[b], kbuf.at[b % 2], k_sem.at[b % 2])

    def v_copy(b):
        return pltpu.make_async_copy(vc_hbm.at[b], vbuf.at[b % 2], v_sem.at[b % 2])

    def wo_copy(p):
        cols = pl.ds(pl.multiple_of(n_part * width * core + width * p, width), width)
        return pltpu.make_async_copy(wo_hbm.at[:, cols], wo.at[p], wo_sem.at[p])

    def x_copy(j):
        rows = pl.ds(pl.multiple_of(64 * j + 32 * y, 32), 32)
        cols = pl.ds(pl.multiple_of(n_part * width * core + width * z, width), width)
        return pltpu.make_async_copy(x_hbm.at[rows, cols], xs.at[j], xs_sem.at[j])

    k_copy(0).start()
    v_copy(0).start()
    for p in range(n_part):
        wo_copy(p).start()
    for j in range(n_seq):
        x_copy(j).start()

    barrier = pltpu.get_barrier_semaphore()
    for peer in (mate, over):
        pl.semaphore_signal(barrier, inc=1, device_id=(dp, z, peer), device_id_type=MESH)

    @pl.when(z > 0)
    def _():
        pl.semaphore_signal(barrier, inc=1, device_id=(dp, z - 1, c), device_id_type=MESH)

    @pl.when(z < last)
    def _():
        pl.semaphore_signal(barrier, inc=1, device_id=(dp, z + 1, c), device_id_type=MESH)

    @pl.when((z == 0) | (z == last))
    def _():
        pl.semaphore_wait(barrier, 3)

    @pl.when((z > 0) & (z < last))
    def _():
        pl.semaphore_wait(barrier, 4)

    sub16 = lax.broadcasted_iota(jnp.int32, (16, 128), 0) & 1
    even_rows = jnp.where(sub16 == 0, 1.0, 0.0).astype(jnp.bfloat16)
    odd_rows = jnp.where(sub16 == 0, 0.0, 1.0).astype(jnp.bfloat16)
    sub8 = lax.broadcasted_iota(jnp.int32, (8, 256), 0) & 1

    def split_rows(k):
        n = k.shape[0]
        k3 = k.reshape(n // 16, 16, 128)
        return jnp.concatenate(
            [(k3 * even_rows[None]).reshape(n, 128), (k3 * odd_rows[None]).reshape(n, 128)], axis=1
        )

    def split_lanes(v):
        n = v.shape[0]
        lane = lax.broadcasted_iota(jnp.int32, (16, n), 1) & 1
        even = jnp.where(lane == 0, 1.0, 0.0).astype(jnp.bfloat16)
        odd = jnp.where(lane == 0, 0.0, 1.0).astype(jnp.bfloat16)
        vt = v.T.reshape(8, 16, n)
        return jnp.concatenate([(vt * even[None]).reshape(128, n), (vt * odd[None]).reshape(128, n)], axis=0)

    def scores(k):
        return jnp.dot(split_rows(k), qt[...], preferred_element_type=jnp.float32)

    def fetch(b):
        @pl.when(b + 1 < n_seq)
        def _():
            k_copy(b + 1).start()

        @pl.when((b > 0) & (b < n_seq))
        def _():
            v_copy(b).start()

    def score_start(b):
        q_rows = pl.multiple_of(64 * b, 64)
        for h in range(2):
            blocks = [
                q_ref[h * 2 + g // 2, pl.ds(q_rows + th * 32, 32), (g % 2) * 128 : (g % 2) * 128 + 128]
                for th in range(2)
                for g in range(4)
            ]
            qt[h * 128 : h * 128 + 128, :] = jnp.concatenate(blocks, axis=0).T
        run_top[...] = jnp.full((8, 256), MASKED, jnp.float32)
        k_copy(b).wait()

    def score_tile(b, t):
        sel = pl.ds(pl.multiple_of(t * tile, tile), tile)
        n_rows = 2 * (len_ref[b] - c * (cache_rows // 2)) - t * tile
        s = scores(kbuf[b % 2, sel, :])
        s = jnp.where(lax.broadcasted_iota(jnp.int32, (tile, 256), 0) < n_rows, s, MASKED)
        s_buf[sel, :] = s
        run_top[...] = jnp.maximum(run_top[...], jnp.max(s.reshape(tile // 8, 8, 256), axis=0))

    def score_end(b):
        key = lax.broadcasted_iota(jnp.int32, (n_new, 256), 0) // 2
        col = lax.broadcasted_iota(jnp.int32, (n_new, 256), 1)
        token = (col // 128) * 32 + (col % 32)
        token = jnp.where(c == 3, token, -1)
        s_new = jnp.where(key <= token, scores(kn_ref[pl.ds(pl.multiple_of(n_new * b, n_new), n_new), :]), MASKED)
        sn_buf[...] = s_new
        top = jnp.maximum(run_top[...], jnp.max(s_new.reshape(n_new // 8, 8, 256), axis=0))
        top0 = jnp.max(jnp.where(sub8 == 0, top, MASKED), axis=0, keepdims=True)
        top1 = jnp.max(jnp.where(sub8 == 0, MASKED, top), axis=0, keepdims=True)
        top_buf[...] = jnp.where(sub8 == 0, top0, top1)

    def weigh(s, v):
        top = top_buf[...]
        base = jnp.where(top > 0.5 * MASKED, top, 0.0)
        n = s.shape[0]
        p = jnp.exp2((s.reshape(n // 8, 8, 256) - base[None]) * EXP2_SCALE)
        out = jnp.dot(split_lanes(v), p.reshape(n, 256).astype(jnp.bfloat16), preferred_element_type=jnp.float32)
        return jnp.sum(p, axis=0), out

    def weigh_start(b):
        run_sum[...], acc[...] = weigh(sn_buf[...], vn_ref[pl.ds(pl.multiple_of(n_new * b, n_new), n_new), :])
        v_copy(b).wait()

    def weigh_tile(b, t):
        sel = pl.ds(pl.multiple_of(t * tile, tile), tile)
        more, out = weigh(s_buf[sel, :], vbuf[b % 2, sel, :])
        acc[...] += out
        run_sum[...] += more

    def weigh_end(b):
        total = run_sum[...]
        pad = jnp.zeros((6, 256), jnp.float32)
        for h in range(2):
            part[b, h, 0:128, :] = acc[h * 128 : h * 128 + 128, :]
            total_h = jnp.sum(jnp.where(sub8 == h, total, 0.0), axis=0, keepdims=True)
            part[b, h, 128:136, :] = jnp.concatenate([top_buf[h : h + 1, :], total_h, pad], axis=0)
        a1(b).start()

    def attend(s):
        b, first = s // 2, s % 2 == 0

        @pl.when(first)
        def _():
            fetch(b)

        @pl.when(first & (b < n_seq))
        def _():
            score_start(b)

        @pl.when(first & (b > 0))
        def _():
            weigh_start(b - 1)

        def tiles(body):
            def one(i, carry):
                body((s % 2) * (n_tiles // 2) + i)
                return carry

            lax.fori_loop(0, n_tiles // 2, one, 0)

        @pl.when(b == 0)
        def _():
            tiles(lambda t: score_tile(b, t))

        @pl.when((b > 0) & (b < n_seq))
        def _():
            def both(t):
                weigh_tile(b - 1, t)
                score_tile(b, t)

            tiles(both)

        @pl.when(b == n_seq)
        def _():
            tiles(lambda t: weigh_tile(b - 1, t))

        @pl.when((s % 2 == 1) & (b > 0))
        def _():
            weigh_end(b - 1)

        @pl.when((s % 2 == 1) & (b < n_seq))
        def _():
            score_end(b)

    def a1(j):
        return send(part.at[j, 1 - core], got1.at[j], a1s.at[j], a1r.at[j], z, mate)

    def a2(j):
        return send(chip.at[j, 1 - y], got2.at[j], a2s.at[j], a2r.at[j], z, over)

    def a3(j, h):
        return send(ob.at[j, h], ob.at[j, h], a3s.at[j], a3r.at[j], z, mate)

    def b_right(j, p):
        return send(prod.at[j, p], from_l.at[j, p], brs.at[j, p], brr.at[j, p], z + 1, c)

    def b_left(j, p):
        return send(prod.at[j, p], from_r.at[j, p], bls.at[j, p], blr.at[j, p], z - 1, c)

    def c_right(j, p):
        return send(full.at[j, c, p], full.at[j, c, p], crs.at[j, p], crr.at[j, p], z + 1, c)

    def c_left(j, p):
        return send(full.at[j, c, p], full.at[j, c, p], cls.at[j, p], clr.at[j, p], z - 1, c)

    def c_over(j, q, p):
        return send(full.at[j, q, p], full.at[j, q, p], cys.at[j, p], cyr.at[j, p], z, over)

    def c_mate(j, q, u, p):
        return send(full.at[j, q, p], full.at[j, q, p], cps.at[j, u, p], cpr.at[j, u, p], z, mate)

    def merge(a, b):
        top = jnp.maximum(a[128:129], b[128:129])
        fa = jnp.exp2((a[128:129] - top) * EXP2_SCALE)
        fb = jnp.exp2((b[128:129] - top) * EXP2_SCALE)
        return a[0:128] * fa + b[0:128] * fb, top, a[129:130] * fa + b[129:130] * fb

    def stage_a1(j):
        a1(j).wait_recv()
        vals, top, total = merge(part[j, core], got1[j])
        for th in range(2):
            sel = slice(128 * th, 128 * th + 128)
            chip[j, th, 0:128] = vals[:, sel]
            chip[j, th, 128:136] = jnp.concatenate([top[:, sel], total[:, sel], jnp.zeros((6, 128), jnp.float32)], axis=0)
        a2(j).start()

    def stage_a2(j):
        a2(j).wait_recv()
        vals, _, total = merge(chip[j, y], got2[j])
        ob[j, core] = (vals / total).T
        a3(j, core).start()

    def stage_a3(j):
        a3(j, 1 - core).wait_recv()

        @pl.when(j == 0)
        def _():
            for p in range(n_part):
                wo_copy(p).wait()

        o = jnp.concatenate([ob[j, h, 32 * g : 32 * g + 32, :] for h in range(2) for g in range(4)], axis=1)
        o = o.astype(jnp.bfloat16)
        for p in range(n_part):
            prod[j, p] = jnp.dot(o, wo[p], preferred_element_type=jnp.float32)

        @pl.when(z == 0)
        def _():
            for p in range(last, 0, -1):
                b_right(j, p).start()

        @pl.when(z == last)
        def _():
            for p in range(last):
                b_left(j, p).start()

    def pass_right(j, p):
        b_right(j, p).wait_recv()
        prod[j, p] = prod[j, p] + from_l[j, p]
        b_right(j, p).start()

    def pass_left(j, p):
        b_left(j, p).wait_recv()
        prod[j, p] = prod[j, p] + from_r[j, p]
        b_left(j, p).start()

    def stage_b1(j):
        @pl.when(z == 1)
        def _():
            pass_right(j, 3)
            pass_right(j, 2)

        @pl.when(z == 2)
        def _():
            pass_left(j, 0)
            pass_left(j, 1)

    def stage_b2(j):
        @pl.when(z == 2)
        def _():
            pass_right(j, 3)

        @pl.when(z == 1)
        def _():
            pass_left(j, 0)

    def stage_c0(j):
        x_copy(j).wait()

        @pl.when(z > 0)
        def _():
            b_right(j, z).wait_recv()
            prod[j, z] = prod[j, z] + from_l[j, z]

        @pl.when(z < last)
        def _():
            b_left(j, z).wait_recv()
            prod[j, z] = prod[j, z] + from_r[j, z]

        full[j, c, z] = prod[j, z] + xs[j].astype(jnp.float32)

        @pl.when(z < last)
        def _():
            c_right(j, z).start()

        @pl.when(z > 0)
        def _():
            c_left(j, z).start()

        c_over(j, c, z).start()
        c_mate(j, c, 0, z).start()

    def stage_c(j, d):
        @pl.when(z - d >= 0)
        def _():
            p = z - d
            c_right(j, p).wait_recv()

            @pl.when(z < last)
            def _():
                c_right(j, p).start()

            c_over(j, c, p).start()
            c_mate(j, c, 0, p).start()

        @pl.when(z + d <= last)
        def _():
            p = z + d
            c_left(j, p).wait_recv()

            @pl.when(z > 0)
            def _():
                c_left(j, p).start()

            c_over(j, c, p).start()
            c_mate(j, c, 0, p).start()

    def stage_over(j):
        for p in range(n_part):
            c_over(j, over, p).wait_recv()
            c_mate(j, over, 1, p).start()

    def stage_out(j):
        for p in range(n_part):
            c_mate(j, mate, 0, p).wait_recv()
            c_mate(j, over_mate, 1, p).wait_recv()
        for q in range(4):
            for p in range(n_part):
                col = width * (n_part * (q % 2) + p)
                rows = pl.ds(pl.multiple_of(64 * j + 32 * (q // 2), 32), 32)
                out_ref[rows, col : col + width] = full[j, q, p].astype(jnp.bfloat16)

    stages = [
        (stage_a1, 1), (stage_a2, 2), (stage_a3, 1), (stage_b1, 3), (stage_b2, 2), (stage_c0, 2),
        (functools.partial(stage_c, d=1), 2), (functools.partial(stage_c, d=2), 3), (functools.partial(stage_c, d=3), 2),
        (stage_over, 5), (stage_out, 5),
    ]
    n_slots = 2 * n_seq + 2 + sum(lag for _, lag in stages)

    def slot(s, carry):
        @pl.when(s < 2 * n_seq + 2)
        def _():
            attend(s)

        after = 3 + sum(lag for _, lag in stages)
        for stage_fn, lag in reversed(stages):
            t = s - after
            after -= lag

            @pl.when((t >= 0) & (t % 2 == 0) & (t < 2 * n_seq))
            def _():
                stage_fn(t // 2)

        return carry

    lax.fori_loop(0, n_slots, slot, 0)

    def drain(j, carry):
        a1(j).wait_send()
        a2(j).wait_send()
        a3(j, core).wait_send()
        for p in range(n_part):
            @pl.when(z < p)
            def _():
                b_right(j, p).wait_send()

            @pl.when(z > p)
            def _():
                b_left(j, p).wait_send()

            @pl.when((z >= p) & (z < last))
            def _():
                c_right(j, p).wait_send()

            @pl.when((z <= p) & (z > 0))
            def _():
                c_left(j, p).wait_send()

            c_over(j, c, p).wait_send()
            c_mate(j, c, 0, p).wait_send()
            c_mate(j, over, 1, p).wait_send()
        return carry

    lax.fori_loop(0, n_seq, drain, 0)


def attend_and_project(prefix_len, q3, kn, vn, kc, vc, x2, w_o):
    rows, d_model = x2.shape
    n_seq, cache_rows, _ = kc.shape
    n_part = 4
    width = d_model // (2 * n_part)
    new_rows = kn.shape[0] // n_seq
    tile = min(2048, cache_rows)
    any_spec = pl.BlockSpec(memory_space=pl.ANY)
    vmem = pl.BlockSpec(memory_space=pltpu.VMEM)
    f32, bf16 = jnp.float32, jnp.bfloat16
    sems = pltpu.SemaphoreType.DMA
    piece = (32, width)
    return pl.pallas_call(
        functools.partial(block_kernel, tile=tile),
        out_shape=pltpu.VMEM((rows, d_model), bf16),
        in_specs=[pl.BlockSpec(memory_space=pltpu.SMEM), vmem, vmem, vmem, any_spec, any_spec, any_spec, any_spec],
        out_specs=vmem,
        scratch_shapes=[
            pltpu.VMEM((2, cache_rows, 128), bf16),
            pltpu.VMEM((2, cache_rows, 128), bf16),
            pltpu.VMEM((256, 256), bf16),
            pltpu.VMEM((cache_rows, 256), f32),
            pltpu.VMEM((new_rows, 256), f32),
            pltpu.VMEM((256, 256), f32),
            pltpu.VMEM((8, 256), f32),
            pltpu.VMEM((8, 256), f32),
            pltpu.VMEM((8, 256), f32),
            pltpu.VMEM((n_part, w_o.shape[0], width), bf16),
            pltpu.VMEM((n_seq, *piece), bf16),
            pltpu.VMEM((n_seq, 2, 136, 256), f32),
            pltpu.VMEM((n_seq, 136, 256), f32),
            pltpu.VMEM((n_seq, 2, 136, 128), f32),
            pltpu.VMEM((n_seq, 136, 128), f32),
            pltpu.VMEM((n_seq, 2, 128, 128), f32),
            pltpu.VMEM((n_seq, n_part, *piece), f32),
            pltpu.VMEM((n_seq, n_part, *piece), f32),
            pltpu.VMEM((n_seq, n_part, *piece), f32),
            pltpu.VMEM((n_seq, 4, n_part, *piece), f32),
            sems((2,)),
            sems((2,)),
            sems((n_part,)),
            sems((n_seq,)),
            *[sems((n_seq,))] * 6,
            *[sems((n_seq, n_part))] * 10,
            sems((n_seq, 2, n_part)),
            sems((n_seq, 2, n_part)),
        ],
        compiler_params=pltpu.CompilerParams(
            collective_id=0, has_side_effects=True, vmem_limit_bytes=57 * 1024 * 1024
        ),
        cost_estimate=pl.CostEstimate(
            flops=4 * n_seq * cache_rows * 256 * 256, bytes_accessed=60 << 20, transcendentals=n_seq * cache_rows * 256
        ),
        name="attend_and_project",
    )(prefix_len, q3, kn, vn, kc, vc, x2, w_o)


def solution(mesh):
    def per_device(hidden, prefix_len, k_cache, v_cache, attn_norm, w_q, w_k, w_v, w_o, q_norm, k_norm):
        n_seq, n_new, d_model = hidden.shape
        x2 = hidden.reshape(n_seq * n_new, d_model)
        q3, k_rows, v_rows = project(prefix_len, x2, attn_norm, w_q, w_k, w_v, q_norm, k_norm)
        out = attend_and_project(
            prefix_len, q3, k_rows, v_rows,
            k_cache.reshape(n_seq, -1, HEAD_DIM), v_cache.reshape(n_seq, -1, HEAD_DIM), x2, w_o,
        )
        new_shape = (n_seq, n_new, 2, HEAD_DIM)
        return out.reshape(hidden.shape), k_rows.reshape(new_shape), v_rows.reshape(new_shape)

    cache_spec = P("dp", "cp", "tp", None)
    arg_specs = (P("dp", None, None), P("dp"), cache_spec, cache_spec, P(None), P(None, "tp"), P(None, "tp"), P(None, "tp"), P("tp", None), P(None), P(None))
    out_specs = (P("dp", None, None), P("dp", None, "tp", None), P("dp", None, "tp", None))
    return jax.shard_map(per_device, mesh=mesh, in_specs=arg_specs, out_specs=out_specs, check_vma=False)
```

```python
import functools

import jax
import jax.numpy as jnp
import numpy as np
from jax import lax
from jax.experimental import pallas as pl
from jax.experimental.pallas import tpu as pltpu
from jax.sharding import PartitionSpec as P

HEAD_DIM = 128
MASKED = -1e30
EXP2_SCALE = HEAD_DIM**-0.5 * 1.4426950408889634
MESH = pl.DeviceIdType.MESH


def block_kernel(
    len_ref, gain, q_gain, k_gain, freq, x_hbm, wq_hbm, wk_hbm, wv_hbm, kc_hbm, vc_hbm, wo_hbm,
    out_ref, kn_ref, vn_ref,
    q_ref, w_buf, cos_t, sin_t, turn, kbuf, vbuf, qt, s_buf, sn_buf, acc, top_buf, run_top, run_sum,
    wo, xs, part, got1, chip, got2, ob, prod, from_l, from_r, full,
    x_sem, w_sem, k_sem, v_sem, wo_sem, xs_sem, a1s, a1r, a2s, a2r, a3s, a3r,
    brs, brr, bls, blr, crs, crr, cls, clr, cys, cyr, cps, cpr, *, tile,
):
    dp, z, c = lax.axis_index("dp"), lax.axis_index("tp"), lax.axis_index("cp")
    y, core = c // 2, c % 2
    mate = 2 * y + (1 - core)
    over = 2 * (1 - y) + core
    over_mate = 2 * (1 - y) + (1 - core)
    n_seq, n_part, width = full.shape[0], full.shape[2], full.shape[4]
    last = n_part - 1
    cache_rows = kbuf.shape[1]
    n_new = kn_ref.shape[0] // n_seq
    n_tok = n_new // 2
    n_tiles = cache_rows // tile
    rows, d_model = out_ref.shape
    half_rows = rows // 2
    n_q = wq_hbm.shape[1] // 256

    def send(src, dst, send_sem, recv_sem, tp, cp):
        return pltpu.make_async_remote_copy(
            src_ref=src, dst_ref=dst, send_sem=send_sem, recv_sem=recv_sem, device_id=(dp, tp, cp), device_id_type=MESH
        )

    def k_copy(b):
        return pltpu.make_async_copy(kc_hbm.at[b], kbuf.at[b % 2], k_sem.at[b % 2])

    def v_copy(b):
        return pltpu.make_async_copy(vc_hbm.at[b], vbuf.at[b % 2], v_sem.at[b % 2])

    def wo_copy(p):
        cols = pl.ds(pl.multiple_of(n_part * width * core + width * p, width), width)
        return pltpu.make_async_copy(wo_hbm.at[:, cols], wo.at[p], wo_sem.at[p])

    def x_copy(j):
        rows = pl.ds(pl.multiple_of(64 * j + 32 * y, 32), 32)
        cols = pl.ds(pl.multiple_of(n_part * width * core + width * z, width), width)
        return pltpu.make_async_copy(x_hbm.at[rows, cols], xs.at[j], xs_sem.at[j])

    def in_copy(half):
        sel = pl.ds(half_rows * half, half_rows)
        return pltpu.make_async_copy(x_hbm.at[sel], out_ref.at[sel], x_sem.at[half])

    w_copies = [
        pltpu.make_async_copy(wq_hbm.at[:, pl.ds(256 * i, 256)], w_buf.at[i], w_sem.at[i]) for i in range(n_q)
    ]
    w_copies.append(pltpu.make_async_copy(wk_hbm, w_buf.at[n_q], w_sem.at[n_q]))
    w_copies.append(pltpu.make_async_copy(wv_hbm, w_buf.at[n_q + 1], w_sem.at[n_q + 1]))
    in_copy(0).start()

    barrier = pltpu.get_barrier_semaphore()
    for peer in (mate, over):
        pl.semaphore_signal(barrier, inc=1, device_id=(dp, z, peer), device_id_type=MESH)

    @pl.when(z > 0)
    def _():
        pl.semaphore_signal(barrier, inc=1, device_id=(dp, z - 1, c), device_id_type=MESH)

    @pl.when(z < last)
    def _():
        pl.semaphore_signal(barrier, inc=1, device_id=(dp, z + 1, c), device_id_type=MESH)

    rope_lane = lax.broadcasted_iota(jnp.int32, (n_tok, 128), 1)
    rope_token = lax.broadcasted_iota(jnp.int32, (n_tok, 128), 0)

    def rope_rows(b, carry):
        angle = (rope_token + len_ref[b]).astype(jnp.float32) * freq[...]
        sel = pl.ds(pl.multiple_of(b * (n_tok), n_tok), n_tok)
        cos_t[sel, :] = jnp.cos(angle)
        sin = jnp.sin(angle)
        sin_t[sel, :] = jnp.where(rope_lane < 64, -sin, sin)
        return carry

    lax.fori_loop(0, n_seq, rope_rows, 0)
    x_gain = gain[...].astype(jnp.float32).reshape(1, d_model)

    def norm_half(half):
        def norm_rows(i, carry):
            sel = pl.ds(pl.multiple_of(half * half_rows + i * 32, 32), 32)
            x = out_ref[sel, :].astype(jnp.float32)
            mean_sq = jnp.mean(x * x, axis=-1, keepdims=True)
            out_ref[sel, :] = (x * lax.rsqrt(mean_sq + 1e-6) * x_gain).astype(jnp.bfloat16)
            return carry

        lax.fori_loop(0, half_rows // 32, norm_rows, 0)

    q_gain_row = q_gain[...].astype(jnp.float32).reshape(1, 128)
    k_gain_row = k_gain[...].astype(jnp.float32).reshape(1, 128)

    def project_tile(i, half):
        sel = slice(half * half_rows, (half + 1) * half_rows)
        lin = jnp.dot(out_ref[sel, :], w_buf[i], preferred_element_type=jnp.float32).astype(jnp.bfloat16)
        lin = lin.astype(jnp.float32)
        head_gain = jnp.where(i < n_q, q_gain_row, k_gain_row)
        for u in range(2):
            raw = lin[:, 128 * u : 128 * u + 128]
            mean_sq = jnp.mean(raw * raw, axis=-1, keepdims=True)
            t = raw * lax.rsqrt(mean_sq + 1e-6) * head_gain
            t = t * cos_t[sel, :] + pltpu.roll(t, 64, 1) * sin_t[sel, :]

            @pl.when(i < n_q)
            def _():
                q_ref[i, sel, 128 * u : 128 * u + 128] = t.astype(jnp.bfloat16)

            @pl.when(i >= n_q)
            def _():
                turn[pl.ds(u, half_rows, stride=2), :] = jnp.where(i == n_q, t, raw)

        new_rows = slice(half * rows, (half + 1) * rows)

        @pl.when(i == n_q)
        def _():
            kn_ref[new_rows, :] = turn[...].astype(jnp.bfloat16)

        @pl.when(i == n_q + 1)
        def _():
            vn_ref[new_rows, :] = turn[...].astype(jnp.bfloat16)

    in_copy(0).wait()
    for copy in w_copies:
        copy.start()
    norm_half(0)
    k_copy(0).start()
    in_copy(1).start()

    def first_tile(i, carry):
        pltpu.make_async_copy(w_buf.at[i], w_buf.at[i], w_sem.at[i]).wait()
        project_tile(i, 0)
        return carry

    lax.fori_loop(0, n_q + 2, first_tile, 0)
    v_copy(0).start()
    for p in range(n_part):
        wo_copy(p).start()
    for j in range(n_seq):
        x_copy(j).start()

    @pl.when((z == 0) | (z == last))
    def _():
        pl.semaphore_wait(barrier, 3)

    @pl.when((z > 0) & (z < last))
    def _():
        pl.semaphore_wait(barrier, 4)

    sub16 = lax.broadcasted_iota(jnp.int32, (16, 128), 0) & 1
    even_rows = jnp.where(sub16 == 0, 1.0, 0.0).astype(jnp.bfloat16)
    odd_rows = jnp.where(sub16 == 0, 0.0, 1.0).astype(jnp.bfloat16)
    sub8 = lax.broadcasted_iota(jnp.int32, (8, 256), 0) & 1

    def split_rows(k):
        n = k.shape[0]
        k3 = k.reshape(n // 16, 16, 128)
        return jnp.concatenate(
            [(k3 * even_rows[None]).reshape(n, 128), (k3 * odd_rows[None]).reshape(n, 128)], axis=1
        )

    def split_lanes(v):
        n = v.shape[0]
        lane = lax.broadcasted_iota(jnp.int32, (16, n), 1) & 1
        even = jnp.where(lane == 0, 1.0, 0.0).astype(jnp.bfloat16)
        odd = jnp.where(lane == 0, 0.0, 1.0).astype(jnp.bfloat16)
        vt = v.T.reshape(8, 16, n)
        return jnp.concatenate([(vt * even[None]).reshape(128, n), (vt * odd[None]).reshape(128, n)], axis=0)

    def scores(k):
        return jnp.dot(split_rows(k), qt[...], preferred_element_type=jnp.float32)

    def fetch(b):
        @pl.when(b + 1 < n_seq)
        def _():
            k_copy(b + 1).start()

        @pl.when((b > 0) & (b < n_seq))
        def _():
            v_copy(b).start()

    def score_start(b):
        q_rows = pl.multiple_of(64 * b, 64)
        for h in range(2):
            blocks = [
                q_ref[h * 2 + g // 2, pl.ds(q_rows + th * 32, 32), (g % 2) * 128 : (g % 2) * 128 + 128]
                for th in range(2)
                for g in range(4)
            ]
            qt[h * 128 : h * 128 + 128, :] = jnp.concatenate(blocks, axis=0).T
        run_top[...] = jnp.full((8, 256), MASKED, jnp.float32)
        k_copy(b).wait()

    def score_tile(b, t):
        sel = pl.ds(pl.multiple_of(t * tile, tile), tile)
        n_rows = 2 * (len_ref[b] - c * (cache_rows // 2)) - t * tile
        s = scores(kbuf[b % 2, sel, :])
        s = jnp.where(lax.broadcasted_iota(jnp.int32, (tile, 256), 0) < n_rows, s, MASKED)
        s_buf[sel, :] = s
        run_top[...] = jnp.maximum(run_top[...], jnp.max(s.reshape(tile // 8, 8, 256), axis=0))

    def score_end(b):
        key = lax.broadcasted_iota(jnp.int32, (n_new, 256), 0) // 2
        col = lax.broadcasted_iota(jnp.int32, (n_new, 256), 1)
        token = (col // 128) * 32 + (col % 32)
        token = jnp.where(c == 3, token, -1)
        s_new = jnp.where(key <= token, scores(kn_ref[pl.ds(pl.multiple_of(n_new * b, n_new), n_new), :]), MASKED)
        sn_buf[...] = s_new
        top = jnp.maximum(run_top[...], jnp.max(s_new.reshape(n_new // 8, 8, 256), axis=0))
        top0 = jnp.max(jnp.where(sub8 == 0, top, MASKED), axis=0, keepdims=True)
        top1 = jnp.max(jnp.where(sub8 == 0, MASKED, top), axis=0, keepdims=True)
        top_buf[...] = jnp.where(sub8 == 0, top0, top1)

    def weigh(s, v):
        top = top_buf[...]
        base = jnp.where(top > 0.5 * MASKED, top, 0.0)
        n = s.shape[0]
        p = jnp.exp2((s.reshape(n // 8, 8, 256) - base[None]) * EXP2_SCALE)
        out = jnp.dot(split_lanes(v), p.reshape(n, 256).astype(jnp.bfloat16), preferred_element_type=jnp.float32)
        return jnp.sum(p, axis=0), out

    def weigh_start(b):
        run_sum[...], acc[...] = weigh(sn_buf[...], vn_ref[pl.ds(pl.multiple_of(n_new * b, n_new), n_new), :])
        v_copy(b).wait()

    def weigh_tile(b, t):
        sel = pl.ds(pl.multiple_of(t * tile, tile), tile)
        more, out = weigh(s_buf[sel, :], vbuf[b % 2, sel, :])
        acc[...] += out
        run_sum[...] += more

    def weigh_end(b):
        total = run_sum[...]
        pad = jnp.zeros((6, 256), jnp.float32)
        for h in range(2):
            part[b, h, 0:128, :] = acc[h * 128 : h * 128 + 128, :]
            total_h = jnp.sum(jnp.where(sub8 == h, total, 0.0), axis=0, keepdims=True)
            part[b, h, 128:136, :] = jnp.concatenate([top_buf[h : h + 1, :], total_h, pad], axis=0)
        a1(b).start()

    def attend(s):
        b, first = s // 2, s % 2 == 0

        @pl.when(first)
        def _():
            fetch(b)

        @pl.when(first & (b < n_seq))
        def _():
            score_start(b)

        @pl.when(first & (b > 0))
        def _():
            weigh_start(b - 1)

        def tiles(body):
            def one(i, carry):
                body((s % 2) * (n_tiles // 2) + i)
                return carry

            lax.fori_loop(0, n_tiles // 2, one, 0)

        @pl.when(b == 0)
        def _():
            tiles(lambda t: score_tile(b, t))

        @pl.when((b > 0) & (b < n_seq))
        def _():
            def both(t):
                weigh_tile(b - 1, t)
                score_tile(b, t)

            tiles(both)

        @pl.when(b == n_seq)
        def _():
            tiles(lambda t: weigh_tile(b - 1, t))

        @pl.when((s % 2 == 1) & (b > 0))
        def _():
            weigh_end(b - 1)

        @pl.when((s % 2 == 1) & (b < n_seq))
        def _():
            score_end(b)

    def a1(j):
        return send(part.at[j, 1 - core], got1.at[j], a1s.at[j], a1r.at[j], z, mate)

    def a2(j):
        return send(chip.at[j, 1 - y], got2.at[j], a2s.at[j], a2r.at[j], z, over)

    def a3(j, h):
        return send(ob.at[j, h], ob.at[j, h], a3s.at[j], a3r.at[j], z, mate)

    def b_right(j, p):
        return send(prod.at[j, p], from_l.at[j, p], brs.at[j, p], brr.at[j, p], z + 1, c)

    def b_left(j, p):
        return send(prod.at[j, p], from_r.at[j, p], bls.at[j, p], blr.at[j, p], z - 1, c)

    def c_right(j, p):
        return send(full.at[j, c, p], full.at[j, c, p], crs.at[j, p], crr.at[j, p], z + 1, c)

    def c_left(j, p):
        return send(full.at[j, c, p], full.at[j, c, p], cls.at[j, p], clr.at[j, p], z - 1, c)

    def c_over(j, q, p):
        return send(full.at[j, q, p], full.at[j, q, p], cys.at[j, p], cyr.at[j, p], z, over)

    def c_mate(j, q, u, p):
        return send(full.at[j, q, p], full.at[j, q, p], cps.at[j, u, p], cpr.at[j, u, p], z, mate)

    def merge(a, b):
        top = jnp.maximum(a[128:129], b[128:129])
        fa = jnp.exp2((a[128:129] - top) * EXP2_SCALE)
        fb = jnp.exp2((b[128:129] - top) * EXP2_SCALE)
        return a[0:128] * fa + b[0:128] * fb, top, a[129:130] * fa + b[129:130] * fb

    def stage_a1(j):
        a1(j).wait_recv()
        vals, top, total = merge(part[j, core], got1[j])
        for th in range(2):
            sel = slice(128 * th, 128 * th + 128)
            chip[j, th, 0:128] = vals[:, sel]
            chip[j, th, 128:136] = jnp.concatenate([top[:, sel], total[:, sel], jnp.zeros((6, 128), jnp.float32)], axis=0)
        a2(j).start()

    def stage_a2(j):
        a2(j).wait_recv()
        vals, _, total = merge(chip[j, y], got2[j])
        ob[j, core] = (vals / total).T
        a3(j, core).start()

    def stage_a3(j):
        a3(j, 1 - core).wait_recv()

        @pl.when(j == 0)
        def _():
            for p in range(n_part):
                wo_copy(p).wait()

        o = jnp.concatenate([ob[j, h, 32 * g : 32 * g + 32, :] for h in range(2) for g in range(4)], axis=1)
        o = o.astype(jnp.bfloat16)
        for p in range(n_part):
            prod[j, p] = jnp.dot(o, wo[p], preferred_element_type=jnp.float32)

        @pl.when(z == 0)
        def _():
            for p in range(last, 0, -1):
                b_right(j, p).start()

        @pl.when(z == last)
        def _():
            for p in range(last):
                b_left(j, p).start()

    def pass_right(j, p):
        b_right(j, p).wait_recv()
        prod[j, p] = prod[j, p] + from_l[j, p]
        b_right(j, p).start()

    def pass_left(j, p):
        b_left(j, p).wait_recv()
        prod[j, p] = prod[j, p] + from_r[j, p]
        b_left(j, p).start()

    def stage_b1(j):
        @pl.when(z == 1)
        def _():
            pass_right(j, 3)
            pass_right(j, 2)

        @pl.when(z == 2)
        def _():
            pass_left(j, 0)
            pass_left(j, 1)

    def stage_b2(j):
        @pl.when(z == 2)
        def _():
            pass_right(j, 3)

        @pl.when(z == 1)
        def _():
            pass_left(j, 0)

    def stage_c0(j):
        x_copy(j).wait()

        @pl.when(z > 0)
        def _():
            b_right(j, z).wait_recv()
            prod[j, z] = prod[j, z] + from_l[j, z]

        @pl.when(z < last)
        def _():
            b_left(j, z).wait_recv()
            prod[j, z] = prod[j, z] + from_r[j, z]

        full[j, c, z] = prod[j, z] + xs[j].astype(jnp.float32)

        @pl.when(z < last)
        def _():
            c_right(j, z).start()

        @pl.when(z > 0)
        def _():
            c_left(j, z).start()

        c_over(j, c, z).start()
        c_mate(j, c, 0, z).start()

    def stage_c(j, d):
        @pl.when(z - d >= 0)
        def _():
            p = z - d
            c_right(j, p).wait_recv()

            @pl.when(z < last)
            def _():
                c_right(j, p).start()

            c_over(j, c, p).start()
            c_mate(j, c, 0, p).start()

        @pl.when(z + d <= last)
        def _():
            p = z + d
            c_left(j, p).wait_recv()

            @pl.when(z > 0)
            def _():
                c_left(j, p).start()

            c_over(j, c, p).start()
            c_mate(j, c, 0, p).start()

    def stage_over(j):
        for p in range(n_part):
            c_over(j, over, p).wait_recv()
            c_mate(j, over, 1, p).start()

    def stage_out(j):
        for p in range(n_part):
            c_mate(j, mate, 0, p).wait_recv()
            c_mate(j, over_mate, 1, p).wait_recv()
        for q in range(4):
            for p in range(n_part):
                col = width * (n_part * (q % 2) + p)
                rows = pl.ds(pl.multiple_of(64 * j + 32 * (q // 2), 32), 32)
                out_ref[rows, col : col + width] = full[j, q, p].astype(jnp.bfloat16)

    stages = [
        (stage_a1, 1), (stage_a2, 2), (stage_a3, 1), (stage_b1, 3), (stage_b2, 2), (stage_c0, 2),
        (functools.partial(stage_c, d=1), 2), (functools.partial(stage_c, d=2), 3), (functools.partial(stage_c, d=3), 2),
        (stage_over, 5), (stage_out, 5),
    ]
    n_slots = 2 * n_seq + 2 + sum(lag for _, lag in stages)

    def slot(s, carry):
        @pl.when(s == 1)
        def _():
            in_copy(1).wait()
            norm_half(1)

        @pl.when((s >= 2) & (s < n_q + 4))
        def _():
            project_tile(s - 2, 1)

        @pl.when(s < 2 * n_seq + 2)
        def _():
            attend(s)

        after = 3 + sum(lag for _, lag in stages)
        for stage_fn, lag in reversed(stages):
            t = s - after
            after -= lag

            @pl.when((t >= 0) & (t % 2 == 0) & (t < 2 * n_seq))
            def _():
                stage_fn(t // 2)

        return carry

    lax.fori_loop(0, n_slots, slot, 0)

    def drain(j, carry):
        a1(j).wait_send()
        a2(j).wait_send()
        a3(j, core).wait_send()
        for p in range(n_part):
            @pl.when(z < p)
            def _():
                b_right(j, p).wait_send()

            @pl.when(z > p)
            def _():
                b_left(j, p).wait_send()

            @pl.when((z >= p) & (z < last))
            def _():
                c_right(j, p).wait_send()

            @pl.when((z <= p) & (z > 0))
            def _():
                c_left(j, p).wait_send()

            c_over(j, c, p).wait_send()
            c_mate(j, c, 0, p).wait_send()
            c_mate(j, over, 1, p).wait_send()
        return carry

    lax.fori_loop(0, n_seq, drain, 0)


def block(prefix_len, gain, q_gain, k_gain, x2, w_q, w_k, w_v, kc, vc, w_o):
    rows, d_model = x2.shape
    n_seq, cache_rows, _ = kc.shape
    n_part = 4
    width = d_model // (2 * n_part)
    n_q = w_q.shape[1] // 256
    new_rows = 2 * rows // n_seq
    tile = min(2048, cache_rows // 2)
    half_dim = HEAD_DIM // 2
    freq = 1.0 / (1000000.0 ** (np.arange(half_dim, dtype=np.float64) * 2.0 / HEAD_DIM))
    freq = jnp.asarray(np.concatenate([freq, freq])[None], jnp.float32)
    hbm = pl.BlockSpec(memory_space=pl.ANY)
    vmem = pl.BlockSpec(memory_space=pltpu.VMEM)
    f32, bf16 = jnp.float32, jnp.bfloat16
    sems = pltpu.SemaphoreType.DMA
    piece = (32, width)
    return pl.pallas_call(
        functools.partial(block_kernel, tile=tile),
        out_shape=(
            pltpu.VMEM((rows, d_model), bf16),
            pltpu.VMEM((2 * rows, 128), bf16),
            pltpu.VMEM((2 * rows, 128), bf16),
        ),
        in_specs=[pl.BlockSpec(memory_space=pltpu.SMEM), vmem, vmem, vmem, vmem, hbm, hbm, hbm, hbm, hbm, hbm, hbm],
        out_specs=(vmem, vmem, vmem),
        scratch_shapes=[
            pltpu.VMEM((n_q, rows, 256), bf16),
            pltpu.VMEM((n_q + 2, d_model, 256), bf16),
            pltpu.VMEM((rows, 128), f32),
            pltpu.VMEM((rows, 128), f32),
            pltpu.VMEM((rows, 128), f32),
            pltpu.VMEM((2, cache_rows, 128), bf16),
            pltpu.VMEM((2, cache_rows, 128), bf16),
            pltpu.VMEM((256, 256), bf16),
            pltpu.VMEM((cache_rows, 256), f32),
            pltpu.VMEM((new_rows, 256), f32),
            pltpu.VMEM((256, 256), f32),
            pltpu.VMEM((8, 256), f32),
            pltpu.VMEM((8, 256), f32),
            pltpu.VMEM((8, 256), f32),
            pltpu.VMEM((n_part, w_o.shape[0], width), bf16),
            pltpu.VMEM((n_seq, *piece), bf16),
            pltpu.VMEM((n_seq, 2, 136, 256), f32),
            pltpu.VMEM((n_seq, 136, 256), f32),
            pltpu.VMEM((n_seq, 2, 136, 128), f32),
            pltpu.VMEM((n_seq, 136, 128), f32),
            pltpu.VMEM((n_seq, 2, 128, 128), f32),
            pltpu.VMEM((n_seq, n_part, *piece), f32),
            pltpu.VMEM((n_seq, n_part, *piece), f32),
            pltpu.VMEM((n_seq, n_part, *piece), f32),
            pltpu.VMEM((n_seq, 4, n_part, *piece), f32),
            sems((2,)),
            sems((n_q + 2,)),
            sems((2,)),
            sems((2,)),
            sems((n_part,)),
            sems((n_seq,)),
            *[sems((n_seq,))] * 6,
            *[sems((n_seq, n_part))] * 10,
            sems((n_seq, 2, n_part)),
            sems((n_seq, 2, n_part)),
        ],
        compiler_params=pltpu.CompilerParams(
            collective_id=0, has_side_effects=True, vmem_limit_bytes=int(58.5 * 1024 * 1024)
        ),
        cost_estimate=pl.CostEstimate(
            flops=4 * n_seq * cache_rows * 256 * 256, bytes_accessed=60 << 20, transcendentals=n_seq * cache_rows * 256
        ),
        name="block",
    )(prefix_len, gain, q_gain, k_gain, freq, x2, w_q, w_k, w_v, kc, vc, w_o)


def solution(mesh):
    def per_device(hidden, prefix_len, k_cache, v_cache, attn_norm, w_q, w_k, w_v, w_o, q_norm, k_norm):
        n_seq, n_new, d_model = hidden.shape
        x2 = hidden.reshape(n_seq * n_new, d_model)
        out, k_rows, v_rows = block(
            prefix_len, attn_norm, q_norm, k_norm, x2, w_q, w_k, w_v,
            k_cache.reshape(n_seq, -1, HEAD_DIM), v_cache.reshape(n_seq, -1, HEAD_DIM), w_o,
        )
        new_shape = (n_seq, n_new, 2, HEAD_DIM)
        return out.reshape(hidden.shape), k_rows.reshape(new_shape), v_rows.reshape(new_shape)

    cache_spec = P("dp", "cp", "tp", None)
    arg_specs = (P("dp", None, None), P("dp"), cache_spec, cache_spec, P(None), P(None, "tp"), P(None, "tp"), P(None, "tp"), P("tp", None), P(None), P(None))
    out_specs = (P("dp", None, None), P("dp", None, "tp", None), P("dp", None, "tp", None))
    return jax.shard_map(per_device, mesh=mesh, in_specs=arg_specs, out_specs=out_specs, check_vma=False)
```

```python
import functools

import jax
import jax.numpy as jnp
import numpy as np
from jax import lax
from jax.experimental import pallas as pl
from jax.experimental.pallas import tpu as pltpu
from jax.sharding import PartitionSpec as P

HEAD_DIM = 128
MASKED = -1e30
EXP2_SCALE = HEAD_DIM**-0.5 * 1.4426950408889634
MESH = pl.DeviceIdType.MESH


def block_kernel(
    len_ref, gain, q_gain, k_gain, freq, x_hbm, wq_hbm, wk_hbm, wv_hbm, kc_hbm, vc_hbm, wo_hbm,
    out_ref, kn_ref, vn_ref,
    q_ref, w_buf, cos_t, sin_t, turn, kbuf, vbuf, qt, s_buf, sn_buf, acc, top_buf, run_top, run_sum,
    wo, xs, part, got1, chip, got2, ob, prod, from_l, from_r, full,
    x_sem, w_sem, k_sem, v_sem, wo_sem, xs_sem, a1s, a1r, a2s, a2r, a3s, a3r,
    brs, brr, bls, blr, crs, crr, cls, clr, cys, cyr, cps, cpr, *, tile,
):
    dp, z, c = lax.axis_index("dp"), lax.axis_index("tp"), lax.axis_index("cp")
    y, core = c // 2, c % 2
    mate = 2 * y + (1 - core)
    over = 2 * (1 - y) + core
    over_mate = 2 * (1 - y) + (1 - core)
    n_seq, n_part, width = full.shape[0], full.shape[2], full.shape[4]
    last = n_part - 1
    cache_rows = kbuf.shape[1]
    n_new = kn_ref.shape[0] // n_seq
    n_tok = n_new // 2
    n_tiles = cache_rows // tile
    rows, d_model = out_ref.shape
    half_rows = rows // 2
    n_q = wq_hbm.shape[1] // 256

    def send(src, dst, send_sem, recv_sem, tp, cp):
        return pltpu.make_async_remote_copy(
            src_ref=src, dst_ref=dst, send_sem=send_sem, recv_sem=recv_sem, device_id=(dp, tp, cp), device_id_type=MESH
        )

    def k_copy(b):
        return pltpu.make_async_copy(kc_hbm.at[b], kbuf.at[b % 2], k_sem.at[b % 2])

    def v_copy(b):
        return pltpu.make_async_copy(vc_hbm.at[b], vbuf.at[b % 2], v_sem.at[b % 2])

    def wo_copy(p):
        cols = pl.ds(pl.multiple_of(n_part * width * core + width * p, width), width)
        return pltpu.make_async_copy(wo_hbm.at[:, cols], wo.at[p], wo_sem.at[p])

    def x_copy(j):
        rows = pl.ds(pl.multiple_of(64 * j + 32 * y, 32), 32)
        cols = pl.ds(pl.multiple_of(n_part * width * core + width * z, width), width)
        return pltpu.make_async_copy(x_hbm.at[rows, cols], xs.at[j], xs_sem.at[j])

    def in_copy(half):
        sel = pl.ds(half_rows * half, half_rows)
        return pltpu.make_async_copy(x_hbm.at[sel], out_ref.at[sel], x_sem.at[half])

    w_copies = [
        pltpu.make_async_copy(wq_hbm.at[:, pl.ds(256 * i, 256)], w_buf.at[i], w_sem.at[i]) for i in range(n_q)
    ]
    w_copies.append(pltpu.make_async_copy(wk_hbm, w_buf.at[n_q], w_sem.at[n_q]))
    w_copies.append(pltpu.make_async_copy(wv_hbm, w_buf.at[n_q + 1], w_sem.at[n_q + 1]))
    in_copy(0).start()

    barrier = pltpu.get_barrier_semaphore()
    for peer in (mate, over):
        pl.semaphore_signal(barrier, inc=1, device_id=(dp, z, peer), device_id_type=MESH)

    @pl.when(z > 0)
    def _():
        pl.semaphore_signal(barrier, inc=1, device_id=(dp, z - 1, c), device_id_type=MESH)

    @pl.when(z < last)
    def _():
        pl.semaphore_signal(barrier, inc=1, device_id=(dp, z + 1, c), device_id_type=MESH)

    rope_lane = lax.broadcasted_iota(jnp.int32, (n_tok, 128), 1)
    rope_token = lax.broadcasted_iota(jnp.int32, (n_tok, 128), 0)

    def rope_rows(b, carry):
        angle = (rope_token + len_ref[b]).astype(jnp.float32) * freq[...]
        sel = pl.ds(pl.multiple_of(b * (n_tok), n_tok), n_tok)
        cos_t[sel, :] = jnp.cos(angle)
        sin = jnp.sin(angle)
        sin_t[sel, :] = jnp.where(rope_lane < 64, -sin, sin)
        return carry

    lax.fori_loop(0, n_seq, rope_rows, 0)
    x_gain = gain[...].astype(jnp.float32).reshape(1, d_model)

    def norm_half(half):
        def norm_rows(i, carry):
            sel = pl.ds(pl.multiple_of(half * half_rows + i * 32, 32), 32)
            x = out_ref[sel, :].astype(jnp.float32)
            mean_sq = jnp.mean(x * x, axis=-1, keepdims=True)
            out_ref[sel, :] = (x * lax.rsqrt(mean_sq + 1e-6) * x_gain).astype(jnp.bfloat16)
            return carry

        lax.fori_loop(0, half_rows // 32, norm_rows, 0)

    q_gain_row = q_gain[...].astype(jnp.float32).reshape(1, 128)
    k_gain_row = k_gain[...].astype(jnp.float32).reshape(1, 128)

    def project_tile(i, half):
        sel = slice(half * half_rows, (half + 1) * half_rows)
        lin = jnp.dot(out_ref[sel, :], w_buf[i], preferred_element_type=jnp.float32).astype(jnp.bfloat16)
        lin = lin.astype(jnp.float32)
        head_gain = jnp.where(i < n_q, q_gain_row, k_gain_row)
        for u in range(2):
            raw = lin[:, 128 * u : 128 * u + 128]
            mean_sq = jnp.mean(raw * raw, axis=-1, keepdims=True)
            t = raw * lax.rsqrt(mean_sq + 1e-6) * head_gain
            t = t * cos_t[sel, :] + pltpu.roll(t, 64, 1) * sin_t[sel, :]

            @pl.when(i < n_q)
            def _():
                q_ref[i, sel, 128 * u : 128 * u + 128] = t.astype(jnp.bfloat16)

            @pl.when(i >= n_q)
            def _():
                turn[pl.ds(u, half_rows, stride=2), :] = jnp.where(i == n_q, t, raw)

        new_rows = slice(half * rows, (half + 1) * rows)

        @pl.when(i == n_q)
        def _():
            kn_ref[new_rows, :] = turn[...].astype(jnp.bfloat16)

        @pl.when(i == n_q + 1)
        def _():
            vn_ref[new_rows, :] = turn[...].astype(jnp.bfloat16)

    in_copy(0).wait()
    for copy in w_copies:
        copy.start()
    norm_half(0)
    k_copy(0).start()
    in_copy(1).start()

    def first_tile(i, carry):
        pltpu.make_async_copy(w_buf.at[i], w_buf.at[i], w_sem.at[i]).wait()
        project_tile(i, 0)
        return carry

    lax.fori_loop(0, n_q + 2, first_tile, 0)
    v_copy(0).start()
    for p in range(n_part):
        wo_copy(p).start()
    for j in range(n_seq):
        x_copy(j).start()

    @pl.when((z == 0) | (z == last))
    def _():
        pl.semaphore_wait(barrier, 3)

    @pl.when((z > 0) & (z < last))
    def _():
        pl.semaphore_wait(barrier, 4)

    sub16 = lax.broadcasted_iota(jnp.int32, (16, 128), 0) & 1
    even_rows = jnp.where(sub16 == 0, 1.0, 0.0).astype(jnp.bfloat16)
    odd_rows = jnp.where(sub16 == 0, 0.0, 1.0).astype(jnp.bfloat16)
    sub8 = lax.broadcasted_iota(jnp.int32, (8, 256), 0) & 1

    def split_rows(k):
        n = k.shape[0]
        k3 = k.reshape(n // 16, 16, 128)
        return jnp.concatenate(
            [(k3 * even_rows[None]).reshape(n, 128), (k3 * odd_rows[None]).reshape(n, 128)], axis=1
        )

    def split_lanes(v):
        n = v.shape[0]
        lane = lax.broadcasted_iota(jnp.int32, (16, n), 1) & 1
        even = jnp.where(lane == 0, 1.0, 0.0).astype(jnp.bfloat16)
        odd = jnp.where(lane == 0, 0.0, 1.0).astype(jnp.bfloat16)
        vt = v.T.reshape(8, 16, n)
        return jnp.concatenate([(vt * even[None]).reshape(128, n), (vt * odd[None]).reshape(128, n)], axis=0)

    def scores(k):
        return jnp.dot(split_rows(k), qt[...], preferred_element_type=jnp.float32)

    def fetch(b):
        @pl.when(b + 1 < n_seq)
        def _():
            k_copy(b + 1).start()

        @pl.when((b > 0) & (b < n_seq))
        def _():
            v_copy(b).start()

    def score_start(b):
        q_rows = pl.multiple_of(64 * b, 64)
        for h in range(2):
            blocks = [
                q_ref[h * 2 + g // 2, pl.ds(q_rows + th * 32, 32), (g % 2) * 128 : (g % 2) * 128 + 128]
                for th in range(2)
                for g in range(4)
            ]
            qt[h * 128 : h * 128 + 128, :] = jnp.concatenate(blocks, axis=0).T
        run_top[...] = jnp.full((8, 256), MASKED, jnp.float32)
        k_copy(b).wait()

    def score_tile(b, t):
        sel = pl.ds(pl.multiple_of(t * tile, tile), tile)
        n_rows = 2 * (len_ref[b] - c * (cache_rows // 2)) - t * tile
        s = scores(kbuf[b % 2, sel, :])
        s = jnp.where(lax.broadcasted_iota(jnp.int32, (tile, 256), 0) < n_rows, s, MASKED)
        s_buf[sel, :] = s
        run_top[...] = jnp.maximum(run_top[...], jnp.max(s.reshape(tile // 8, 8, 256), axis=0))

    def score_end(b):
        key = lax.broadcasted_iota(jnp.int32, (n_new, 256), 0) // 2
        col = lax.broadcasted_iota(jnp.int32, (n_new, 256), 1)
        token = (col // 128) * 32 + (col % 32)
        token = jnp.where(c == 3, token, -1)
        s_new = jnp.where(key <= token, scores(kn_ref[pl.ds(pl.multiple_of(n_new * b, n_new), n_new), :]), MASKED)
        sn_buf[...] = s_new
        top = jnp.maximum(run_top[...], jnp.max(s_new.reshape(n_new // 8, 8, 256), axis=0))
        top0 = jnp.max(jnp.where(sub8 == 0, top, MASKED), axis=0, keepdims=True)
        top1 = jnp.max(jnp.where(sub8 == 0, MASKED, top), axis=0, keepdims=True)
        top_buf[...] = jnp.where(sub8 == 0, top0, top1)

    def weigh(s, v):
        top = top_buf[...]
        base = jnp.where(top > 0.5 * MASKED, top, 0.0)
        n = s.shape[0]
        p = jnp.exp2((s.reshape(n // 8, 8, 256) - base[None]) * EXP2_SCALE)
        out = jnp.dot(split_lanes(v), p.reshape(n, 256).astype(jnp.bfloat16), preferred_element_type=jnp.float32)
        return jnp.sum(p, axis=0), out

    def weigh_start(b):
        run_sum[...], acc[...] = weigh(sn_buf[...], vn_ref[pl.ds(pl.multiple_of(n_new * b, n_new), n_new), :])
        v_copy(b).wait()

    def weigh_tile(b, t):
        sel = pl.ds(pl.multiple_of(t * tile, tile), tile)
        more, out = weigh(s_buf[sel, :], vbuf[b % 2, sel, :])
        acc[...] += out
        run_sum[...] += more

    def weigh_end(b):
        total = run_sum[...]
        pad = jnp.zeros((6, 256), jnp.float32)
        for h in range(2):
            part[b, h, 0:128, :] = acc[h * 128 : h * 128 + 128, :]
            total_h = jnp.sum(jnp.where(sub8 == h, total, 0.0), axis=0, keepdims=True)
            part[b, h, 128:136, :] = jnp.concatenate([top_buf[h : h + 1, :], total_h, pad], axis=0)
        a1(b).start()

    def attend(s):
        b, first = s // 2, s % 2 == 0

        @pl.when(first)
        def _():
            fetch(b)

        @pl.when(first & (b < n_seq))
        def _():
            score_start(b)

        @pl.when(first & (b > 0))
        def _():
            weigh_start(b - 1)

        def tiles(body):
            def one(i, carry):
                body((s % 2) * (n_tiles // 2) + i)
                return carry

            lax.fori_loop(0, n_tiles // 2, one, 0)

        @pl.when(b == 0)
        def _():
            tiles(lambda t: score_tile(b, t))

        @pl.when((b > 0) & (b < n_seq))
        def _():
            def both(t):
                weigh_tile(b - 1, t)
                score_tile(b, t)

            tiles(both)

        @pl.when(b == n_seq)
        def _():
            tiles(lambda t: weigh_tile(b - 1, t))

        @pl.when((s % 2 == 1) & (b > 0))
        def _():
            weigh_end(b - 1)

        @pl.when((s % 2 == 1) & (b < n_seq))
        def _():
            score_end(b)

    def a1(j):
        return send(part.at[j, 1 - core], got1.at[j], a1s.at[j], a1r.at[j], z, mate)

    def a2(j):
        return send(chip.at[j, 1 - y], got2.at[j], a2s.at[j], a2r.at[j], z, over)

    def a3(j, h):
        return send(ob.at[j, h], ob.at[j, h], a3s.at[j], a3r.at[j], z, mate)

    def b_right(j, p):
        return send(prod.at[j, p], from_l.at[j, p], brs.at[j, p], brr.at[j, p], z + 1, c)

    def b_left(j, p):
        return send(prod.at[j, p], from_r.at[j, p], bls.at[j, p], blr.at[j, p], z - 1, c)

    def c_right(j, p):
        return send(full.at[j, c, p], full.at[j, c, p], crs.at[j, p], crr.at[j, p], z + 1, c)

    def c_left(j, p):
        return send(full.at[j, c, p], full.at[j, c, p], cls.at[j, p], clr.at[j, p], z - 1, c)

    def c_over(j, q, p):
        return send(full.at[j, q, p], full.at[j, q, p], cys.at[j, p], cyr.at[j, p], z, over)

    def c_mate(j, q, u, p):
        return send(full.at[j, q, p], full.at[j, q, p], cps.at[j, u, p], cpr.at[j, u, p], z, mate)

    def merge(a, b):
        top = jnp.maximum(a[128:129], b[128:129])
        fa = jnp.exp2((a[128:129] - top) * EXP2_SCALE)
        fb = jnp.exp2((b[128:129] - top) * EXP2_SCALE)
        return a[0:128] * fa + b[0:128] * fb, top, a[129:130] * fa + b[129:130] * fb

    def stage_a1(j):
        a1(j).wait_recv()
        vals, top, total = merge(part[j, core], got1[j])
        for th in range(2):
            sel = slice(128 * th, 128 * th + 128)
            chip[j, th, 0:128] = vals[:, sel]
            chip[j, th, 128:136] = jnp.concatenate([top[:, sel], total[:, sel], jnp.zeros((6, 128), jnp.float32)], axis=0)
        a2(j).start()

    def stage_a2(j):
        a2(j).wait_recv()
        vals, _, total = merge(chip[j, y], got2[j])
        ob[j, core] = (vals / total).T
        a3(j, core).start()

    def stage_a3(j):
        a3(j, 1 - core).wait_recv()

        @pl.when(j == 0)
        def _():
            for p in range(n_part):
                wo_copy(p).wait()

        o = jnp.concatenate([ob[j, h, 32 * g : 32 * g + 32, :] for h in range(2) for g in range(4)], axis=1)
        o = o.astype(jnp.bfloat16)
        for p in range(n_part):
            prod[j, p] = jnp.dot(o, wo[p], preferred_element_type=jnp.float32)

        @pl.when(z == 0)
        def _():
            for p in range(last, 0, -1):
                b_right(j, p).start()

        @pl.when(z == last)
        def _():
            for p in range(last):
                b_left(j, p).start()

    def pass_right(j, p):
        b_right(j, p).wait_recv()
        prod[j, p] = prod[j, p] + from_l[j, p]
        b_right(j, p).start()

    def pass_left(j, p):
        b_left(j, p).wait_recv()
        prod[j, p] = prod[j, p] + from_r[j, p]
        b_left(j, p).start()

    def stage_b1(j):
        @pl.when(z == 1)
        def _():
            pass_right(j, 3)
            pass_right(j, 2)

        @pl.when(z == 2)
        def _():
            pass_left(j, 0)
            pass_left(j, 1)

    def stage_b2(j):
        @pl.when(z == 2)
        def _():
            pass_right(j, 3)

        @pl.when(z == 1)
        def _():
            pass_left(j, 0)

    def stage_c0(j):
        x_copy(j).wait()

        @pl.when(z > 0)
        def _():
            b_right(j, z).wait_recv()
            prod[j, z] = prod[j, z] + from_l[j, z]

        @pl.when(z < last)
        def _():
            b_left(j, z).wait_recv()
            prod[j, z] = prod[j, z] + from_r[j, z]

        full[j, c, z] = prod[j, z] + xs[j].astype(jnp.float32)

        @pl.when(z < last)
        def _():
            c_right(j, z).start()

        @pl.when(z > 0)
        def _():
            c_left(j, z).start()

        c_over(j, c, z).start()
        c_mate(j, c, 0, z).start()

    def stage_c(j, d):
        @pl.when(z - d >= 0)
        def _():
            p = z - d
            c_right(j, p).wait_recv()

            @pl.when(z < last)
            def _():
                c_right(j, p).start()

            c_over(j, c, p).start()
            c_mate(j, c, 0, p).start()

        @pl.when(z + d <= last)
        def _():
            p = z + d
            c_left(j, p).wait_recv()

            @pl.when(z > 0)
            def _():
                c_left(j, p).start()

            c_over(j, c, p).start()
            c_mate(j, c, 0, p).start()

    def stage_over(j):
        for p in range(n_part):
            c_over(j, over, p).wait_recv()
            c_mate(j, over, 1, p).start()

    def stage_out(j):
        for p in range(n_part):
            c_mate(j, mate, 0, p).wait_recv()
            c_mate(j, over_mate, 1, p).wait_recv()
        for q in range(4):
            for p in range(n_part):
                col = width * (n_part * (q % 2) + p)
                rows = pl.ds(pl.multiple_of(64 * j + 32 * (q // 2), 32), 32)
                out_ref[rows, col : col + width] = full[j, q, p].astype(jnp.bfloat16)

    stages = [
        (stage_a1, 1), (stage_a2, 1), (stage_a3, 1), (stage_b1, 1), (stage_b2, 1), (stage_c0, 1),
        (functools.partial(stage_c, d=1), 1), (functools.partial(stage_c, d=2), 1), (functools.partial(stage_c, d=3), 2),
        (stage_over, 5), (stage_out, 6),
    ]
    n_slots = 2 * n_seq + 2 + sum(lag for _, lag in stages)

    def slot(s, carry):
        @pl.when(s == 1)
        def _():
            in_copy(1).wait()
            norm_half(1)

        @pl.when((s >= 2) & (s < n_q + 4))
        def _():
            project_tile(s - 2, 1)

        @pl.when(s < 2 * n_seq + 2)
        def _():
            attend(s)

        after = 3
        for stage_fn, lag in stages:
            after += lag
            t = s - after

            @pl.when((t >= 0) & (t % 2 == 0) & (t < 2 * n_seq))
            def _():
                stage_fn(t // 2)

        return carry

    lax.fori_loop(0, n_slots, slot, 0)

    def drain(j, carry):
        a1(j).wait_send()
        a2(j).wait_send()
        a3(j, core).wait_send()
        for p in range(n_part):
            @pl.when(z < p)
            def _():
                b_right(j, p).wait_send()

            @pl.when(z > p)
            def _():
                b_left(j, p).wait_send()

            @pl.when((z >= p) & (z < last))
            def _():
                c_right(j, p).wait_send()

            @pl.when((z <= p) & (z > 0))
            def _():
                c_left(j, p).wait_send()

            c_over(j, c, p).wait_send()
            c_mate(j, c, 0, p).wait_send()
            c_mate(j, over, 1, p).wait_send()
        return carry

    lax.fori_loop(0, n_seq, drain, 0)


def block(prefix_len, gain, q_gain, k_gain, x2, w_q, w_k, w_v, kc, vc, w_o):
    rows, d_model = x2.shape
    n_seq, cache_rows, _ = kc.shape
    n_part = 4
    width = d_model // (2 * n_part)
    n_q = w_q.shape[1] // 256
    new_rows = 2 * rows // n_seq
    tile = min(2048, cache_rows // 2)
    half_dim = HEAD_DIM // 2
    freq = 1.0 / (1000000.0 ** (np.arange(half_dim, dtype=np.float64) * 2.0 / HEAD_DIM))
    freq = jnp.asarray(np.concatenate([freq, freq])[None], jnp.float32)
    hbm = pl.BlockSpec(memory_space=pl.ANY)
    vmem = pl.BlockSpec(memory_space=pltpu.VMEM)
    f32, bf16 = jnp.float32, jnp.bfloat16
    sems = pltpu.SemaphoreType.DMA
    piece = (32, width)
    return pl.pallas_call(
        functools.partial(block_kernel, tile=tile),
        out_shape=(
            pltpu.VMEM((rows, d_model), bf16),
            pltpu.VMEM((2 * rows, 128), bf16),
            pltpu.VMEM((2 * rows, 128), bf16),
        ),
        in_specs=[pl.BlockSpec(memory_space=pltpu.SMEM), vmem, vmem, vmem, vmem, hbm, hbm, hbm, hbm, hbm, hbm, hbm],
        out_specs=(vmem, vmem, vmem),
        scratch_shapes=[
            pltpu.VMEM((n_q, rows, 256), bf16),
            pltpu.VMEM((n_q + 2, d_model, 256), bf16),
            pltpu.VMEM((rows, 128), f32),
            pltpu.VMEM((rows, 128), f32),
            pltpu.VMEM((rows, 128), f32),
            pltpu.VMEM((2, cache_rows, 128), bf16),
            pltpu.VMEM((2, cache_rows, 128), bf16),
            pltpu.VMEM((256, 256), bf16),
            pltpu.VMEM((cache_rows, 256), f32),
            pltpu.VMEM((new_rows, 256), f32),
            pltpu.VMEM((256, 256), f32),
            pltpu.VMEM((8, 256), f32),
            pltpu.VMEM((8, 256), f32),
            pltpu.VMEM((8, 256), f32),
            pltpu.VMEM((n_part, w_o.shape[0], width), bf16),
            pltpu.VMEM((n_seq, *piece), bf16),
            pltpu.VMEM((n_seq, 2, 136, 256), f32),
            pltpu.VMEM((n_seq, 136, 256), f32),
            pltpu.VMEM((n_seq, 2, 136, 128), f32),
            pltpu.VMEM((n_seq, 136, 128), f32),
            pltpu.VMEM((n_seq, 2, 128, 128), f32),
            pltpu.VMEM((n_seq, n_part, *piece), f32),
            pltpu.VMEM((n_seq, n_part, *piece), f32),
            pltpu.VMEM((n_seq, n_part, *piece), f32),
            pltpu.VMEM((n_seq, 4, n_part, *piece), f32),
            sems((2,)),
            sems((n_q + 2,)),
            sems((2,)),
            sems((2,)),
            sems((n_part,)),
            sems((n_seq,)),
            *[sems((n_seq,))] * 6,
            *[sems((n_seq, n_part))] * 10,
            sems((n_seq, 2, n_part)),
            sems((n_seq, 2, n_part)),
        ],
        compiler_params=pltpu.CompilerParams(
            collective_id=0, has_side_effects=True, vmem_limit_bytes=int(58.5 * 1024 * 1024)
        ),
        cost_estimate=pl.CostEstimate(
            flops=4 * n_seq * cache_rows * 256 * 256, bytes_accessed=60 << 20, transcendentals=n_seq * cache_rows * 256
        ),
        name="block",
    )(prefix_len, gain, q_gain, k_gain, freq, x2, w_q, w_k, w_v, kc, vc, w_o)


def solution(mesh):
    def per_device(hidden, prefix_len, k_cache, v_cache, attn_norm, w_q, w_k, w_v, w_o, q_norm, k_norm):
        n_seq, n_new, d_model = hidden.shape
        x2 = hidden.reshape(n_seq * n_new, d_model)
        out, k_rows, v_rows = block(
            prefix_len, attn_norm, q_norm, k_norm, x2, w_q, w_k, w_v,
            k_cache.reshape(n_seq, -1, HEAD_DIM), v_cache.reshape(n_seq, -1, HEAD_DIM), w_o,
        )
        new_shape = (n_seq, n_new, 2, HEAD_DIM)
        return out.reshape(hidden.shape), k_rows.reshape(new_shape), v_rows.reshape(new_shape)

    cache_spec = P("dp", "cp", "tp", None)
    arg_specs = (P("dp", None, None), P("dp"), cache_spec, cache_spec, P(None), P(None, "tp"), P(None, "tp"), P(None, "tp"), P("tp", None), P(None), P(None))
    out_specs = (P("dp", None, None), P("dp", None, "tp", None), P("dp", None, "tp", None))
    return jax.shard_map(per_device, mesh=mesh, in_specs=arg_specs, out_specs=out_specs, check_vma=False)
```

```python
import functools

import jax
import jax.numpy as jnp
import numpy as np
from jax import lax
from jax.experimental import pallas as pl
from jax.experimental.pallas import tpu as pltpu
from jax.sharding import PartitionSpec as P

HEAD_DIM = 128
MASKED = -1e30
EXP2_SCALE = HEAD_DIM**-0.5 * 1.4426950408889634
MESH = pl.DeviceIdType.MESH


def block_kernel(
    len_ref, gain, q_gain, k_gain, freq, x_hbm, wq_hbm, wk_hbm, wv_hbm, kc_hbm, vc_hbm, wo_hbm,
    out_ref, kn_ref, vn_ref,
    q_ref, w_buf, cos_t, sin_t, turn, kbuf, vbuf, qt, s_buf, sn_buf, acc, top_buf, run_top, run_sum,
    wo, xs, part, got1, chip, got2, ob, prod, from_l, from_r, full,
    x_sem, w_sem, k_sem, v_sem, wo_sem, xs_sem, a1s, a1r, a2s, a2r, a3s, a3r,
    brs, brr, bls, blr, crs, crr, cls, clr, cys, cyr, cps, cpr, *, tile,
):
    dp, z, c = lax.axis_index("dp"), lax.axis_index("tp"), lax.axis_index("cp")
    y, core = c // 2, c % 2
    mate = 2 * y + (1 - core)
    over = 2 * (1 - y) + core
    over_mate = 2 * (1 - y) + (1 - core)
    n_seq, n_part, width = full.shape[0], full.shape[2], full.shape[4]
    last = n_part - 1
    cache_rows = kbuf.shape[1]
    n_new = kn_ref.shape[0] // n_seq
    n_tok = n_new // 2
    n_tiles = cache_rows // tile
    rows, d_model = out_ref.shape
    half_rows = rows // 2
    n_q = wq_hbm.shape[1] // 256

    def send(src, dst, send_sem, recv_sem, tp, cp):
        return pltpu.make_async_remote_copy(
            src_ref=src, dst_ref=dst, send_sem=send_sem, recv_sem=recv_sem, device_id=(dp, tp, cp), device_id_type=MESH
        )

    def k_copy(b):
        return pltpu.make_async_copy(kc_hbm.at[b], kbuf.at[b % 2], k_sem.at[b % 2])

    def v_copy(b):
        return pltpu.make_async_copy(vc_hbm.at[b], vbuf.at[b % 2], v_sem.at[b % 2])

    def wo_copy(p):
        cols = pl.ds(pl.multiple_of(n_part * width * core + width * p, width), width)
        return pltpu.make_async_copy(wo_hbm.at[:, cols], wo.at[p], wo_sem.at[p])

    owner = jnp.clip(z - 1, 0, 1)

    def x_copy(j):
        rows = pl.ds(pl.multiple_of(64 * j + 32 * y, 32), 32)
        cols = pl.ds(pl.multiple_of(n_part * width * core + 2 * width * owner, 2 * width), 2 * width)
        return pltpu.make_async_copy(x_hbm.at[rows, cols], xs.at[j], xs_sem.at[j])

    def in_copy(half):
        sel = pl.ds(half_rows * half, half_rows)
        return pltpu.make_async_copy(x_hbm.at[sel], out_ref.at[sel], x_sem.at[half])

    w_copies = [
        pltpu.make_async_copy(wq_hbm.at[:, pl.ds(256 * i, 256)], w_buf.at[i], w_sem.at[i]) for i in range(n_q)
    ]
    w_copies.append(pltpu.make_async_copy(wk_hbm, w_buf.at[n_q], w_sem.at[n_q]))
    w_copies.append(pltpu.make_async_copy(wv_hbm, w_buf.at[n_q + 1], w_sem.at[n_q + 1]))
    in_copy(0).start()

    barrier = pltpu.get_barrier_semaphore()
    for peer in (mate, over):
        pl.semaphore_signal(barrier, inc=1, device_id=(dp, z, peer), device_id_type=MESH)

    @pl.when(z > 0)
    def _():
        pl.semaphore_signal(barrier, inc=1, device_id=(dp, z - 1, c), device_id_type=MESH)

    @pl.when(z < last)
    def _():
        pl.semaphore_signal(barrier, inc=1, device_id=(dp, z + 1, c), device_id_type=MESH)

    rope_lane = lax.broadcasted_iota(jnp.int32, (n_tok, 128), 1)
    rope_token = lax.broadcasted_iota(jnp.int32, (n_tok, 128), 0)

    def rope_rows(b, carry):
        angle = (rope_token + len_ref[b]).astype(jnp.float32) * freq[...]
        sel = pl.ds(pl.multiple_of(b * (n_tok), n_tok), n_tok)
        cos_t[sel, :] = jnp.cos(angle)
        sin = jnp.sin(angle)
        sin_t[sel, :] = jnp.where(rope_lane < 64, -sin, sin)
        return carry

    lax.fori_loop(0, n_seq, rope_rows, 0)
    x_gain = gain[...].astype(jnp.float32).reshape(1, d_model)

    def norm_half(half):
        def norm_rows(i, carry):
            sel = pl.ds(pl.multiple_of(half * half_rows + i * 32, 32), 32)
            x = out_ref[sel, :].astype(jnp.float32)
            mean_sq = jnp.mean(x * x, axis=-1, keepdims=True)
            out_ref[sel, :] = (x * lax.rsqrt(mean_sq + 1e-6) * x_gain).astype(jnp.bfloat16)
            return carry

        lax.fori_loop(0, half_rows // 32, norm_rows, 0)

    q_gain_row = q_gain[...].astype(jnp.float32).reshape(1, 128)
    k_gain_row = k_gain[...].astype(jnp.float32).reshape(1, 128)

    def project_tile(i, half):
        sel = slice(half * half_rows, (half + 1) * half_rows)
        lin = jnp.dot(out_ref[sel, :], w_buf[i], preferred_element_type=jnp.float32).astype(jnp.bfloat16)
        lin = lin.astype(jnp.float32)
        head_gain = jnp.where(i < n_q, q_gain_row, k_gain_row)
        for u in range(2):
            raw = lin[:, 128 * u : 128 * u + 128]
            mean_sq = jnp.mean(raw * raw, axis=-1, keepdims=True)
            t = raw * lax.rsqrt(mean_sq + 1e-6) * head_gain
            t = t * cos_t[sel, :] + pltpu.roll(t, 64, 1) * sin_t[sel, :]

            @pl.when(i < n_q)
            def _():
                q_ref[i, sel, 128 * u : 128 * u + 128] = t.astype(jnp.bfloat16)

            @pl.when(i >= n_q)
            def _():
                turn[pl.ds(u, half_rows, stride=2), :] = jnp.where(i == n_q, t, raw)

        new_rows = slice(half * rows, (half + 1) * rows)

        @pl.when(i == n_q)
        def _():
            kn_ref[new_rows, :] = turn[...].astype(jnp.bfloat16)

        @pl.when(i == n_q + 1)
        def _():
            vn_ref[new_rows, :] = turn[...].astype(jnp.bfloat16)

    in_copy(0).wait()
    for copy in w_copies:
        copy.start()
    norm_half(0)
    k_copy(0).start()
    in_copy(1).start()

    def first_tile(i, carry):
        pltpu.make_async_copy(w_buf.at[i], w_buf.at[i], w_sem.at[i]).wait()
        project_tile(i, 0)
        return carry

    lax.fori_loop(0, n_q + 2, first_tile, 0)
    v_copy(0).start()
    for p in range(n_part):
        wo_copy(p).start()
    for j in range(n_seq):
        x_copy(j).start()

    @pl.when((z == 0) | (z == last))
    def _():
        pl.semaphore_wait(barrier, 3)

    @pl.when((z > 0) & (z < last))
    def _():
        pl.semaphore_wait(barrier, 4)

    sub16 = lax.broadcasted_iota(jnp.int32, (16, 128), 0) & 1
    even_rows = jnp.where(sub16 == 0, 1.0, 0.0).astype(jnp.bfloat16)
    odd_rows = jnp.where(sub16 == 0, 0.0, 1.0).astype(jnp.bfloat16)
    sub8 = lax.broadcasted_iota(jnp.int32, (8, 256), 0) & 1

    def split_rows(k):
        n = k.shape[0]
        k3 = k.reshape(n // 16, 16, 128)
        return jnp.concatenate(
            [(k3 * even_rows[None]).reshape(n, 128), (k3 * odd_rows[None]).reshape(n, 128)], axis=1
        )

    def split_lanes(v):
        n = v.shape[0]
        lane = lax.broadcasted_iota(jnp.int32, (16, n), 1) & 1
        even = jnp.where(lane == 0, 1.0, 0.0).astype(jnp.bfloat16)
        odd = jnp.where(lane == 0, 0.0, 1.0).astype(jnp.bfloat16)
        vt = v.T.reshape(8, 16, n)
        return jnp.concatenate([(vt * even[None]).reshape(128, n), (vt * odd[None]).reshape(128, n)], axis=0)

    def scores(k):
        return jnp.dot(split_rows(k), qt[...], preferred_element_type=jnp.float32)

    def fetch(b):
        @pl.when(b + 1 < n_seq)
        def _():
            k_copy(b + 1).start()

        @pl.when((b > 0) & (b < n_seq))
        def _():
            v_copy(b).start()

    def score_start(b):
        q_rows = pl.multiple_of(64 * b, 64)
        for h in range(2):
            blocks = [
                q_ref[h * 2 + g // 2, pl.ds(q_rows + th * 32, 32), (g % 2) * 128 : (g % 2) * 128 + 128]
                for th in range(2)
                for g in range(4)
            ]
            qt[h * 128 : h * 128 + 128, :] = jnp.concatenate(blocks, axis=0).T
        run_top[...] = jnp.full((8, 256), MASKED, jnp.float32)
        k_copy(b).wait()

    def score_tile(b, t):
        sel = pl.ds(pl.multiple_of(t * tile, tile), tile)
        n_rows = 2 * (len_ref[b] - c * (cache_rows // 2)) - t * tile
        s = scores(kbuf[b % 2, sel, :])
        s = jnp.where(lax.broadcasted_iota(jnp.int32, (tile, 256), 0) < n_rows, s, MASKED)
        s_buf[sel, :] = s
        run_top[...] = jnp.maximum(run_top[...], jnp.max(s.reshape(tile // 8, 8, 256), axis=0))

    def score_end(b):
        key = lax.broadcasted_iota(jnp.int32, (n_new, 256), 0) // 2
        col = lax.broadcasted_iota(jnp.int32, (n_new, 256), 1)
        token = (col // 128) * 32 + (col % 32)
        token = jnp.where(c == 3, token, -1)
        s_new = jnp.where(key <= token, scores(kn_ref[pl.ds(pl.multiple_of(n_new * b, n_new), n_new), :]), MASKED)
        sn_buf[...] = s_new
        top = jnp.maximum(run_top[...], jnp.max(s_new.reshape(n_new // 8, 8, 256), axis=0))
        top0 = jnp.max(jnp.where(sub8 == 0, top, MASKED), axis=0, keepdims=True)
        top1 = jnp.max(jnp.where(sub8 == 0, MASKED, top), axis=0, keepdims=True)
        top_buf[...] = jnp.where(sub8 == 0, top0, top1)

    def weigh(s, v):
        top = top_buf[...]
        base = jnp.where(top > 0.5 * MASKED, top, 0.0)
        n = s.shape[0]
        p = jnp.exp2((s.reshape(n // 8, 8, 256) - base[None]) * EXP2_SCALE)
        out = jnp.dot(split_lanes(v), p.reshape(n, 256).astype(jnp.bfloat16), preferred_element_type=jnp.float32)
        return jnp.sum(p, axis=0), out

    def weigh_start(b):
        run_sum[...], acc[...] = weigh(sn_buf[...], vn_ref[pl.ds(pl.multiple_of(n_new * b, n_new), n_new), :])
        v_copy(b).wait()

    def weigh_tile(b, t):
        sel = pl.ds(pl.multiple_of(t * tile, tile), tile)
        more, out = weigh(s_buf[sel, :], vbuf[b % 2, sel, :])
        acc[...] += out
        run_sum[...] += more

    def weigh_end(b):
        total = run_sum[...]
        pad = jnp.zeros((6, 256), jnp.float32)
        for h in range(2):
            part[b, h, 0:128, :] = acc[h * 128 : h * 128 + 128, :]
            total_h = jnp.sum(jnp.where(sub8 == h, total, 0.0), axis=0, keepdims=True)
            part[b, h, 128:136, :] = jnp.concatenate([top_buf[h : h + 1, :], total_h, pad], axis=0)
        a1(b).start()

    def attend(s):
        b, first = s // 2, s % 2 == 0

        @pl.when(first)
        def _():
            fetch(b)

        @pl.when(first & (b < n_seq))
        def _():
            score_start(b)

        @pl.when(first & (b > 0))
        def _():
            weigh_start(b - 1)

        def tiles(body):
            def one(i, carry):
                body((s % 2) * (n_tiles // 2) + i)
                return carry

            lax.fori_loop(0, n_tiles // 2, one, 0)

        @pl.when(b == 0)
        def _():
            tiles(lambda t: score_tile(b, t))

        @pl.when((b > 0) & (b < n_seq))
        def _():
            def both(t):
                weigh_tile(b - 1, t)
                score_tile(b, t)

            tiles(both)

        @pl.when(b == n_seq)
        def _():
            tiles(lambda t: weigh_tile(b - 1, t))

        @pl.when((s % 2 == 1) & (b > 0))
        def _():
            weigh_end(b - 1)

        @pl.when((s % 2 == 1) & (b < n_seq))
        def _():
            score_end(b)

    def a1(j):
        return send(part.at[j, 1 - core], got1.at[j], a1s.at[j], a1r.at[j], z, mate)

    def a2(j):
        return send(chip.at[j, 1 - y], got2.at[j], a2s.at[j], a2r.at[j], z, over)

    def a3(j, h):
        return send(ob.at[j, h], ob.at[j, h], a3s.at[j], a3r.at[j], z, mate)

    def b_right(j, p):
        return send(prod.at[j, p], from_l.at[j, p], brs.at[j, p], brr.at[j, p], z + 1, c)

    def b_left(j, p):
        return send(prod.at[j, p], from_r.at[j, p], bls.at[j, p], blr.at[j, p], z - 1, c)

    def c_right(j, p):
        return send(full.at[j, c, p], full.at[j, c, p], crs.at[j, p], crr.at[j, p], z + 1, c)

    def c_left(j, p):
        return send(full.at[j, c, p], full.at[j, c, p], cls.at[j, p], clr.at[j, p], z - 1, c)

    def c_over(j, q, p):
        return send(full.at[j, q, p], full.at[j, q, p], cys.at[j, p], cyr.at[j, p], z, over)

    def c_mate(j, q, u, p):
        return send(full.at[j, q, p], full.at[j, q, p], cps.at[j, u, p], cpr.at[j, u, p], z, mate)

    def merge(a, b):
        top = jnp.maximum(a[128:129], b[128:129])
        fa = jnp.exp2((a[128:129] - top) * EXP2_SCALE)
        fb = jnp.exp2((b[128:129] - top) * EXP2_SCALE)
        return a[0:128] * fa + b[0:128] * fb, top, a[129:130] * fa + b[129:130] * fb

    def stage_a1(j):
        a1(j).wait_recv()
        vals, top, total = merge(part[j, core], got1[j])
        for th in range(2):
            sel = slice(128 * th, 128 * th + 128)
            chip[j, th, 0:128] = vals[:, sel]
            chip[j, th, 128:136] = jnp.concatenate([top[:, sel], total[:, sel], jnp.zeros((6, 128), jnp.float32)], axis=0)
        a2(j).start()

    def stage_a2(j):
        a2(j).wait_recv()
        vals, _, total = merge(chip[j, y], got2[j])
        ob[j, core] = (vals / total).T
        a3(j, core).start()

    def stage_a3(j):
        a3(j, 1 - core).wait_recv()

        @pl.when(j == 0)
        def _():
            for p in range(n_part):
                wo_copy(p).wait()

        o = jnp.concatenate([ob[j, h, 32 * g : 32 * g + 32, :] for h in range(2) for g in range(4)], axis=1)
        o = o.astype(jnp.bfloat16)
        for p in range(n_part):
            prod[j, p] = jnp.dot(o, wo[p], preferred_element_type=jnp.float32)

        @pl.when(z == 0)
        def _():
            for p in (2, 3, 0, 1):
                b_right(j, p).start()

        @pl.when(z == last)
        def _():
            for p in (0, 1, 2, 3):
                b_left(j, p).start()

    def pass_right(j, p):
        b_right(j, p).wait_recv()
        prod[j, p] = prod[j, p] + from_l[j, p]
        b_right(j, p).start()

    def pass_left(j, p):
        b_left(j, p).wait_recv()
        prod[j, p] = prod[j, p] + from_r[j, p]
        b_left(j, p).start()

    def stage_b1(j):
        @pl.when(z == 1)
        def _():
            pass_right(j, 2)
            pass_right(j, 3)

        @pl.when(z == 2)
        def _():
            pass_left(j, 0)
            pass_left(j, 1)

    def spread(j, p):
        c_over(j, c, p).start()
        c_mate(j, c, 0, p).start()

    def stage_c0(j):
        x_copy(j).wait()

        def finish(p):
            b_right(j, p).wait_recv()
            b_left(j, p).wait_recv()
            x = xs[j, :, width * (p % 2) : width * (p % 2) + width].astype(jnp.float32)
            full[j, c, p] = prod[j, p] + from_l[j, p] + from_r[j, p] + x
            c_right(j, p).start()
            c_left(j, p).start()
            spread(j, p)

        @pl.when(z == 1)
        def _():
            finish(0)
            finish(1)

        @pl.when(z == 2)
        def _():
            finish(2)
            finish(3)

    def from_right(j, p, onward):
        c_left(j, p).wait_recv()
        if onward:
            c_left(j, p).start()
        spread(j, p)

    def from_left(j, p, onward):
        c_right(j, p).wait_recv()
        if onward:
            c_right(j, p).start()
        spread(j, p)

    def stage_c1(j):
        @pl.when(z == 0)
        def _():
            from_right(j, 0, False)
            from_right(j, 1, False)

        @pl.when(z == 1)
        def _():
            from_right(j, 2, True)
            from_right(j, 3, True)

        @pl.when(z == 2)
        def _():
            from_left(j, 0, True)
            from_left(j, 1, True)

        @pl.when(z == 3)
        def _():
            from_left(j, 2, False)
            from_left(j, 3, False)

    def stage_c2(j):
        @pl.when(z == 0)
        def _():
            from_right(j, 2, False)
            from_right(j, 3, False)

        @pl.when(z == 3)
        def _():
            from_left(j, 0, False)
            from_left(j, 1, False)

    def stage_over(j):
        for p in range(n_part):
            c_over(j, over, p).wait_recv()
            c_mate(j, over, 1, p).start()

    def stage_out(j):
        for p in range(n_part):
            c_mate(j, mate, 0, p).wait_recv()
            c_mate(j, over_mate, 1, p).wait_recv()
        for q in range(4):
            for p in range(n_part):
                col = width * (n_part * (q % 2) + p)
                rows = pl.ds(pl.multiple_of(64 * j + 32 * (q // 2), 32), 32)
                out_ref[rows, col : col + width] = full[j, q, p].astype(jnp.bfloat16)

    stages = [
        (stage_a1, 1), (stage_a2, 2), (stage_a3, 1), (stage_b1, 2), (stage_c0, 1), (stage_c1, 2), (stage_c2, 1),
        (stage_over, 6), (stage_out, 2),
    ]
    n_slots = 2 * n_seq + 2 + sum(lag for _, lag in stages)

    def slot(s, carry):
        @pl.when(s == 1)
        def _():
            in_copy(1).wait()
            norm_half(1)

        @pl.when((s >= 2) & (s < n_q + 4))
        def _():
            project_tile(s - 2, 1)

        @pl.when(s < 2 * n_seq + 2)
        def _():
            attend(s)

        after = 3 + sum(lag for _, lag in stages)
        for stage_fn, lag in reversed(stages):
            t = s - after
            after -= lag

            @pl.when((t >= 0) & (t % 2 == 0) & (t < 2 * n_seq))
            def _():
                stage_fn(t // 2)

        return carry

    lax.fori_loop(0, n_slots, slot, 0)

    def drain(j, carry):
        a1(j).wait_send()
        a2(j).wait_send()
        a3(j, core).wait_send()
        for p in range(n_part):
            @pl.when((z == 0) | ((z == 1) & (p >= 2)))
            def _():
                b_right(j, p).wait_send()

            @pl.when((z == 3) | ((z == 2) & (p < 2)))
            def _():
                b_left(j, p).wait_send()

            @pl.when((z == 2) | ((z == 1) & (p < 2)))
            def _():
                c_right(j, p).wait_send()

            @pl.when((z == 1) | ((z == 2) & (p >= 2)))
            def _():
                c_left(j, p).wait_send()

            c_over(j, c, p).wait_send()
            c_mate(j, c, 0, p).wait_send()
            c_mate(j, over, 1, p).wait_send()
        return carry

    lax.fori_loop(0, n_seq, drain, 0)


def block(prefix_len, gain, q_gain, k_gain, x2, w_q, w_k, w_v, kc, vc, w_o):
    rows, d_model = x2.shape
    n_seq, cache_rows, _ = kc.shape
    n_part = 4
    width = d_model // (2 * n_part)
    n_q = w_q.shape[1] // 256
    new_rows = 2 * rows // n_seq
    tile = min(2048, cache_rows // 2)
    half_dim = HEAD_DIM // 2
    freq = 1.0 / (1000000.0 ** (np.arange(half_dim, dtype=np.float64) * 2.0 / HEAD_DIM))
    freq = jnp.asarray(np.concatenate([freq, freq])[None], jnp.float32)
    hbm = pl.BlockSpec(memory_space=pl.ANY)
    vmem = pl.BlockSpec(memory_space=pltpu.VMEM)
    f32, bf16 = jnp.float32, jnp.bfloat16
    sems = pltpu.SemaphoreType.DMA
    piece = (32, width)
    return pl.pallas_call(
        functools.partial(block_kernel, tile=tile),
        out_shape=(
            pltpu.VMEM((rows, d_model), bf16),
            pltpu.VMEM((2 * rows, 128), bf16),
            pltpu.VMEM((2 * rows, 128), bf16),
        ),
        in_specs=[pl.BlockSpec(memory_space=pltpu.SMEM), vmem, vmem, vmem, vmem, hbm, hbm, hbm, hbm, hbm, hbm, hbm],
        out_specs=(vmem, vmem, vmem),
        scratch_shapes=[
            pltpu.VMEM((n_q, rows, 256), bf16),
            pltpu.VMEM((n_q + 2, d_model, 256), bf16),
            pltpu.VMEM((rows, 128), f32),
            pltpu.VMEM((rows, 128), f32),
            pltpu.VMEM((rows, 128), f32),
            pltpu.VMEM((2, cache_rows, 128), bf16),
            pltpu.VMEM((2, cache_rows, 128), bf16),
            pltpu.VMEM((256, 256), bf16),
            pltpu.VMEM((cache_rows, 256), f32),
            pltpu.VMEM((new_rows, 256), f32),
            pltpu.VMEM((256, 256), f32),
            pltpu.VMEM((8, 256), f32),
            pltpu.VMEM((8, 256), f32),
            pltpu.VMEM((8, 256), f32),
            pltpu.VMEM((n_part, w_o.shape[0], width), bf16),
            pltpu.VMEM((n_seq, 32, 2 * width), bf16),
            pltpu.VMEM((n_seq, 2, 136, 256), f32),
            pltpu.VMEM((n_seq, 136, 256), f32),
            pltpu.VMEM((n_seq, 2, 136, 128), f32),
            pltpu.VMEM((n_seq, 136, 128), f32),
            pltpu.VMEM((n_seq, 2, 128, 128), f32),
            pltpu.VMEM((n_seq, n_part, *piece), f32),
            pltpu.VMEM((n_seq, n_part, *piece), f32),
            pltpu.VMEM((n_seq, n_part, *piece), f32),
            pltpu.VMEM((n_seq, 4, n_part, *piece), f32),
            sems((2,)),
            sems((n_q + 2,)),
            sems((2,)),
            sems((2,)),
            sems((n_part,)),
            sems((n_seq,)),
            *[sems((n_seq,))] * 6,
            *[sems((n_seq, n_part))] * 10,
            sems((n_seq, 2, n_part)),
            sems((n_seq, 2, n_part)),
        ],
        compiler_params=pltpu.CompilerParams(
            collective_id=0, has_side_effects=True, vmem_limit_bytes=int(58.5 * 1024 * 1024)
        ),
        cost_estimate=pl.CostEstimate(
            flops=4 * n_seq * cache_rows * 256 * 256, bytes_accessed=60 << 20, transcendentals=n_seq * cache_rows * 256
        ),
        name="block",
    )(prefix_len, gain, q_gain, k_gain, freq, x2, w_q, w_k, w_v, kc, vc, w_o)


def store_kernel(out_in, k_in, v_in, out_hbm, k_hbm, v_hbm, sem):
    copies = [
        pltpu.make_async_copy(src, dst, sem.at[i])
        for i, (src, dst) in enumerate(((out_in, out_hbm), (k_in, k_hbm), (v_in, v_hbm)))
    ]
    for copy in copies:
        copy.start()
    for copy in copies:
        copy.wait()


def store(*arrays):
    hbm = pl.BlockSpec(memory_space=pl.ANY)
    return pl.pallas_call(
        store_kernel,
        out_shape=tuple(jax.ShapeDtypeStruct(a.shape, a.dtype) for a in arrays),
        in_specs=[hbm] * 3,
        out_specs=(hbm,) * 3,
        scratch_shapes=[pltpu.SemaphoreType.DMA((3,))],
        compiler_params=pltpu.CompilerParams(vmem_limit_bytes=1024 * 1024),
        name="store",
    )(*arrays)


def solution(mesh):
    def per_device(hidden, prefix_len, k_cache, v_cache, attn_norm, w_q, w_k, w_v, w_o, q_norm, k_norm):
        n_seq, n_new, d_model = hidden.shape
        x2 = hidden.reshape(n_seq * n_new, d_model)
        results = block(
            prefix_len, attn_norm, q_norm, k_norm, x2, w_q, w_k, w_v,
            k_cache.reshape(n_seq, -1, HEAD_DIM), v_cache.reshape(n_seq, -1, HEAD_DIM), w_o,
        )
        out, k_rows, v_rows = store(*results)
        new_shape = (n_seq, n_new, 2, HEAD_DIM)
        return out.reshape(hidden.shape), k_rows.reshape(new_shape), v_rows.reshape(new_shape)

    cache_spec = P("dp", "cp", "tp", None)
    arg_specs = (P("dp", None, None), P("dp"), cache_spec, cache_spec, P(None), P(None, "tp"), P(None, "tp"), P(None, "tp"), P("tp", None), P(None), P(None))
    out_specs = (P("dp", None, None), P("dp", None, "tp", None), P("dp", None, "tp", None))
    return jax.shard_map(per_device, mesh=mesh, in_specs=arg_specs, out_specs=out_specs, check_vma=False)
```

```python
import functools

import jax
import jax.numpy as jnp
import numpy as np
from jax import lax
from jax.experimental import pallas as pl
from jax.experimental.pallas import tpu as pltpu
from jax.sharding import PartitionSpec as P

HEAD_DIM = 128
MASKED = -1e30
EXP2_SCALE = HEAD_DIM**-0.5 * 1.4426950408889634
MESH = pl.DeviceIdType.MESH


def block_kernel(
    len_ref, gain, q_gain, k_gain, freq, x_hbm, wq_hbm, wk_hbm, wv_hbm, kc_hbm, vc_hbm, wo_hbm,
    out_ref, kn_ref, vn_ref,
    q_ref, w_buf, cos_t, sin_t, turn, mine, theirs, kbuf, vbuf, qt, s_buf, sn_buf, acc, top_buf, run_top, run_sum,
    wo, xs, part, got1, chip, got2, ob, prod, from_l, from_r, full,
    x_sem, w_sem, k_sem, v_sem, wo_sem, xs_sem, a1s, a1r, a2s, a2r, a3s, a3r,
    shs, shr, brs, brr, bls, blr, crs, crr, cls, clr, cys, cyr, cps, cpr, *, tile,
):
    dp, z, c = lax.axis_index("dp"), lax.axis_index("tp"), lax.axis_index("cp")
    y, core = c // 2, c % 2
    mate = 2 * y + (1 - core)
    over = 2 * (1 - y) + core
    over_mate = 2 * (1 - y) + (1 - core)
    n_seq, n_part, width = full.shape[0], full.shape[2], full.shape[4]
    last = n_part - 1
    cache_rows = kbuf.shape[1]
    n_new = kn_ref.shape[0] // n_seq
    n_tok = n_new // 2
    n_tiles = cache_rows // tile
    rows, d_model = out_ref.shape
    half_rows = rows // 2
    n_q = wq_hbm.shape[1] // 256

    def send(src, dst, send_sem, recv_sem, tp, cp):
        return pltpu.make_async_remote_copy(
            src_ref=src, dst_ref=dst, send_sem=send_sem, recv_sem=recv_sem, device_id=(dp, tp, cp), device_id_type=MESH
        )

    def k_copy(b):
        return pltpu.make_async_copy(kc_hbm.at[b], kbuf.at[b % 2], k_sem.at[b % 2])

    def v_copy(b):
        return pltpu.make_async_copy(vc_hbm.at[b], vbuf.at[b % 2], v_sem.at[b % 2])

    def wo_copy(p):
        cols = pl.ds(pl.multiple_of(n_part * width * core + width * p, width), width)
        return pltpu.make_async_copy(wo_hbm.at[:, cols], wo.at[p], wo_sem.at[p])

    owner = jnp.clip(z - 1, 0, 1)

    def x_copy(j):
        rows = pl.ds(pl.multiple_of(64 * j + 32 * y, 32), 32)
        cols = pl.ds(pl.multiple_of(n_part * width * core + 2 * width * owner, 2 * width), 2 * width)
        return pltpu.make_async_copy(x_hbm.at[rows, cols], xs.at[j], xs_sem.at[j])

    def in_copy(half):
        sel = pl.ds(half_rows * half, half_rows)
        return pltpu.make_async_copy(x_hbm.at[sel], out_ref.at[sel], x_sem.at[half])

    w_copies = [
        pltpu.make_async_copy(wq_hbm.at[:, pl.ds(256 * i, 256)], w_buf.at[i], w_sem.at[i]) for i in range(n_q)
    ]
    w_copies.append(pltpu.make_async_copy(wk_hbm, w_buf.at[n_q], w_sem.at[n_q]))
    w_copies.append(pltpu.make_async_copy(wv_hbm, w_buf.at[n_q + 1], w_sem.at[n_q + 1]))
    in_copy(0).start()

    barrier = pltpu.get_barrier_semaphore()
    for peer in (mate, over):
        pl.semaphore_signal(barrier, inc=1, device_id=(dp, z, peer), device_id_type=MESH)

    @pl.when(z > 0)
    def _():
        pl.semaphore_signal(barrier, inc=1, device_id=(dp, z - 1, c), device_id_type=MESH)

    @pl.when(z < last)
    def _():
        pl.semaphore_signal(barrier, inc=1, device_id=(dp, z + 1, c), device_id_type=MESH)

    rope_lane = lax.broadcasted_iota(jnp.int32, (n_tok, 128), 1)
    rope_token = lax.broadcasted_iota(jnp.int32, (n_tok, 128), 0)

    def rope_rows(b, carry):
        angle = (rope_token + len_ref[b]).astype(jnp.float32) * freq[...]
        sel = pl.ds(pl.multiple_of(b * (n_tok), n_tok), n_tok)
        cos_t[sel, :] = jnp.cos(angle)
        sin = jnp.sin(angle)
        sin_t[sel, :] = jnp.where(rope_lane < 64, -sin, sin)
        return carry

    lax.fori_loop(0, n_seq, rope_rows, 0)
    x_gain = gain[...].astype(jnp.float32).reshape(1, d_model)

    def norm_half(half):
        def norm_rows(i, carry):
            sel = pl.ds(pl.multiple_of(half * half_rows + i * 32, 32), 32)
            x = out_ref[sel, :].astype(jnp.float32)
            mean_sq = jnp.mean(x * x, axis=-1, keepdims=True)
            out_ref[sel, :] = (x * lax.rsqrt(mean_sq + 1e-6) * x_gain).astype(jnp.bfloat16)
            return carry

        lax.fori_loop(0, half_rows // 32, norm_rows, 0)

    q_gain_row = q_gain[...].astype(jnp.float32).reshape(1, 128)
    k_gain_row = k_gain[...].astype(jnp.float32).reshape(1, 128)

    def half_sel(half):
        return slice(half * half_rows, (half + 1) * half_rows)

    def compute_tile(i, half):
        sel = half_sel(half)
        lin = jnp.dot(out_ref[sel, :], w_buf[i], preferred_element_type=jnp.float32).astype(jnp.bfloat16)
        lin = lin.astype(jnp.float32)
        head_gain = jnp.where(i < n_q, q_gain_row, k_gain_row)
        vals = []
        for u in range(2):
            raw = lin[:, 128 * u : 128 * u + 128]
            mean_sq = jnp.mean(raw * raw, axis=-1, keepdims=True)
            t = raw * lax.rsqrt(mean_sq + 1e-6) * head_gain
            t = t * cos_t[sel, :] + pltpu.roll(t, 64, 1) * sin_t[sel, :]
            vals.append(jnp.where(i == n_q + 1, raw, t))
        return vals

    def store_tile(i, half, vals):
        sel = half_sel(half)

        @pl.when(i < n_q)
        def _():
            for u in range(2):
                q_ref[i, sel, 128 * u : 128 * u + 128] = vals[u].astype(jnp.bfloat16)

        @pl.when(i >= n_q)
        def _():
            for u in range(2):
                turn[pl.ds(u, half_rows, stride=2), :] = vals[u]

        new_rows = slice(half * rows, (half + 1) * rows)

        @pl.when(i == n_q)
        def _():
            kn_ref[new_rows, :] = turn[...].astype(jnp.bfloat16)

        @pl.when(i == n_q + 1)
        def _():
            vn_ref[new_rows, :] = turn[...].astype(jnp.bfloat16)

    n_share = (n_q + 2) // 2

    def share(m):
        return send(mine.at[m], theirs.at[m], shs.at[m], shr.at[m], z, mate)

    def share_tile(m):
        i = 2 * m + core
        vals = compute_tile(i, 1)
        for u in range(2):
            mine[m, :, 128 * u : 128 * u + 128] = vals[u]
        share(m).start()
        store_tile(i, 1, vals)

    def take_tile(m):
        share(m).wait_recv()
        store_tile(2 * m + 1 - core, 1, [theirs[m, :, 128 * u : 128 * u + 128] for u in range(2)])

    in_copy(0).wait()
    for copy in w_copies:
        copy.start()
    norm_half(0)
    k_copy(0).start()
    in_copy(1).start()

    def first_tile(i, carry):
        pltpu.make_async_copy(w_buf.at[i], w_buf.at[i], w_sem.at[i]).wait()
        store_tile(i, 0, compute_tile(i, 0))
        return carry

    lax.fori_loop(0, n_q + 2, first_tile, 0)
    v_copy(0).start()
    for p in range(n_part):
        wo_copy(p).start()
    for j in range(n_seq):
        x_copy(j).start()

    @pl.when((z == 0) | (z == last))
    def _():
        pl.semaphore_wait(barrier, 3)

    @pl.when((z > 0) & (z < last))
    def _():
        pl.semaphore_wait(barrier, 4)

    sub16 = lax.broadcasted_iota(jnp.int32, (16, 128), 0) & 1
    even_rows = jnp.where(sub16 == 0, 1.0, 0.0).astype(jnp.bfloat16)
    odd_rows = jnp.where(sub16 == 0, 0.0, 1.0).astype(jnp.bfloat16)
    sub8 = lax.broadcasted_iota(jnp.int32, (8, 256), 0) & 1

    def split_rows(k):
        n = k.shape[0]
        k3 = k.reshape(n // 16, 16, 128)
        return jnp.concatenate(
            [(k3 * even_rows[None]).reshape(n, 128), (k3 * odd_rows[None]).reshape(n, 128)], axis=1
        )

    def split_lanes(v):
        n = v.shape[0]
        lane = lax.broadcasted_iota(jnp.int32, (16, n), 1) & 1
        even = jnp.where(lane == 0, 1.0, 0.0).astype(jnp.bfloat16)
        odd = jnp.where(lane == 0, 0.0, 1.0).astype(jnp.bfloat16)
        vt = v.T.reshape(8, 16, n)
        return jnp.concatenate([(vt * even[None]).reshape(128, n), (vt * odd[None]).reshape(128, n)], axis=0)

    def scores(k):
        return jnp.dot(split_rows(k), qt[...], preferred_element_type=jnp.float32)

    def fetch(b):
        @pl.when(b + 1 < n_seq)
        def _():
            k_copy(b + 1).start()

        @pl.when((b > 0) & (b < n_seq))
        def _():
            v_copy(b).start()

    def score_start(b):
        q_rows = pl.multiple_of(64 * b, 64)
        for h in range(2):
            blocks = [
                q_ref[h * 2 + g // 2, pl.ds(q_rows + th * 32, 32), (g % 2) * 128 : (g % 2) * 128 + 128]
                for th in range(2)
                for g in range(4)
            ]
            qt[h * 128 : h * 128 + 128, :] = jnp.concatenate(blocks, axis=0).T
        run_top[...] = jnp.full((8, 256), MASKED, jnp.float32)
        k_copy(b).wait()

    def score_tile(b, t):
        sel = pl.ds(pl.multiple_of(t * tile, tile), tile)
        n_rows = 2 * (len_ref[b] - c * (cache_rows // 2)) - t * tile
        s = scores(kbuf[b % 2, sel, :])
        s = jnp.where(lax.broadcasted_iota(jnp.int32, (tile, 256), 0) < n_rows, s, MASKED)
        s_buf[sel, :] = s
        run_top[...] = jnp.maximum(run_top[...], jnp.max(s.reshape(tile // 8, 8, 256), axis=0))

    def score_end(b):
        key = lax.broadcasted_iota(jnp.int32, (n_new, 256), 0) // 2
        col = lax.broadcasted_iota(jnp.int32, (n_new, 256), 1)
        token = (col // 128) * 32 + (col % 32)
        token = jnp.where(c == 3, token, -1)
        s_new = jnp.where(key <= token, scores(kn_ref[pl.ds(pl.multiple_of(n_new * b, n_new), n_new), :]), MASKED)
        sn_buf[...] = s_new
        top = jnp.maximum(run_top[...], jnp.max(s_new.reshape(n_new // 8, 8, 256), axis=0))
        top0 = jnp.max(jnp.where(sub8 == 0, top, MASKED), axis=0, keepdims=True)
        top1 = jnp.max(jnp.where(sub8 == 0, MASKED, top), axis=0, keepdims=True)
        top_buf[...] = jnp.where(sub8 == 0, top0, top1)

    def weigh(s, v):
        top = top_buf[...]
        base = jnp.where(top > 0.5 * MASKED, top, 0.0)
        n = s.shape[0]
        p = jnp.exp2((s.reshape(n // 8, 8, 256) - base[None]) * EXP2_SCALE)
        out = jnp.dot(split_lanes(v), p.reshape(n, 256).astype(jnp.bfloat16), preferred_element_type=jnp.float32)
        return jnp.sum(p, axis=0), out

    def weigh_start(b):
        run_sum[...], acc[...] = weigh(sn_buf[...], vn_ref[pl.ds(pl.multiple_of(n_new * b, n_new), n_new), :])
        v_copy(b).wait()

    def weigh_tile(b, t):
        sel = pl.ds(pl.multiple_of(t * tile, tile), tile)
        more, out = weigh(s_buf[sel, :], vbuf[b % 2, sel, :])
        acc[...] += out
        run_sum[...] += more

    def weigh_end(b):
        total = run_sum[...]
        pad = jnp.zeros((6, 256), jnp.float32)
        for h in range(2):
            part[b, h, 0:128, :] = acc[h * 128 : h * 128 + 128, :]
            total_h = jnp.sum(jnp.where(sub8 == h, total, 0.0), axis=0, keepdims=True)
            part[b, h, 128:136, :] = jnp.concatenate([top_buf[h : h + 1, :], total_h, pad], axis=0)
        a1(b).start()

    def attend(s):
        b, first = s // 2, s % 2 == 0

        @pl.when(first)
        def _():
            fetch(b)

        @pl.when(first & (b < n_seq))
        def _():
            score_start(b)

        @pl.when(first & (b > 0))
        def _():
            weigh_start(b - 1)

        def tiles(body):
            def one(i, carry):
                body((s % 2) * (n_tiles // 2) + i)
                return carry

            lax.fori_loop(0, n_tiles // 2, one, 0)

        @pl.when(b == 0)
        def _():
            tiles(lambda t: score_tile(b, t))

        @pl.when((b > 0) & (b < n_seq))
        def _():
            def both(t):
                weigh_tile(b - 1, t)
                score_tile(b, t)

            tiles(both)

        @pl.when(b == n_seq)
        def _():
            tiles(lambda t: weigh_tile(b - 1, t))

        @pl.when((s % 2 == 1) & (b > 0))
        def _():
            weigh_end(b - 1)

        @pl.when((s % 2 == 1) & (b < n_seq))
        def _():
            score_end(b)

    def a1(j):
        return send(part.at[j, 1 - core], got1.at[j], a1s.at[j], a1r.at[j], z, mate)

    def a2(j):
        return send(chip.at[j, 1 - y], got2.at[j], a2s.at[j], a2r.at[j], z, over)

    def a3(j, h):
        return send(ob.at[j, h], ob.at[j, h], a3s.at[j], a3r.at[j], z, mate)

    def b_right(j, p):
        return send(prod.at[j, p], from_l.at[j, p], brs.at[j, p], brr.at[j, p], z + 1, c)

    def b_left(j, p):
        return send(prod.at[j, p], from_r.at[j, p], bls.at[j, p], blr.at[j, p], z - 1, c)

    def c_right(j, p):
        return send(full.at[j, c, p], full.at[j, c, p], crs.at[j, p], crr.at[j, p], z + 1, c)

    def c_left(j, p):
        return send(full.at[j, c, p], full.at[j, c, p], cls.at[j, p], clr.at[j, p], z - 1, c)

    def c_over(j, q, p):
        return send(full.at[j, q, p], full.at[j, q, p], cys.at[j, p], cyr.at[j, p], z, over)

    def c_mate(j, q, u, p):
        return send(full.at[j, q, p], full.at[j, q, p], cps.at[j, u, p], cpr.at[j, u, p], z, mate)

    def merge(a, b):
        top = jnp.maximum(a[128:129], b[128:129])
        fa = jnp.exp2((a[128:129] - top) * EXP2_SCALE)
        fb = jnp.exp2((b[128:129] - top) * EXP2_SCALE)
        return a[0:128] * fa + b[0:128] * fb, top, a[129:130] * fa + b[129:130] * fb

    def stage_a1(j):
        a1(j).wait_recv()
        vals, top, total = merge(part[j, core], got1[j])
        for th in range(2):
            sel = slice(128 * th, 128 * th + 128)
            chip[j, th, 0:128] = vals[:, sel]
            chip[j, th, 128:136] = jnp.concatenate([top[:, sel], total[:, sel], jnp.zeros((6, 128), jnp.float32)], axis=0)
        a2(j).start()

    def stage_a2(j):
        a2(j).wait_recv()
        vals, _, total = merge(chip[j, y], got2[j])
        ob[j, core] = (vals / total).T
        a3(j, core).start()

    def stage_a3(j):
        a3(j, 1 - core).wait_recv()

        @pl.when(j == 0)
        def _():
            for p in range(n_part):
                wo_copy(p).wait()

        o = jnp.concatenate([ob[j, h, 32 * g : 32 * g + 32, :] for h in range(2) for g in range(4)], axis=1)
        o = o.astype(jnp.bfloat16)
        for p in range(n_part):
            prod[j, p] = jnp.dot(o, wo[p], preferred_element_type=jnp.float32)

        @pl.when(z == 0)
        def _():
            for p in (2, 3, 0, 1):
                b_right(j, p).start()

        @pl.when(z == last)
        def _():
            for p in (0, 1, 2, 3):
                b_left(j, p).start()

    def pass_right(j, p):
        b_right(j, p).wait_recv()
        prod[j, p] = prod[j, p] + from_l[j, p]
        b_right(j, p).start()

    def pass_left(j, p):
        b_left(j, p).wait_recv()
        prod[j, p] = prod[j, p] + from_r[j, p]
        b_left(j, p).start()

    def stage_b1(j):
        @pl.when(z == 1)
        def _():
            pass_right(j, 2)
            pass_right(j, 3)

        @pl.when(z == 2)
        def _():
            pass_left(j, 0)
            pass_left(j, 1)

    def spread(j, p):
        c_over(j, c, p).start()
        c_mate(j, c, 0, p).start()

    def stage_c0(j):
        x_copy(j).wait()

        def finish(p):
            b_right(j, p).wait_recv()
            b_left(j, p).wait_recv()
            x = xs[j, :, width * (p % 2) : width * (p % 2) + width].astype(jnp.float32)
            full[j, c, p] = prod[j, p] + from_l[j, p] + from_r[j, p] + x
            c_right(j, p).start()
            c_left(j, p).start()
            spread(j, p)

        @pl.when(z == 1)
        def _():
            finish(0)
            finish(1)

        @pl.when(z == 2)
        def _():
            finish(2)
            finish(3)

    def from_right(j, p, onward):
        c_left(j, p).wait_recv()
        if onward:
            c_left(j, p).start()
        spread(j, p)

    def from_left(j, p, onward):
        c_right(j, p).wait_recv()
        if onward:
            c_right(j, p).start()
        spread(j, p)

    def stage_c1(j):
        @pl.when(z == 0)
        def _():
            from_right(j, 0, False)
            from_right(j, 1, False)

        @pl.when(z == 1)
        def _():
            from_right(j, 2, True)
            from_right(j, 3, True)

        @pl.when(z == 2)
        def _():
            from_left(j, 0, True)
            from_left(j, 1, True)

        @pl.when(z == 3)
        def _():
            from_left(j, 2, False)
            from_left(j, 3, False)

    def stage_c2(j):
        @pl.when(z == 0)
        def _():
            from_right(j, 2, False)
            from_right(j, 3, False)

        @pl.when(z == 3)
        def _():
            from_left(j, 0, False)
            from_left(j, 1, False)

    def stage_over(j):
        for p in range(n_part):
            c_over(j, over, p).wait_recv()
            c_mate(j, over, 1, p).start()

    def stage_out(j):
        for p in range(n_part):
            c_mate(j, mate, 0, p).wait_recv()
            c_mate(j, over_mate, 1, p).wait_recv()
        for q in range(4):
            for p in range(n_part):
                col = width * (n_part * (q % 2) + p)
                rows = pl.ds(pl.multiple_of(64 * j + 32 * (q // 2), 32), 32)
                out_ref[rows, col : col + width] = full[j, q, p].astype(jnp.bfloat16)

    stages = [
        (stage_a1, 1), (stage_a2, 2), (stage_a3, 1), (stage_b1, 2), (stage_c0, 2), (stage_c1, 1), (stage_c2, 1),
        (stage_over, 3), (stage_out, 2),
    ]
    n_slots = 2 * n_seq + 2 + sum(lag for _, lag in stages)

    def slot(s, carry):
        @pl.when(s == 1)
        def _():
            in_copy(1).wait()
            norm_half(1)

        @pl.when((s >= 2) & (s < 2 + n_share))
        def _():
            share_tile(s - 2)

        @pl.when((s >= 4) & (s < 4 + n_share))
        def _():
            take_tile(s - 4)

        @pl.when(s < 2 * n_seq + 2)
        def _():
            attend(s)

        after = 3 + sum(lag for _, lag in stages)
        for stage_fn, lag in reversed(stages):
            t = s - after
            after -= lag

            @pl.when((t >= 0) & (t % 2 == 0) & (t < 2 * n_seq))
            def _():
                stage_fn(t // 2)

        return carry

    lax.fori_loop(0, n_slots, slot, 0)

    def drain(j, carry):
        a1(j).wait_send()
        a2(j).wait_send()
        a3(j, core).wait_send()
        for p in range(n_part):
            @pl.when((z == 0) | ((z == 1) & (p >= 2)))
            def _():
                b_right(j, p).wait_send()

            @pl.when((z == 3) | ((z == 2) & (p < 2)))
            def _():
                b_left(j, p).wait_send()

            @pl.when((z == 2) | ((z == 1) & (p < 2)))
            def _():
                c_right(j, p).wait_send()

            @pl.when((z == 1) | ((z == 2) & (p >= 2)))
            def _():
                c_left(j, p).wait_send()

            c_over(j, c, p).wait_send()
            c_mate(j, c, 0, p).wait_send()
            c_mate(j, over, 1, p).wait_send()
        return carry

    for m in range(n_share):
        share(m).wait_send()
    lax.fori_loop(0, n_seq, drain, 0)


def block(prefix_len, gain, q_gain, k_gain, x2, w_q, w_k, w_v, kc, vc, w_o):
    rows, d_model = x2.shape
    n_seq, cache_rows, _ = kc.shape
    n_part = 4
    width = d_model // (2 * n_part)
    n_q = w_q.shape[1] // 256
    new_rows = 2 * rows // n_seq
    n_share = (n_q + 2) // 2
    tile = min(2048, cache_rows // 2)
    half_dim = HEAD_DIM // 2
    freq = 1.0 / (1000000.0 ** (np.arange(half_dim, dtype=np.float64) * 2.0 / HEAD_DIM))
    freq = jnp.asarray(np.concatenate([freq, freq])[None], jnp.float32)
    hbm = pl.BlockSpec(memory_space=pl.ANY)
    vmem = pl.BlockSpec(memory_space=pltpu.VMEM)
    f32, bf16 = jnp.float32, jnp.bfloat16
    sems = pltpu.SemaphoreType.DMA
    piece = (32, width)
    return pl.pallas_call(
        functools.partial(block_kernel, tile=tile),
        out_shape=(
            pltpu.VMEM((rows, d_model), bf16),
            pltpu.VMEM((2 * rows, 128), bf16),
            pltpu.VMEM((2 * rows, 128), bf16),
        ),
        in_specs=[pl.BlockSpec(memory_space=pltpu.SMEM), vmem, vmem, vmem, vmem, hbm, hbm, hbm, hbm, hbm, hbm, hbm],
        out_specs=(vmem, vmem, vmem),
        scratch_shapes=[
            pltpu.VMEM((n_q, rows, 256), bf16),
            pltpu.VMEM((n_q + 2, d_model, 256), bf16),
            pltpu.VMEM((rows, 128), f32),
            pltpu.VMEM((rows, 128), f32),
            pltpu.VMEM((rows, 128), f32),
            pltpu.VMEM((n_share, rows // 2, 256), f32),
            pltpu.VMEM((n_share, rows // 2, 256), f32),
            pltpu.VMEM((2, cache_rows, 128), bf16),
            pltpu.VMEM((2, cache_rows, 128), bf16),
            pltpu.VMEM((256, 256), bf16),
            pltpu.VMEM((cache_rows, 256), f32),
            pltpu.VMEM((new_rows, 256), f32),
            pltpu.VMEM((256, 256), f32),
            pltpu.VMEM((8, 256), f32),
            pltpu.VMEM((8, 256), f32),
            pltpu.VMEM((8, 256), f32),
            pltpu.VMEM((n_part, w_o.shape[0], width), bf16),
            pltpu.VMEM((n_seq, 32, 2 * width), bf16),
            pltpu.VMEM((n_seq, 2, 136, 256), f32),
            pltpu.VMEM((n_seq, 136, 256), f32),
            pltpu.VMEM((n_seq, 2, 136, 128), f32),
            pltpu.VMEM((n_seq, 136, 128), f32),
            pltpu.VMEM((n_seq, 2, 128, 128), f32),
            pltpu.VMEM((n_seq, n_part, *piece), f32),
            pltpu.VMEM((n_seq, n_part, *piece), f32),
            pltpu.VMEM((n_seq, n_part, *piece), f32),
            pltpu.VMEM((n_seq, 4, n_part, *piece), f32),
            sems((2,)),
            sems((n_q + 2,)),
            sems((2,)),
            sems((2,)),
            sems((n_part,)),
            sems((n_seq,)),
            *[sems((n_seq,))] * 6,
            *[sems((n_share,))] * 2,
            *[sems((n_seq, n_part))] * 10,
            sems((n_seq, 2, n_part)),
            sems((n_seq, 2, n_part)),
        ],
        compiler_params=pltpu.CompilerParams(
            collective_id=0, has_side_effects=True, vmem_limit_bytes=int(58.5 * 1024 * 1024)
        ),
        cost_estimate=pl.CostEstimate(
            flops=4 * n_seq * cache_rows * 256 * 256, bytes_accessed=60 << 20, transcendentals=n_seq * cache_rows * 256
        ),
        name="block",
    )(prefix_len, gain, q_gain, k_gain, freq, x2, w_q, w_k, w_v, kc, vc, w_o)


def store_kernel(out_in, k_in, v_in, out_hbm, k_hbm, v_hbm, sem):
    copies = [
        pltpu.make_async_copy(src, dst, sem.at[i])
        for i, (src, dst) in enumerate(((out_in, out_hbm), (k_in, k_hbm), (v_in, v_hbm)))
    ]
    for copy in copies:
        copy.start()
    for copy in copies:
        copy.wait()


def store(*arrays):
    hbm = pl.BlockSpec(memory_space=pl.ANY)
    return pl.pallas_call(
        store_kernel,
        out_shape=tuple(jax.ShapeDtypeStruct(a.shape, a.dtype) for a in arrays),
        in_specs=[hbm] * 3,
        out_specs=(hbm,) * 3,
        scratch_shapes=[pltpu.SemaphoreType.DMA((3,))],
        compiler_params=pltpu.CompilerParams(vmem_limit_bytes=1024 * 1024),
        name="store",
    )(*arrays)


def solution(mesh):
    def per_device(hidden, prefix_len, k_cache, v_cache, attn_norm, w_q, w_k, w_v, w_o, q_norm, k_norm):
        n_seq, n_new, d_model = hidden.shape
        x2 = hidden.reshape(n_seq * n_new, d_model)
        results = block(
            prefix_len, attn_norm, q_norm, k_norm, x2, w_q, w_k, w_v,
            k_cache.reshape(n_seq, -1, HEAD_DIM), v_cache.reshape(n_seq, -1, HEAD_DIM), w_o,
        )
        out, k_rows, v_rows = store(*results)
        new_shape = (n_seq, n_new, 2, HEAD_DIM)
        return out.reshape(hidden.shape), k_rows.reshape(new_shape), v_rows.reshape(new_shape)

    cache_spec = P("dp", "cp", "tp", None)
    arg_specs = (P("dp", None, None), P("dp"), cache_spec, cache_spec, P(None), P(None, "tp"), P(None, "tp"), P(None, "tp"), P("tp", None), P(None), P(None))
    out_specs = (P("dp", None, None), P("dp", None, "tp", None), P("dp", None, "tp", None))
    return jax.shard_map(per_device, mesh=mesh, in_specs=arg_specs, out_specs=out_specs, check_vma=False)
```

```python
import functools

import jax
import jax.numpy as jnp
import numpy as np
from jax import lax
from jax.experimental import pallas as pl
from jax.experimental.pallas import tpu as pltpu
from jax.sharding import PartitionSpec as P

HEAD_DIM = 128
MASKED = -1e30
EXP2_SCALE = HEAD_DIM**-0.5 * 1.4426950408889634
MESH = pl.DeviceIdType.MESH


def block_kernel(
    len_ref, gain, q_gain, k_gain, freq, x_hbm, wq_hbm, wk_hbm, wv_hbm, kc_hbm, vc_hbm, wo_hbm,
    out_ref, kn_ref, vn_ref,
    q_ref, w_buf, cos_t, sin_t, turn, mine, theirs, kbuf, vbuf, qt, s_buf, sn_buf, acc, top_buf, run_top, run_sum,
    wo, xs, part, got1, chip, got2, ob, prod, from_l, from_r, full,
    x_sem, w_sem, k_sem, v_sem, wo_sem, xs_sem, a1s, a1r, a2s, a2r, a3s, a3r,
    shs, shr, brs, brr, bls, blr, crs, crr, cls, clr, cys, cyr, cps, cpr, *, tile,
):
    dp, z, c = lax.axis_index("dp"), lax.axis_index("tp"), lax.axis_index("cp")
    y, core = c // 2, c % 2
    mate = 2 * y + (1 - core)
    over = 2 * (1 - y) + core
    over_mate = 2 * (1 - y) + (1 - core)
    n_seq, n_part, width = full.shape[0], full.shape[2], full.shape[4]
    last = n_part - 1
    cache_rows = kbuf.shape[1]
    n_new = kn_ref.shape[0] // n_seq
    n_tok = n_new // 2
    n_tiles = cache_rows // tile
    rows, d_model = out_ref.shape
    half_rows = rows // 2
    n_q = wq_hbm.shape[1] // 256

    def send(src, dst, send_sem, recv_sem, tp, cp):
        return pltpu.make_async_remote_copy(
            src_ref=src, dst_ref=dst, send_sem=send_sem, recv_sem=recv_sem, device_id=(dp, tp, cp), device_id_type=MESH
        )

    def k_copy(b):
        return pltpu.make_async_copy(kc_hbm.at[b], kbuf.at[b % 2], k_sem.at[b % 2])

    def v_copy(b):
        return pltpu.make_async_copy(vc_hbm.at[b], vbuf.at[b % 2], v_sem.at[b % 2])

    def wo_copy(p):
        cols = pl.ds(pl.multiple_of(n_part * width * core + width * p, width), width)
        return pltpu.make_async_copy(wo_hbm.at[:, cols], wo.at[p], wo_sem.at[p])

    owner = jnp.clip(z - 1, 0, 1)

    def x_copy(j):
        rows = pl.ds(pl.multiple_of(64 * j + 32 * y, 32), 32)
        cols = pl.ds(pl.multiple_of(n_part * width * core + 2 * width * owner, 2 * width), 2 * width)
        return pltpu.make_async_copy(x_hbm.at[rows, cols], xs.at[j], xs_sem.at[j])

    def in_copy(half):
        sel = pl.ds(half_rows * half, half_rows)
        return pltpu.make_async_copy(x_hbm.at[sel], out_ref.at[sel], x_sem.at[half])

    w_copies = [
        pltpu.make_async_copy(wq_hbm.at[:, pl.ds(256 * i, 256)], w_buf.at[i], w_sem.at[i]) for i in range(n_q)
    ]
    w_copies.append(pltpu.make_async_copy(wk_hbm, w_buf.at[n_q], w_sem.at[n_q]))
    w_copies.append(pltpu.make_async_copy(wv_hbm, w_buf.at[n_q + 1], w_sem.at[n_q + 1]))
    in_copy(0).start()

    barrier = pltpu.get_barrier_semaphore()
    for peer in (mate, over):
        pl.semaphore_signal(barrier, inc=1, device_id=(dp, z, peer), device_id_type=MESH)

    @pl.when(z > 0)
    def _():
        pl.semaphore_signal(barrier, inc=1, device_id=(dp, z - 1, c), device_id_type=MESH)

    @pl.when(z < last)
    def _():
        pl.semaphore_signal(barrier, inc=1, device_id=(dp, z + 1, c), device_id_type=MESH)

    rope_lane = lax.broadcasted_iota(jnp.int32, (n_tok, HEAD_DIM), 1)
    rope_token = lax.broadcasted_iota(jnp.int32, (n_tok, HEAD_DIM), 0)

    def rope_rows(b, carry):
        angle = (rope_token + len_ref[b]).astype(jnp.float32) * freq[...]
        sel = pl.ds(pl.multiple_of(b * (n_tok), n_tok), n_tok)
        cos_t[sel, :] = jnp.cos(angle)
        sin = jnp.sin(angle)
        sin_t[sel, :] = jnp.where(rope_lane < 64, -sin, sin)
        return carry

    lax.fori_loop(0, n_seq, rope_rows, 0)
    x_gain = gain[...].astype(jnp.float32).reshape(1, d_model)

    def norm_half(half):
        def norm_rows(i, carry):
            sel = pl.ds(pl.multiple_of(half * half_rows + i * 32, 32), 32)
            x = out_ref[sel, :].astype(jnp.float32)
            mean_sq = jnp.mean(x * x, axis=-1, keepdims=True)
            out_ref[sel, :] = (x * lax.rsqrt(mean_sq + 1e-6) * x_gain).astype(jnp.bfloat16)
            return carry

        lax.fori_loop(0, half_rows // 32, norm_rows, 0)

    q_gain_row = q_gain[...].astype(jnp.float32).reshape(1, HEAD_DIM)
    k_gain_row = k_gain[...].astype(jnp.float32).reshape(1, HEAD_DIM)

    def half_sel(half):
        return slice(half * half_rows, (half + 1) * half_rows)

    def compute_tile(i, half):
        sel = half_sel(half)
        lin = jnp.dot(out_ref[sel, :], w_buf[i], preferred_element_type=jnp.float32).astype(jnp.bfloat16)
        lin = lin.astype(jnp.float32)
        head_gain = jnp.where(i < n_q, q_gain_row, k_gain_row)
        vals = []
        for u in range(2):
            raw = lin[:, HEAD_DIM * u : HEAD_DIM * u + HEAD_DIM]
            mean_sq = jnp.mean(raw * raw, axis=-1, keepdims=True)
            t = raw * lax.rsqrt(mean_sq + 1e-6) * head_gain
            t = t * cos_t[sel, :] + pltpu.roll(t, 64, 1) * sin_t[sel, :]
            vals.append(jnp.where(i == n_q + 1, raw, t))
        return vals

    def store_tile(i, half, vals):
        sel = half_sel(half)

        @pl.when(i < n_q)
        def _():
            for u in range(2):
                q_ref[i, sel, HEAD_DIM * u : HEAD_DIM * u + HEAD_DIM] = vals[u].astype(jnp.bfloat16)

        @pl.when(i >= n_q)
        def _():
            for u in range(2):
                turn[pl.ds(u, half_rows, stride=2), :] = vals[u]

        new_rows = slice(half * rows, (half + 1) * rows)

        @pl.when(i == n_q)
        def _():
            kn_ref[new_rows, :] = turn[...].astype(jnp.bfloat16)

        @pl.when(i == n_q + 1)
        def _():
            vn_ref[new_rows, :] = turn[...].astype(jnp.bfloat16)

    n_share = (n_q + 2) // 2

    def share(m):
        return send(mine.at[m], theirs.at[m], shs.at[m], shr.at[m], z, mate)

    def share_tile(m):
        i = 2 * m + core
        vals = compute_tile(i, 1)
        for u in range(2):
            mine[m, :, HEAD_DIM * u : HEAD_DIM * u + HEAD_DIM] = vals[u]
        share(m).start()
        store_tile(i, 1, vals)

    def take_tile(m):
        share(m).wait_recv()
        store_tile(2 * m + 1 - core, 1, [theirs[m, :, HEAD_DIM * u : HEAD_DIM * u + HEAD_DIM] for u in range(2)])

    in_copy(0).wait()
    for copy in w_copies:
        copy.start()
    norm_half(0)
    k_copy(0).start()
    in_copy(1).start()

    def first_tile(i, carry):
        pltpu.make_async_copy(w_buf.at[i], w_buf.at[i], w_sem.at[i]).wait()
        store_tile(i, 0, compute_tile(i, 0))
        return carry

    lax.fori_loop(0, n_q + 2, first_tile, 0)
    v_copy(0).start()
    for p in range(n_part):
        wo_copy(p).start()
    for j in range(n_seq):
        x_copy(j).start()

    @pl.when((z == 0) | (z == last))
    def _():
        pl.semaphore_wait(barrier, 3)

    @pl.when((z > 0) & (z < last))
    def _():
        pl.semaphore_wait(barrier, 4)

    sub16 = lax.broadcasted_iota(jnp.int32, (16, HEAD_DIM), 0) & 1
    even_rows = jnp.where(sub16 == 0, 1.0, 0.0).astype(jnp.bfloat16)
    odd_rows = jnp.where(sub16 == 0, 0.0, 1.0).astype(jnp.bfloat16)
    sub8 = lax.broadcasted_iota(jnp.int32, (8, 256), 0) & 1

    def split_rows(k):
        n = k.shape[0]
        k3 = k.reshape(n // 16, 16, HEAD_DIM)
        return jnp.concatenate(
            [(k3 * even_rows[None]).reshape(n, HEAD_DIM), (k3 * odd_rows[None]).reshape(n, HEAD_DIM)], axis=1
        )

    def split_lanes(v):
        n = v.shape[0]
        lane = lax.broadcasted_iota(jnp.int32, (16, n), 1) & 1
        even = jnp.where(lane == 0, 1.0, 0.0).astype(jnp.bfloat16)
        odd = jnp.where(lane == 0, 0.0, 1.0).astype(jnp.bfloat16)
        vt = v.T.reshape(8, 16, n)
        return jnp.concatenate([(vt * even[None]).reshape(HEAD_DIM, n), (vt * odd[None]).reshape(HEAD_DIM, n)], axis=0)

    def scores(k):
        return jnp.dot(split_rows(k), qt[...], preferred_element_type=jnp.float32)

    def fetch(b):
        @pl.when(b + 1 < n_seq)
        def _():
            k_copy(b + 1).start()

        @pl.when((b > 0) & (b < n_seq))
        def _():
            v_copy(b).start()

    def score_start(b):
        q_rows = pl.multiple_of(64 * b, 64)
        for h in range(2):
            blocks = [
                q_ref[h * 2 + g // 2, pl.ds(q_rows + th * 32, 32), (g % 2) * HEAD_DIM : (g % 2) * HEAD_DIM + HEAD_DIM]
                for th in range(2)
                for g in range(4)
            ]
            qt[h * HEAD_DIM : h * HEAD_DIM + HEAD_DIM, :] = jnp.concatenate(blocks, axis=0).T
        run_top[...] = jnp.full((8, 256), MASKED, jnp.float32)
        k_copy(b).wait()

    def score_tile(b, t):
        sel = pl.ds(pl.multiple_of(t * tile, tile), tile)
        n_rows = 2 * (len_ref[b] - c * (cache_rows // 2)) - t * tile
        s = scores(kbuf[b % 2, sel, :])
        s = jnp.where(lax.broadcasted_iota(jnp.int32, (tile, 256), 0) < n_rows, s, MASKED)
        s_buf[sel, :] = s
        run_top[...] = jnp.maximum(run_top[...], jnp.max(s.reshape(tile // 8, 8, 256), axis=0))

    def score_end(b):
        key = lax.broadcasted_iota(jnp.int32, (n_new, 256), 0) // 2
        col = lax.broadcasted_iota(jnp.int32, (n_new, 256), 1)
        token = (col // HEAD_DIM) * 32 + (col % 32)
        token = jnp.where(c == 3, token, -1)
        s_new = jnp.where(key <= token, scores(kn_ref[pl.ds(pl.multiple_of(n_new * b, n_new), n_new), :]), MASKED)
        sn_buf[...] = s_new
        top = jnp.maximum(run_top[...], jnp.max(s_new.reshape(n_new // 8, 8, 256), axis=0))
        top0 = jnp.max(jnp.where(sub8 == 0, top, MASKED), axis=0, keepdims=True)
        top1 = jnp.max(jnp.where(sub8 == 0, MASKED, top), axis=0, keepdims=True)
        top_buf[...] = jnp.where(sub8 == 0, top0, top1)

    def weigh(s, v):
        top = top_buf[...]
        base = jnp.where(top > 0.5 * MASKED, top, 0.0)
        n = s.shape[0]
        p = jnp.exp2((s.reshape(n // 8, 8, 256) - base[None]) * EXP2_SCALE)
        out = jnp.dot(split_lanes(v), p.reshape(n, 256).astype(jnp.bfloat16), preferred_element_type=jnp.float32)
        return jnp.sum(p, axis=0), out

    def weigh_start(b):
        run_sum[...], acc[...] = weigh(sn_buf[...], vn_ref[pl.ds(pl.multiple_of(n_new * b, n_new), n_new), :])
        v_copy(b).wait()

    def weigh_tile(b, t):
        sel = pl.ds(pl.multiple_of(t * tile, tile), tile)
        more, out = weigh(s_buf[sel, :], vbuf[b % 2, sel, :])
        acc[...] += out
        run_sum[...] += more

    def weigh_end(b):
        total = run_sum[...]
        pad = jnp.zeros((6, 256), jnp.float32)
        for h in range(2):
            part[b, h, 0:HEAD_DIM, :] = acc[h * HEAD_DIM : h * HEAD_DIM + HEAD_DIM, :]
            total_h = jnp.sum(jnp.where(sub8 == h, total, 0.0), axis=0, keepdims=True)
            part[b, h, HEAD_DIM:136, :] = jnp.concatenate([top_buf[h : h + 1, :], total_h, pad], axis=0)
        a1(b).start()

    def attend(s):
        b, first = s // 2, s % 2 == 0

        @pl.when(first)
        def _():
            fetch(b)

        @pl.when(first & (b < n_seq))
        def _():
            score_start(b)

        @pl.when(first & (b > 0))
        def _():
            weigh_start(b - 1)

        def tiles(body):
            def one(i, carry):
                body((s % 2) * (n_tiles // 2) + i)
                return carry

            lax.fori_loop(0, n_tiles // 2, one, 0)

        @pl.when(b == 0)
        def _():
            tiles(lambda t: score_tile(b, t))

        @pl.when((b > 0) & (b < n_seq))
        def _():
            def both(t):
                weigh_tile(b - 1, t)
                score_tile(b, t)

            tiles(both)

        @pl.when(b == n_seq)
        def _():
            tiles(lambda t: weigh_tile(b - 1, t))

        @pl.when((s % 2 == 1) & (b > 0))
        def _():
            weigh_end(b - 1)

        @pl.when((s % 2 == 1) & (b < n_seq))
        def _():
            score_end(b)

    def a1(j):
        return send(part.at[j, 1 - core], got1.at[j], a1s.at[j], a1r.at[j], z, mate)

    def a2(j):
        return send(chip.at[j, 1 - y], got2.at[j], a2s.at[j], a2r.at[j], z, over)

    def a3(j, h):
        return send(ob.at[j, h], ob.at[j, h], a3s.at[j], a3r.at[j], z, mate)

    def b_right(j, p):
        return send(prod.at[j, p], from_l.at[j, p], brs.at[j, p], brr.at[j, p], z + 1, c)

    def b_left(j, p):
        return send(prod.at[j, p], from_r.at[j, p], bls.at[j, p], blr.at[j, p], z - 1, c)

    def c_right(j, p):
        return send(full.at[j, c, p], full.at[j, c, p], crs.at[j, p], crr.at[j, p], z + 1, c)

    def c_left(j, p):
        return send(full.at[j, c, p], full.at[j, c, p], cls.at[j, p], clr.at[j, p], z - 1, c)

    def c_over(j, q, p):
        return send(full.at[j, q, p], full.at[j, q, p], cys.at[j, p], cyr.at[j, p], z, over)

    def c_mate(j, q, u, p):
        return send(full.at[j, q, p], full.at[j, q, p], cps.at[j, u, p], cpr.at[j, u, p], z, mate)

    def merge(a, b):
        top = jnp.maximum(a[HEAD_DIM:129], b[HEAD_DIM:129])
        fa = jnp.exp2((a[HEAD_DIM:129] - top) * EXP2_SCALE)
        fb = jnp.exp2((b[HEAD_DIM:129] - top) * EXP2_SCALE)
        return a[0:HEAD_DIM] * fa + b[0:HEAD_DIM] * fb, top, a[129:130] * fa + b[129:130] * fb

    def stage_a1(j):
        a1(j).wait_recv()
        vals, top, total = merge(part[j, core], got1[j])
        for th in range(2):
            sel = slice(HEAD_DIM * th, HEAD_DIM * th + HEAD_DIM)
            chip[j, th, 0:HEAD_DIM] = vals[:, sel]
            chip[j, th, HEAD_DIM:136] = jnp.concatenate([top[:, sel], total[:, sel], jnp.zeros((6, HEAD_DIM), jnp.float32)], axis=0)
        a2(j).start()

    def stage_a2(j):
        a2(j).wait_recv()
        vals, _, total = merge(chip[j, y], got2[j])
        ob[j, core] = (vals / total).T
        a3(j, core).start()

    def stage_a3(j):
        a3(j, 1 - core).wait_recv()

        @pl.when(j == 0)
        def _():
            for p in range(n_part):
                wo_copy(p).wait()

        o = jnp.concatenate([ob[j, h, 32 * g : 32 * g + 32, :] for h in range(2) for g in range(4)], axis=1)
        o = o.astype(jnp.bfloat16)
        for p in range(n_part):
            prod[j, p] = jnp.dot(o, wo[p], preferred_element_type=jnp.float32)

        @pl.when(z == 0)
        def _():
            for p in (2, 3, 0, 1):
                b_right(j, p).start()

        @pl.when(z == last)
        def _():
            for p in (0, 1, 2, 3):
                b_left(j, p).start()

    def pass_right(j, p):
        b_right(j, p).wait_recv()
        prod[j, p] = prod[j, p] + from_l[j, p]
        b_right(j, p).start()

    def pass_left(j, p):
        b_left(j, p).wait_recv()
        prod[j, p] = prod[j, p] + from_r[j, p]
        b_left(j, p).start()

    def stage_b1(j):
        @pl.when(z == 1)
        def _():
            pass_right(j, 2)
            pass_right(j, 3)

        @pl.when(z == 2)
        def _():
            pass_left(j, 0)
            pass_left(j, 1)

    def spread(j, p):
        c_over(j, c, p).start()
        c_mate(j, c, 0, p).start()

    def stage_c0(j):
        x_copy(j).wait()

        def finish(p):
            b_right(j, p).wait_recv()
            b_left(j, p).wait_recv()
            x = xs[j, :, width * (p % 2) : width * (p % 2) + width].astype(jnp.float32)
            full[j, c, p] = prod[j, p] + from_l[j, p] + from_r[j, p] + x
            c_right(j, p).start()
            c_left(j, p).start()
            spread(j, p)

        @pl.when(z == 1)
        def _():
            finish(0)
            finish(1)

        @pl.when(z == 2)
        def _():
            finish(2)
            finish(3)

    def from_right(j, p, onward):
        c_left(j, p).wait_recv()
        if onward:
            c_left(j, p).start()
        spread(j, p)

    def from_left(j, p, onward):
        c_right(j, p).wait_recv()
        if onward:
            c_right(j, p).start()
        spread(j, p)

    def stage_c1(j):
        @pl.when(z == 0)
        def _():
            from_right(j, 0, False)
            from_right(j, 1, False)

        @pl.when(z == 1)
        def _():
            from_right(j, 2, True)
            from_right(j, 3, True)

        @pl.when(z == 2)
        def _():
            from_left(j, 0, True)
            from_left(j, 1, True)

        @pl.when(z == 3)
        def _():
            from_left(j, 2, False)
            from_left(j, 3, False)

    def stage_c2(j):
        @pl.when(z == 0)
        def _():
            from_right(j, 2, False)
            from_right(j, 3, False)

        @pl.when(z == 3)
        def _():
            from_left(j, 0, False)
            from_left(j, 1, False)

    def stage_over(j):
        for p in range(n_part):
            c_over(j, over, p).wait_recv()
            c_mate(j, over, 1, p).start()

    def stage_out(j):
        for p in range(n_part):
            c_mate(j, mate, 0, p).wait_recv()
            c_mate(j, over_mate, 1, p).wait_recv()
        for q in range(4):
            for p in range(n_part):
                col = width * (n_part * (q % 2) + p)
                rows = pl.ds(pl.multiple_of(64 * j + 32 * (q // 2), 32), 32)
                out_ref[rows, col : col + width] = full[j, q, p].astype(jnp.bfloat16)

    stages = [
        (stage_a1, 1), (stage_a2, 2), (stage_a3, 1), (stage_b1, 2), (stage_c0, 2), (stage_c1, 1), (stage_c2, 1),
        (stage_over, 3), (stage_out, 2),
    ]
    n_slots = 2 * n_seq + 2 + sum(lag for _, lag in stages)

    def slot(s, carry):
        @pl.when(s == 1)
        def _():
            in_copy(1).wait()
            norm_half(1)

        @pl.when((s >= 2) & (s < 2 + n_share))
        def _():
            share_tile(s - 2)

        @pl.when((s >= 4) & (s < 4 + n_share))
        def _():
            take_tile(s - 4)

        @pl.when(s < 2 * n_seq + 2)
        def _():
            attend(s)

        after = 3 + sum(lag for _, lag in stages)
        for stage_fn, lag in reversed(stages):
            t = s - after
            after -= lag

            @pl.when((t >= 0) & (t % 2 == 0) & (t < 2 * n_seq))
            def _():
                stage_fn(t // 2)

        return carry

    lax.fori_loop(0, n_slots, slot, 0)

    def drain(j, carry):
        a1(j).wait_send()
        a2(j).wait_send()
        a3(j, core).wait_send()
        for p in range(n_part):
            @pl.when((z == 0) | ((z == 1) & (p >= 2)))
            def _():
                b_right(j, p).wait_send()

            @pl.when((z == 3) | ((z == 2) & (p < 2)))
            def _():
                b_left(j, p).wait_send()

            @pl.when((z == 2) | ((z == 1) & (p < 2)))
            def _():
                c_right(j, p).wait_send()

            @pl.when((z == 1) | ((z == 2) & (p >= 2)))
            def _():
                c_left(j, p).wait_send()

            c_over(j, c, p).wait_send()
            c_mate(j, c, 0, p).wait_send()
            c_mate(j, over, 1, p).wait_send()
        return carry

    for m in range(n_share):
        share(m).wait_send()
    lax.fori_loop(0, n_seq, drain, 0)


def block(prefix_len, gain, q_gain, k_gain, x2, w_q, w_k, w_v, kc, vc, w_o):
    rows, d_model = x2.shape
    n_seq, cache_rows, _ = kc.shape
    n_part = 4
    width = d_model // (2 * n_part)
    n_q = w_q.shape[1] // 256
    new_rows = 2 * rows // n_seq
    n_share = (n_q + 2) // 2
    tile = min(2048, cache_rows // 2)
    half_dim = HEAD_DIM // 2
    freq = 1.0 / (1000000.0 ** (np.arange(half_dim, dtype=np.float64) * 2.0 / HEAD_DIM))
    freq = jnp.asarray(np.concatenate([freq, freq])[None], jnp.float32)
    hbm = pl.BlockSpec(memory_space=pl.ANY)
    vmem = pl.BlockSpec(memory_space=pltpu.VMEM)
    f32, bf16 = jnp.float32, jnp.bfloat16
    sems = pltpu.SemaphoreType.DMA
    piece = (32, width)
    return pl.pallas_call(
        functools.partial(block_kernel, tile=tile),
        out_shape=(
            pltpu.VMEM((rows, d_model), bf16),
            pltpu.VMEM((2 * rows, HEAD_DIM), bf16),
            pltpu.VMEM((2 * rows, HEAD_DIM), bf16),
        ),
        in_specs=[pl.BlockSpec(memory_space=pltpu.SMEM), vmem, vmem, vmem, vmem, hbm, hbm, hbm, hbm, hbm, hbm, hbm],
        out_specs=(vmem, vmem, vmem),
        scratch_shapes=[
            pltpu.VMEM((n_q, rows, 256), bf16),
            pltpu.VMEM((n_q + 2, d_model, 256), bf16),
            pltpu.VMEM((rows, HEAD_DIM), f32),
            pltpu.VMEM((rows, HEAD_DIM), f32),
            pltpu.VMEM((rows, HEAD_DIM), f32),
            pltpu.VMEM((n_share, rows // 2, 256), f32),
            pltpu.VMEM((n_share, rows // 2, 256), f32),
            pltpu.VMEM((2, cache_rows, HEAD_DIM), bf16),
            pltpu.VMEM((2, cache_rows, HEAD_DIM), bf16),
            pltpu.VMEM((256, 256), bf16),
            pltpu.VMEM((cache_rows, 256), f32),
            pltpu.VMEM((new_rows, 256), f32),
            pltpu.VMEM((256, 256), f32),
            pltpu.VMEM((8, 256), f32),
            pltpu.VMEM((8, 256), f32),
            pltpu.VMEM((8, 256), f32),
            pltpu.VMEM((n_part, w_o.shape[0], width), bf16),
            pltpu.VMEM((n_seq, 32, 2 * width), bf16),
            pltpu.VMEM((n_seq, 2, 136, 256), f32),
            pltpu.VMEM((n_seq, 136, 256), f32),
            pltpu.VMEM((n_seq, 2, 136, HEAD_DIM), f32),
            pltpu.VMEM((n_seq, 136, HEAD_DIM), f32),
            pltpu.VMEM((n_seq, 2, HEAD_DIM, HEAD_DIM), f32),
            pltpu.VMEM((n_seq, n_part, *piece), f32),
            pltpu.VMEM((n_seq, n_part, *piece), f32),
            pltpu.VMEM((n_seq, n_part, *piece), f32),
            pltpu.VMEM((n_seq, 4, n_part, *piece), f32),
            sems((2,)),
            sems((n_q + 2,)),
            sems((2,)),
            sems((2,)),
            sems((n_part,)),
            sems((n_seq,)),
            *[sems((n_seq,))] * 6,
            *[sems((n_share,))] * 2,
            *[sems((n_seq, n_part))] * 10,
            sems((n_seq, 2, n_part)),
            sems((n_seq, 2, n_part)),
        ],
        compiler_params=pltpu.CompilerParams(
            collective_id=0, has_side_effects=True, vmem_limit_bytes=int(58.5 * 1024 * 1024)
        ),
        cost_estimate=pl.CostEstimate(
            flops=4 * n_seq * cache_rows * 256 * 256, bytes_accessed=60 << 20, transcendentals=n_seq * cache_rows * 256
        ),
        name="block",
    )(prefix_len, gain, q_gain, k_gain, freq, x2, w_q, w_k, w_v, kc, vc, w_o)


def store_kernel(out_in, k_in, v_in, out_hbm, k_hbm, v_hbm, sem):
    copies = [
        pltpu.make_async_copy(src, dst, sem.at[i])
        for i, (src, dst) in enumerate(((out_in, out_hbm), (k_in, k_hbm), (v_in, v_hbm)))
    ]
    for copy in copies:
        copy.start()
    for copy in copies:
        copy.wait()


def store(*arrays):
    hbm = pl.BlockSpec(memory_space=pl.ANY)
    return pl.pallas_call(
        store_kernel,
        out_shape=tuple(jax.ShapeDtypeStruct(a.shape, a.dtype) for a in arrays),
        in_specs=[hbm] * 3,
        out_specs=(hbm,) * 3,
        scratch_shapes=[pltpu.SemaphoreType.DMA((3,))],
        compiler_params=pltpu.CompilerParams(vmem_limit_bytes=1024 * 1024),
        name="store",
    )(*arrays)


def solution(mesh):
    def per_device(hidden, prefix_len, k_cache, v_cache, attn_norm, w_q, w_k, w_v, w_o, q_norm, k_norm):
        n_seq, n_new, d_model = hidden.shape
        x2 = hidden.reshape(n_seq * n_new, d_model)
        results = block(
            prefix_len, attn_norm, q_norm, k_norm, x2, w_q, w_k, w_v,
            k_cache.reshape(n_seq, -1, HEAD_DIM), v_cache.reshape(n_seq, -1, HEAD_DIM), w_o,
        )
        out, k_rows, v_rows = store(*results)
        new_shape = (n_seq, n_new, 2, HEAD_DIM)
        return out.reshape(hidden.shape), k_rows.reshape(new_shape), v_rows.reshape(new_shape)

    cache_spec = P("dp", "cp", "tp", None)
    arg_specs = (P("dp", None, None), P("dp"), cache_spec, cache_spec, P(None), P(None, "tp"), P(None, "tp"), P(None, "tp"), P("tp", None), P(None), P(None))
    out_specs = (P("dp", None, None), P("dp", None, "tp", None), P("dp", None, "tp", None))
    return jax.shard_map(per_device, mesh=mesh, in_specs=arg_specs, out_specs=out_specs, check_vma=False)
```

```python
import functools

import jax
import jax.numpy as jnp
import numpy as np
from jax import lax
from jax.experimental import pallas as pl
from jax.experimental.pallas import tpu as pltpu
from jax.sharding import PartitionSpec as P

HEAD_DIM = 128
MASKED = -1e30
EXP2_SCALE = HEAD_DIM**-0.5 * 1.4426950408889634
MESH = pl.DeviceIdType.MESH


def block_kernel(
    len_ref, gain, q_gain, k_gain, freq, x_hbm, wq_hbm, wk_hbm, wv_hbm, kc_hbm, vc_hbm, wo_hbm,
    out_ref, kn_ref, vn_ref,
    q_ref, w_buf, cos_t, sin_t, turn, mine, theirs, kbuf, vbuf, qt, s_buf, sn_buf, acc, top_buf, run_top, run_sum,
    wo, xs, part, got1, chip, got2, ob, prod, from_l, from_r, full,
    x_sem, w_sem, k_sem, v_sem, wo_sem, xs_sem, a1s, a1r, a2s, a2r, a3s, a3r,
    shs, shr, brs, brr, bls, blr, crs, crr, cls, clr, cys, cyr, cps, cpr, *, tile,
):
    dp, z, c = lax.axis_index("dp"), lax.axis_index("tp"), lax.axis_index("cp")
    y, core = c // 2, c % 2
    mate = 2 * y + (1 - core)
    over = 2 * (1 - y) + core
    over_mate = 2 * (1 - y) + (1 - core)
    n_seq, n_part, width = full.shape[0], full.shape[2], full.shape[4]
    last = n_part - 1
    cache_rows = kbuf.shape[1]
    n_new = kn_ref.shape[0] // n_seq
    n_tok = n_new // 2
    n_tiles = cache_rows // tile
    rows, d_model = out_ref.shape
    half_rows = rows // 2
    n_q = wq_hbm.shape[1] // 256

    def send(src, dst, send_sem, recv_sem, tp, cp):
        return pltpu.make_async_remote_copy(
            src_ref=src, dst_ref=dst, send_sem=send_sem, recv_sem=recv_sem, device_id=(dp, tp, cp), device_id_type=MESH
        )

    def k_copy(b):
        return pltpu.make_async_copy(kc_hbm.at[b], kbuf.at[b % 2], k_sem.at[b % 2])

    def v_copy(b):
        return pltpu.make_async_copy(vc_hbm.at[b], vbuf.at[b % 2], v_sem.at[b % 2])

    def wo_copy(p):
        cols = pl.ds(pl.multiple_of(n_part * width * core + width * p, width), width)
        return pltpu.make_async_copy(wo_hbm.at[:, cols], wo.at[p], wo_sem.at[p])

    owner = jnp.clip(z - 1, 0, 1)

    def x_copy(j):
        rows = pl.ds(pl.multiple_of(64 * j + 32 * y, 32), 32)
        cols = pl.ds(pl.multiple_of(n_part * width * core + 2 * width * owner, 2 * width), 2 * width)
        return pltpu.make_async_copy(x_hbm.at[rows, cols], xs.at[j], xs_sem.at[j])

    def in_copy(half):
        sel = pl.ds(half_rows * half, half_rows)
        return pltpu.make_async_copy(x_hbm.at[sel], out_ref.at[sel], x_sem.at[half])

    w_copies = [
        pltpu.make_async_copy(wq_hbm.at[:, pl.ds(256 * i, 256)], w_buf.at[i], w_sem.at[i]) for i in range(n_q)
    ]
    w_copies.append(pltpu.make_async_copy(wk_hbm, w_buf.at[n_q], w_sem.at[n_q]))
    w_copies.append(pltpu.make_async_copy(wv_hbm, w_buf.at[n_q + 1], w_sem.at[n_q + 1]))
    in_copy(0).start()

    barrier = pltpu.get_barrier_semaphore()
    for peer in (mate, over):
        pl.semaphore_signal(barrier, inc=1, device_id=(dp, z, peer), device_id_type=MESH)

    @pl.when(z > 0)
    def _():
        pl.semaphore_signal(barrier, inc=1, device_id=(dp, z - 1, c), device_id_type=MESH)

    @pl.when(z < last)
    def _():
        pl.semaphore_signal(barrier, inc=1, device_id=(dp, z + 1, c), device_id_type=MESH)

    rope_lane = lax.broadcasted_iota(jnp.int32, (n_tok, HEAD_DIM), 1)
    rope_token = lax.broadcasted_iota(jnp.int32, (n_tok, HEAD_DIM), 0)

    def rope_rows(b, carry):
        angle = (rope_token + len_ref[b]).astype(jnp.float32) * freq[...]
        sel = pl.ds(pl.multiple_of(b * (n_tok), n_tok), n_tok)
        cos_t[sel, :] = jnp.cos(angle)
        sin = jnp.sin(angle)
        sin_t[sel, :] = jnp.where(rope_lane < 64, -sin, sin)
        return carry

    lax.fori_loop(0, n_seq, rope_rows, 0)
    x_gain = gain[...].astype(jnp.float32).reshape(1, d_model)

    def norm_half(half):
        def norm_rows(i, carry):
            sel = pl.ds(pl.multiple_of(half * half_rows + i * 32, 32), 32)
            x = out_ref[sel, :].astype(jnp.float32)
            mean_sq = jnp.mean(x * x, axis=-1, keepdims=True)
            out_ref[sel, :] = (x * lax.rsqrt(mean_sq + 1e-6) * x_gain).astype(jnp.bfloat16)
            return carry

        lax.fori_loop(0, half_rows // 32, norm_rows, 0)

    q_gain_row = q_gain[...].astype(jnp.float32).reshape(1, HEAD_DIM)
    k_gain_row = k_gain[...].astype(jnp.float32).reshape(1, HEAD_DIM)

    def half_sel(half):
        return slice(half * half_rows, (half + 1) * half_rows)

    def compute_tile(i, half):
        sel = half_sel(half)
        lin = jnp.dot(out_ref[sel, :], w_buf[i], preferred_element_type=jnp.float32).astype(jnp.bfloat16)
        lin = lin.astype(jnp.float32)
        head_gain = jnp.where(i < n_q, q_gain_row, k_gain_row)
        vals = []
        for u in range(2):
            raw = lin[:, HEAD_DIM * u : HEAD_DIM * u + HEAD_DIM]
            mean_sq = jnp.mean(raw * raw, axis=-1, keepdims=True)
            t = raw * lax.rsqrt(mean_sq + 1e-6) * head_gain
            t = t * cos_t[sel, :] + pltpu.roll(t, 64, 1) * sin_t[sel, :]
            vals.append(jnp.where(i == n_q + 1, raw, t))
        return vals

    def store_tile(i, half, vals):
        sel = half_sel(half)

        @pl.when(i < n_q)
        def _():
            for u in range(2):
                q_ref[i, sel, HEAD_DIM * u : HEAD_DIM * u + HEAD_DIM] = vals[u].astype(jnp.bfloat16)

        @pl.when(i >= n_q)
        def _():
            for u in range(2):
                turn[pl.ds(u, half_rows, stride=2), :] = vals[u]

        new_rows = slice(half * rows, (half + 1) * rows)

        @pl.when(i == n_q)
        def _():
            kn_ref[new_rows, :] = turn[...].astype(jnp.bfloat16)

        @pl.when(i == n_q + 1)
        def _():
            vn_ref[new_rows, :] = turn[...].astype(jnp.bfloat16)

    n_share = (n_q + 2) // 2

    def share(m):
        return send(mine.at[m], theirs.at[m], shs.at[m], shr.at[m], z, mate)

    def share_tile(m):
        i = 2 * m + core
        vals = compute_tile(i, 1)
        for u in range(2):
            mine[m, :, HEAD_DIM * u : HEAD_DIM * u + HEAD_DIM] = vals[u]
        share(m).start()
        store_tile(i, 1, vals)

    def take_tile(m):
        share(m).wait_recv()
        store_tile(2 * m + 1 - core, 1, [theirs[m, :, HEAD_DIM * u : HEAD_DIM * u + HEAD_DIM] for u in range(2)])

    in_copy(0).wait()
    for copy in w_copies:
        copy.start()
    norm_half(0)
    k_copy(0).start()
    in_copy(1).start()

    def first_tile(i, carry):
        pltpu.make_async_copy(w_buf.at[i], w_buf.at[i], w_sem.at[i]).wait()
        store_tile(i, 0, compute_tile(i, 0))
        return carry

    lax.fori_loop(0, n_q + 2, first_tile, 0)
    v_copy(0).start()
    for p in range(n_part):
        wo_copy(p).start()
    for j in range(n_seq):
        x_copy(j).start()

    @pl.when((z == 0) | (z == last))
    def _():
        pl.semaphore_wait(barrier, 3)

    @pl.when((z > 0) & (z < last))
    def _():
        pl.semaphore_wait(barrier, 4)

    sub16 = lax.broadcasted_iota(jnp.int32, (16, HEAD_DIM), 0) & 1
    even_rows = jnp.where(sub16 == 0, 1.0, 0.0).astype(jnp.bfloat16)
    odd_rows = jnp.where(sub16 == 0, 0.0, 1.0).astype(jnp.bfloat16)
    sub8 = lax.broadcasted_iota(jnp.int32, (8, 256), 0) & 1

    def split_rows(k):
        n = k.shape[0]
        k3 = k.reshape(n // 16, 16, HEAD_DIM)
        return jnp.concatenate(
            [(k3 * even_rows[None]).reshape(n, HEAD_DIM), (k3 * odd_rows[None]).reshape(n, HEAD_DIM)], axis=1
        )

    def split_lanes(v):
        n = v.shape[0]
        lane = lax.broadcasted_iota(jnp.int32, (16, n), 1) & 1
        even = jnp.where(lane == 0, 1.0, 0.0).astype(jnp.bfloat16)
        odd = jnp.where(lane == 0, 0.0, 1.0).astype(jnp.bfloat16)
        vt = v.T.reshape(8, 16, n)
        return jnp.concatenate([(vt * even[None]).reshape(HEAD_DIM, n), (vt * odd[None]).reshape(HEAD_DIM, n)], axis=0)

    def scores(k):
        return jnp.dot(split_rows(k), qt[...], preferred_element_type=jnp.float32)

    def fetch(b):
        @pl.when(b + 1 < n_seq)
        def _():
            k_copy(b + 1).start()

        @pl.when((b > 0) & (b < n_seq))
        def _():
            v_copy(b).start()

    def score_start(b):
        q_rows = pl.multiple_of(64 * b, 64)
        for h in range(2):
            blocks = [
                q_ref[h * 2 + g // 2, pl.ds(q_rows + th * 32, 32), (g % 2) * HEAD_DIM : (g % 2) * HEAD_DIM + HEAD_DIM]
                for th in range(2)
                for g in range(4)
            ]
            qt[h * HEAD_DIM : h * HEAD_DIM + HEAD_DIM, :] = jnp.concatenate(blocks, axis=0).T
        run_top[...] = jnp.full((8, 256), MASKED, jnp.float32)
        k_copy(b).wait()

    def score_tile(b, t):
        sel = pl.ds(pl.multiple_of(t * tile, tile), tile)
        n_rows = 2 * (len_ref[b] - c * (cache_rows // 2)) - t * tile
        s = scores(kbuf[b % 2, sel, :])
        s = jnp.where(lax.broadcasted_iota(jnp.int32, (tile, 256), 0) < n_rows, s, MASKED)
        s_buf[sel, :] = s
        run_top[...] = jnp.maximum(run_top[...], jnp.max(s.reshape(tile // 8, 8, 256), axis=0))

    def score_end(b):
        key = lax.broadcasted_iota(jnp.int32, (n_new, 256), 0) // 2
        col = lax.broadcasted_iota(jnp.int32, (n_new, 256), 1)
        token = (col // HEAD_DIM) * 32 + (col % 32)
        token = jnp.where(c == 3, token, -1)
        s_new = jnp.where(key <= token, scores(kn_ref[pl.ds(pl.multiple_of(n_new * b, n_new), n_new), :]), MASKED)
        sn_buf[...] = s_new
        top = jnp.maximum(run_top[...], jnp.max(s_new.reshape(n_new // 8, 8, 256), axis=0))
        top0 = jnp.max(jnp.where(sub8 == 0, top, MASKED), axis=0, keepdims=True)
        top1 = jnp.max(jnp.where(sub8 == 0, MASKED, top), axis=0, keepdims=True)
        top_buf[...] = jnp.where(sub8 == 0, top0, top1)

    def weigh(s, v):
        top = top_buf[...]
        base = jnp.where(top > 0.5 * MASKED, top, 0.0)
        n = s.shape[0]
        p = jnp.exp2((s.reshape(n // 8, 8, 256) - base[None]) * EXP2_SCALE)
        out = jnp.dot(split_lanes(v), p.reshape(n, 256).astype(jnp.bfloat16), preferred_element_type=jnp.float32)
        return jnp.sum(p, axis=0), out

    def weigh_start(b):
        run_sum[...], acc[...] = weigh(sn_buf[...], vn_ref[pl.ds(pl.multiple_of(n_new * b, n_new), n_new), :])
        v_copy(b).wait()

    def weigh_tile(b, t):
        sel = pl.ds(pl.multiple_of(t * tile, tile), tile)
        more, out = weigh(s_buf[sel, :], vbuf[b % 2, sel, :])
        acc[...] += out
        run_sum[...] += more

    def weigh_end(b):
        total = run_sum[...]
        pad = jnp.zeros((6, 256), jnp.float32)
        for h in range(2):
            part[b, h, 0:HEAD_DIM, :] = acc[h * HEAD_DIM : h * HEAD_DIM + HEAD_DIM, :]
            total_h = jnp.sum(jnp.where(sub8 == h, total, 0.0), axis=0, keepdims=True)
            part[b, h, HEAD_DIM:136, :] = jnp.concatenate([top_buf[h : h + 1, :], total_h, pad], axis=0)
        a1(b).start()

    def attend(s):
        b, first = s // 2, s % 2 == 0

        def tiles(body, start, count):
            def one(i, carry):
                body(start + i)
                return carry

            lax.fori_loop(0, count, one, 0)

        half = n_tiles // 2
        start = jnp.where(b == 0, 0, (s % 2) * half)
        count = jnp.where(b == 0, n_tiles, half)

        @pl.when(first)
        def _():
            fetch(b)

        @pl.when(first & (b < n_seq))
        def _():
            score_start(b)

        @pl.when((first & (b > 1)) | (s == 1))
        def _():
            weigh_start(jnp.where(s == 1, 0, b - 1))

        @pl.when((s == 0) | (b == 1))
        def _():
            tiles(lambda t: score_tile(b, t), start, count)

        @pl.when((b > 1) & (b < n_seq))
        def _():
            def both(t):
                weigh_tile(b - 1, t)
                score_tile(b, t)

            tiles(both, start, half)

        @pl.when((s == 1) | (b == n_seq))
        def _():
            tiles(lambda t: weigh_tile(jnp.where(s == 1, 0, b - 1), t), start, count)

        @pl.when(((s % 2 == 1) & (b > 1)) | (s == 1))
        def _():
            weigh_end(jnp.where(s == 1, 0, b - 1))

        @pl.when(((s % 2 == 1) & (b > 0) & (b < n_seq)) | (s == 0))
        def _():
            score_end(b)

    def a1(j):
        return send(part.at[j, 1 - core], got1.at[j], a1s.at[j], a1r.at[j], z, mate)

    def a2(j):
        return send(chip.at[j, 1 - y], got2.at[j], a2s.at[j], a2r.at[j], z, over)

    def a3(j, h):
        return send(ob.at[j, h], ob.at[j, h], a3s.at[j], a3r.at[j], z, mate)

    def b_right(j, p):
        return send(prod.at[j, p], from_l.at[j, p], brs.at[j, p], brr.at[j, p], z + 1, c)

    def b_left(j, p):
        return send(prod.at[j, p], from_r.at[j, p], bls.at[j, p], blr.at[j, p], z - 1, c)

    def c_right(j, p):
        return send(full.at[j, c, p], full.at[j, c, p], crs.at[j, p], crr.at[j, p], z + 1, c)

    def c_left(j, p):
        return send(full.at[j, c, p], full.at[j, c, p], cls.at[j, p], clr.at[j, p], z - 1, c)

    def c_over(j, q, p):
        return send(full.at[j, q, p], full.at[j, q, p], cys.at[j, p], cyr.at[j, p], z, over)

    def c_mate(j, q, u, p):
        return send(full.at[j, q, p], full.at[j, q, p], cps.at[j, u, p], cpr.at[j, u, p], z, mate)

    def merge(a, b):
        top = jnp.maximum(a[HEAD_DIM:129], b[HEAD_DIM:129])
        fa = jnp.exp2((a[HEAD_DIM:129] - top) * EXP2_SCALE)
        fb = jnp.exp2((b[HEAD_DIM:129] - top) * EXP2_SCALE)
        return a[0:HEAD_DIM] * fa + b[0:HEAD_DIM] * fb, top, a[129:130] * fa + b[129:130] * fb

    def stage_a1(j):
        a1(j).wait_recv()
        vals, top, total = merge(part[j, core], got1[j])
        for th in range(2):
            sel = slice(HEAD_DIM * th, HEAD_DIM * th + HEAD_DIM)
            chip[j, th, 0:HEAD_DIM] = vals[:, sel]
            chip[j, th, HEAD_DIM:136] = jnp.concatenate([top[:, sel], total[:, sel], jnp.zeros((6, HEAD_DIM), jnp.float32)], axis=0)
        a2(j).start()

    def stage_a2(j):
        a2(j).wait_recv()
        vals, _, total = merge(chip[j, y], got2[j])
        ob[j, core] = (vals / total).T
        a3(j, core).start()

    def stage_a3(j):
        a3(j, 1 - core).wait_recv()

        @pl.when(j == 0)
        def _():
            for p in range(n_part):
                wo_copy(p).wait()

        o = jnp.concatenate([ob[j, h, 32 * g : 32 * g + 32, :] for h in range(2) for g in range(4)], axis=1)
        o = o.astype(jnp.bfloat16)
        for p in range(n_part):
            prod[j, p] = jnp.dot(o, wo[p], preferred_element_type=jnp.float32)

        @pl.when(z == 0)
        def _():
            for p in (2, 3, 0, 1):
                b_right(j, p).start()

        @pl.when(z == last)
        def _():
            for p in (0, 1, 2, 3):
                b_left(j, p).start()

    def pass_right(j, p):
        b_right(j, p).wait_recv()
        prod[j, p] = prod[j, p] + from_l[j, p]
        b_right(j, p).start()

    def pass_left(j, p):
        b_left(j, p).wait_recv()
        prod[j, p] = prod[j, p] + from_r[j, p]
        b_left(j, p).start()

    def stage_b1(j):
        @pl.when(z == 1)
        def _():
            pass_right(j, 2)
            pass_right(j, 3)

        @pl.when(z == 2)
        def _():
            pass_left(j, 0)
            pass_left(j, 1)

    def spread(j, p):
        c_over(j, c, p).start()
        c_mate(j, c, 0, p).start()

    def stage_c0(j):
        x_copy(j).wait()

        def finish(p):
            b_right(j, p).wait_recv()
            b_left(j, p).wait_recv()
            x = xs[j, :, width * (p % 2) : width * (p % 2) + width].astype(jnp.float32)
            full[j, c, p] = prod[j, p] + from_l[j, p] + from_r[j, p] + x
            c_right(j, p).start()
            c_left(j, p).start()
            spread(j, p)

        @pl.when(z == 1)
        def _():
            finish(0)
            finish(1)

        @pl.when(z == 2)
        def _():
            finish(2)
            finish(3)

    def from_right(j, p, onward):
        c_left(j, p).wait_recv()
        if onward:
            c_left(j, p).start()
        spread(j, p)

    def from_left(j, p, onward):
        c_right(j, p).wait_recv()
        if onward:
            c_right(j, p).start()
        spread(j, p)

    def stage_c1(j):
        @pl.when(z == 0)
        def _():
            from_right(j, 0, False)
            from_right(j, 1, False)

        @pl.when(z == 1)
        def _():
            from_right(j, 2, True)
            from_right(j, 3, True)

        @pl.when(z == 2)
        def _():
            from_left(j, 0, True)
            from_left(j, 1, True)

        @pl.when(z == 3)
        def _():
            from_left(j, 2, False)
            from_left(j, 3, False)

    def stage_c2(j):
        @pl.when(z == 0)
        def _():
            from_right(j, 2, False)
            from_right(j, 3, False)

        @pl.when(z == 3)
        def _():
            from_left(j, 0, False)
            from_left(j, 1, False)

    def stage_over(j):
        for p in range(n_part):
            c_over(j, over, p).wait_recv()
            c_mate(j, over, 1, p).start()

    def stage_out(j):
        for p in range(n_part):
            c_mate(j, mate, 0, p).wait_recv()
            c_mate(j, over_mate, 1, p).wait_recv()
        for q in range(4):
            for p in range(n_part):
                col = width * (n_part * (q % 2) + p)
                rows = pl.ds(pl.multiple_of(64 * j + 32 * (q // 2), 32), 32)
                out_ref[rows, col : col + width] = full[j, q, p].astype(jnp.bfloat16)

    stages = [
        (stage_a1, 1), (stage_a2, 2), (stage_a3, 1), (stage_b1, 2), (stage_c0, 2), (stage_c1, 1), (stage_c2, 1),
        (stage_over, 3), (stage_out, 2),
    ]
    n_slots = 2 * n_seq + 2 + sum(lag for _, lag in stages)

    def slot(s, carry):
        @pl.when(s == 2)
        def _():
            in_copy(1).wait()
            norm_half(1)

        @pl.when((s >= 3) & (s < 3 + n_share))
        def _():
            share_tile(s - 3)

        @pl.when((s >= 5) & (s < 5 + n_share))
        def _():
            take_tile(s - 5)

        @pl.when(s < 2 * n_seq + 2)
        def _():
            attend(s)

        after = 3 + sum(lag for _, lag in stages)
        for stage_fn, lag in reversed(stages):
            t = s - after
            after -= lag

            @pl.when((t == -2) | ((t > 0) & (t % 2 == 0) & (t < 2 * n_seq)))
            def _():
                stage_fn(jnp.maximum(t, 0) // 2)

        return carry

    lax.fori_loop(0, n_slots, slot, 0)

    def drain(j, carry):
        a1(j).wait_send()
        a2(j).wait_send()
        a3(j, core).wait_send()
        for p in range(n_part):
            @pl.when((z == 0) | ((z == 1) & (p >= 2)))
            def _():
                b_right(j, p).wait_send()

            @pl.when((z == 3) | ((z == 2) & (p < 2)))
            def _():
                b_left(j, p).wait_send()

            @pl.when((z == 2) | ((z == 1) & (p < 2)))
            def _():
                c_right(j, p).wait_send()

            @pl.when((z == 1) | ((z == 2) & (p >= 2)))
            def _():
                c_left(j, p).wait_send()

            c_over(j, c, p).wait_send()
            c_mate(j, c, 0, p).wait_send()
            c_mate(j, over, 1, p).wait_send()
        return carry

    for m in range(n_share):
        share(m).wait_send()
    lax.fori_loop(0, n_seq, drain, 0)


def block(prefix_len, gain, q_gain, k_gain, x2, w_q, w_k, w_v, kc, vc, w_o):
    rows, d_model = x2.shape
    n_seq, cache_rows, _ = kc.shape
    n_part = 4
    width = d_model // (2 * n_part)
    n_q = w_q.shape[1] // 256
    new_rows = 2 * rows // n_seq
    n_share = (n_q + 2) // 2
    tile = min(2048, cache_rows // 2)
    half_dim = HEAD_DIM // 2
    freq = 1.0 / (1000000.0 ** (np.arange(half_dim, dtype=np.float64) * 2.0 / HEAD_DIM))
    freq = jnp.asarray(np.concatenate([freq, freq])[None], jnp.float32)
    hbm = pl.BlockSpec(memory_space=pl.ANY)
    vmem = pl.BlockSpec(memory_space=pltpu.VMEM)
    f32, bf16 = jnp.float32, jnp.bfloat16
    sems = pltpu.SemaphoreType.DMA
    piece = (32, width)
    return pl.pallas_call(
        functools.partial(block_kernel, tile=tile),
        out_shape=(
            pltpu.VMEM((rows, d_model), bf16),
            pltpu.VMEM((2 * rows, HEAD_DIM), bf16),
            pltpu.VMEM((2 * rows, HEAD_DIM), bf16),
        ),
        in_specs=[pl.BlockSpec(memory_space=pltpu.SMEM), vmem, vmem, vmem, vmem, hbm, hbm, hbm, hbm, hbm, hbm, hbm],
        out_specs=(vmem, vmem, vmem),
        scratch_shapes=[
            pltpu.VMEM((n_q, rows, 256), bf16),
            pltpu.VMEM((n_q + 2, d_model, 256), bf16),
            pltpu.VMEM((rows, HEAD_DIM), f32),
            pltpu.VMEM((rows, HEAD_DIM), f32),
            pltpu.VMEM((rows, HEAD_DIM), f32),
            pltpu.VMEM((n_share, rows // 2, 256), f32),
            pltpu.VMEM((n_share, rows // 2, 256), f32),
            pltpu.VMEM((2, cache_rows, HEAD_DIM), bf16),
            pltpu.VMEM((2, cache_rows, HEAD_DIM), bf16),
            pltpu.VMEM((256, 256), bf16),
            pltpu.VMEM((cache_rows, 256), f32),
            pltpu.VMEM((new_rows, 256), f32),
            pltpu.VMEM((256, 256), f32),
            pltpu.VMEM((8, 256), f32),
            pltpu.VMEM((8, 256), f32),
            pltpu.VMEM((8, 256), f32),
            pltpu.VMEM((n_part, w_o.shape[0], width), bf16),
            pltpu.VMEM((n_seq, 32, 2 * width), bf16),
            pltpu.VMEM((n_seq, 2, 136, 256), f32),
            pltpu.VMEM((n_seq, 136, 256), f32),
            pltpu.VMEM((n_seq, 2, 136, HEAD_DIM), f32),
            pltpu.VMEM((n_seq, 136, HEAD_DIM), f32),
            pltpu.VMEM((n_seq, 2, HEAD_DIM, HEAD_DIM), f32),
            pltpu.VMEM((n_seq, n_part, *piece), f32),
            pltpu.VMEM((n_seq, n_part, *piece), f32),
            pltpu.VMEM((n_seq, n_part, *piece), f32),
            pltpu.VMEM((n_seq, 4, n_part, *piece), f32),
            sems((2,)),
            sems((n_q + 2,)),
            sems((2,)),
            sems((2,)),
            sems((n_part,)),
            sems((n_seq,)),
            *[sems((n_seq,))] * 6,
            *[sems((n_share,))] * 2,
            *[sems((n_seq, n_part))] * 10,
            sems((n_seq, 2, n_part)),
            sems((n_seq, 2, n_part)),
        ],
        compiler_params=pltpu.CompilerParams(
            collective_id=0, has_side_effects=True, vmem_limit_bytes=int(58.5 * 1024 * 1024)
        ),
        cost_estimate=pl.CostEstimate(
            flops=4 * n_seq * cache_rows * 256 * 256, bytes_accessed=60 << 20, transcendentals=n_seq * cache_rows * 256
        ),
        name="block",
    )(prefix_len, gain, q_gain, k_gain, freq, x2, w_q, w_k, w_v, kc, vc, w_o)


def store_kernel(out_in, k_in, v_in, out_hbm, k_hbm, v_hbm, sem):
    copies = [
        pltpu.make_async_copy(src, dst, sem.at[i])
        for i, (src, dst) in enumerate(((out_in, out_hbm), (k_in, k_hbm), (v_in, v_hbm)))
    ]
    for copy in copies:
        copy.start()
    for copy in copies:
        copy.wait()


def store(*arrays):
    hbm = pl.BlockSpec(memory_space=pl.ANY)
    return pl.pallas_call(
        store_kernel,
        out_shape=tuple(jax.ShapeDtypeStruct(a.shape, a.dtype) for a in arrays),
        in_specs=[hbm] * 3,
        out_specs=(hbm,) * 3,
        scratch_shapes=[pltpu.SemaphoreType.DMA((3,))],
        compiler_params=pltpu.CompilerParams(vmem_limit_bytes=1024 * 1024),
        name="store",
    )(*arrays)


def solution(mesh):
    def per_device(hidden, prefix_len, k_cache, v_cache, attn_norm, w_q, w_k, w_v, w_o, q_norm, k_norm):
        n_seq, n_new, d_model = hidden.shape
        x2 = hidden.reshape(n_seq * n_new, d_model)
        results = block(
            prefix_len, attn_norm, q_norm, k_norm, x2, w_q, w_k, w_v,
            k_cache.reshape(n_seq, -1, HEAD_DIM), v_cache.reshape(n_seq, -1, HEAD_DIM), w_o,
        )
        out, k_rows, v_rows = store(*results)
        new_shape = (n_seq, n_new, 2, HEAD_DIM)
        return out.reshape(hidden.shape), k_rows.reshape(new_shape), v_rows.reshape(new_shape)

    cache_spec = P("dp", "cp", "tp", None)
    arg_specs = (P("dp", None, None), P("dp"), cache_spec, cache_spec, P(None), P(None, "tp"), P(None, "tp"), P(None, "tp"), P("tp", None), P(None), P(None))
    out_specs = (P("dp", None, None), P("dp", None, "tp", None), P("dp", None, "tp", None))
    return jax.shard_map(per_device, mesh=mesh, in_specs=arg_specs, out_specs=out_specs, check_vma=False)
```
